8 devices in a mesh: dp: 1 (over z), sz: 2 (over y), sy: 2 (over x), sx: 2 (over core).
Axes of the slice: x: 2, y: 2, z: 1, core: 2. Of those that a mesh axis runs over, the one named last changes fastest.
Arguments:
- rhs_grid: float32 [256, 256, 256], P(('dp', 'sx'), 'sy', 'sz')
- u_start: float32 [256, 256, 256], P(('dp', 'sx'), 'sy', 'sz')
Outputs:
- output: float32 [256, 256, 256], P(('dp', 'sx'), 'sy', 'sz')
All inputs are finite; a program needn't handle non-finite values.
Results may differ from the reference program's by a relative error of at most 0.001.
Values sent between devices are 32-bit elements.
A program may use at most 1 GiB of HBM per device.

```python
import math
import jax
import jax.numpy as jnp
from jax import lax

GRID_SIZE = 256
LEVELS = 4
SMOOTH_SWEEPS = 2
COARSE_SWEEPS = 16
BUMPS = 8


def setup_inputs(seed: int = 0, part: int = 0) -> dict:
    key = jax.random.fold_in(jax.random.key(seed), part)
    key_amp, key_pos, key_bump, key_init = jax.random.split(key, 4)
    cells = jnp.arange(GRID_SIZE, dtype=jnp.float32)
    coords = (cells + 1.0) / (GRID_SIZE + 1)
    sine = jnp.sin(math.pi * coords)
    mode_amp = jax.random.uniform(key_amp, (), jnp.float32, 0.5, 1.5)
    smooth = (3.0 * math.pi ** 2) * mode_amp * sine[:, None, None] * sine[None, :, None] * sine[None, None, :]
    centers = jax.random.randint(key_pos, (BUMPS, 3), 1, 8).astype(jnp.float32) * (GRID_SIZE // 8) - 0.5
    width = GRID_SIZE / 32.0
    bump_amp = jax.random.normal(key_bump, (BUMPS,), jnp.float32) * (0.8 * ((GRID_SIZE + 1) / width) ** 2)
    gauss = jnp.exp(-((cells[None, :, None] - centers[:, None, :]) ** 2) / (2.0 * width ** 2))
    bumps = jnp.einsum('bi,bj,bk->ijk', gauss[:, :, 0] * bump_amp[:, None], gauss[:, :, 1], gauss[:, :, 2])
    rhs_grid = smooth + bumps
    u_start = jax.random.normal(key_init, (GRID_SIZE, GRID_SIZE, GRID_SIZE), jnp.float32)
    return {'rhs_grid': rhs_grid, 'u_start': u_start}


def neighbour_sum(field):
    padded = jnp.pad(field, 1)
    return (padded[:-2, 1:-1, 1:-1] + padded[2:, 1:-1, 1:-1]
            + padded[1:-1, :-2, 1:-1] + padded[1:-1, 2:, 1:-1]
            + padded[1:-1, 1:-1, :-2] + padded[1:-1, 1:-1, 2:])


def residual(source, field, stiffness):
    return source - stiffness * (6.0 * field - neighbour_sum(field))


def jacobi_sweep(source, field, stiffness):
    return field + residual(source, field, stiffness) / (9.0 * stiffness)


def restrict_axis(fine, axis):
    half = fine.shape[axis] // 2
    pairs = fine.reshape(fine.shape[:axis] + (half, 2) + fine.shape[axis + 1:])
    even = lax.index_in_dim(pairs, 0, axis + 1, keepdims=False)
    odd = lax.index_in_dim(pairs, 1, axis + 1, keepdims=False)
    lower = jnp.zeros_like(lax.slice_in_dim(odd, 0, 1, axis=axis))
    odd_prev = jnp.concatenate([lower, lax.slice_in_dim(odd, 0, half - 1, axis=axis)], axis=axis)
    return 0.25 * (odd_prev + odd) + 0.5 * even


def prolong_axis(coarse, axis):
    length = coarse.shape[axis]
    upper = jnp.zeros_like(lax.slice_in_dim(coarse, 0, 1, axis=axis))
    shifted = jnp.concatenate([lax.slice_in_dim(coarse, 1, length, axis=axis), upper], axis=axis)
    stacked = jnp.stack([coarse, 0.5 * (coarse + shifted)], axis=axis + 1)
    return stacked.reshape(coarse.shape[:axis] + (2 * length,) + coarse.shape[axis + 1:])


def restrict(fine):
    for axis in range(3):
        fine = restrict_axis(fine, axis)
    return fine


def prolong(coarse):
    for axis in range(3):
        coarse = prolong_axis(coarse, axis)
    return coarse


def vcycle(level, source, field):
    stiffness = ((GRID_SIZE + 1) / 2 ** level) ** 2
    coarsest = level == LEVELS - 1
    sweeps = COARSE_SWEEPS if coarsest else SMOOTH_SWEEPS
    if field is None:
        field = source / (9.0 * stiffness)
        sweeps = sweeps - 1
    for sweep in range(sweeps):
        field = jacobi_sweep(source, field, stiffness)
    if coarsest:
        return field
    correction = vcycle(level + 1, restrict(residual(source, field, stiffness)), None)
    field = field + prolong(correction)
    for sweep in range(SMOOTH_SWEEPS):
        field = jacobi_sweep(source, field, stiffness)
    return field


def reference(rhs_grid, u_start):
    return vcycle(0, rhs_grid, u_start)
```

```python
import functools
import jax
import jax.numpy as jnp
from jax import lax
from jax.experimental import pallas as pl
from jax.experimental.pallas import tpu as pltpu
from jax.sharding import PartitionSpec as P

N = 128
PR = 144
NC = 4
CR = 128 // NC
YR = 136
XR = 72
GI = 16
S, W = 8, 128
LAST = W - 1
MESH = pl.DeviceIdType.MESH
F32 = jnp.float32
HI = lax.Precision.HIGHEST


class Lev:
    def __init__(self, n, h, pj, kp, hb, ni, region, unroll, group):
        self.n, self.h, self.pj, self.kp, self.hb, self.ni = n, h, pj, kp, hb, ni
        self.region, self.unroll, self.group = region, unroll, group
        self.nk = n + 2 * kp
        self.planes = n + 2 * pj
        self.rows = self.planes * self.nk


L1 = Lev(64, 4, 6, 8, 8, 128, 68, 4, 1)
L2 = Lev(32, 5, 10, 8, 8, 64, 40, 8, 12)
L3 = Lev(16, 16, 18, 16, 16, 32, 32, 8, 10)
LEVS = (L1, L2, L3)


def up8(x):
    return (x + 7) // 8 * 8


def eight(r):
    return pl.ds(r, S)


def body(h2, f_hbm, u_hbm, out_hbm, A, B, F, Y, X, XP, RXP, TS, KS, PK, RZ, PY, RY,
         G1, V1, W1, G2, V2, W2, G3, V3, W3, E, T2,
         RY1, SZ1, RZ1, RY2, SZ2, RZ2, RY3, SZ3, RZ3,
         ld, st, xs, xr, zs, zr, ys, yr, cs, cr):
    cx, cy, cz = lax.axis_index('sx'), lax.axis_index('sy'), lax.axis_index('sz')
    lane = lax.broadcasted_iota(jnp.int32, (CR, W), 1)
    lane0, lane127 = lane == 0, lane == LAST
    even = lane % 2 == 0
    ninth = F32(1.0 / 9.0)
    px, py, pz = {'sx': 1 - cx}, {'sy': 1 - cy}, {'sz': 1 - cz}
    edge = LAST * (1 - cz)
    bufs = (A, B)

    def flat(ref):
        return ref.reshape(ref.shape[0] * ref.shape[1], ref.shape[2])

    A2, B2, Y2, X2 = flat(A), flat(B), flat(Y), flat(X)
    flats = (A2, B2)

    def chunk_of(c):
        return c * cy + (NC - 1 - c) * (1 - cy)

    def load(k):
        rows = pl.ds(k * CR, CR)
        a = pltpu.make_async_copy(u_hbm.at[:, rows, :], A.at[pl.ds(1, N), pl.ds(S + k * CR, CR), :], ld.at[0, k])
        b = pltpu.make_async_copy(f_hbm.at[:, rows, :], F.at[:, rows, :], ld.at[1, k])
        return a, b
    for k in range(NC):
        for cp in load(k):
            cp.start()

    barrier = pltpu.get_barrier_semaphore()
    for p in (px, py, pz):
        pl.semaphore_signal(barrier, inc=1, device_id=p, device_id_type=MESH)
    pl.semaphore_wait(barrier, 3)

    zero = jnp.zeros((S, W), F32)
    blank = jnp.zeros((CR, W), F32)

    def zero_rows(ref2, count):
        @pl.loop(0, count // 64)
        def _(t):
            ref2[pl.ds(pl.multiple_of(t * 64, 64), 64), :] = jnp.zeros((64, W), F32)
        if count % 64:
            ref2[pl.ds(count // 64 * 64, count % 64), :] = jnp.zeros((count % 64, W), F32)
    for ref in (G1, V1, W1, G2, V2, W2, G3, V3, W3, E):
        zero_rows(ref, ref.shape[0])

    for buf in bufs:
        gx = 129 * cx
        @pl.loop(0, PR // S)
        def _(t):
            buf[gx, eight(pl.multiple_of(t * S, S)), :] = zero

        @pl.loop(0, 130)
        def _(i):
            buf[i, eight(0), :] = zero
            buf[i, eight(136), :] = zero

    @pl.loop(0, 65)
    def _(i):
        Y[i, eight(0), :] = zero

    @pl.loop(0, XR // S)
    def _(t):
        X[W, eight(pl.multiple_of(t * S, S)), :] = zero
    for q in range(5):
        TS[q, eight(0), :] = zero

    def x_copy(par, k):
        rows = pl.ds(pl.multiple_of(S + k * CR, S), CR)
        return pltpu.make_async_remote_copy(
            src_ref=bufs[par].at[W - LAST * cx, rows, :], dst_ref=bufs[par].at[129 * cx, rows, :],
            send_sem=xs.at[par, k], recv_sem=xr.at[par, k], device_id=px, device_id_type=MESH)

    def z_copy(par, k):
        rows = pl.ds(pl.multiple_of(k * CR, S), CR)
        return pltpu.make_async_remote_copy(
            src_ref=PK.at[par, rows, :], dst_ref=RZ.at[par, rows, :],
            send_sem=zs.at[par, k], recv_sem=zr.at[par, k], device_id=pz, device_id_type=MESH)

    def y_copy(par):
        return pltpu.make_async_remote_copy(
            src_ref=PY.at[par], dst_ref=RY.at[par],
            send_sem=ys.at[par], recv_sem=yr.at[par], device_id=py, device_id_type=MESH)

    def send(par, c, k):
        x_copy(par, k).start()
        z_copy(par, k).start()

        @pl.when(c == 0)
        def _():
            j = LAST * (1 - cy)
            for t in range(16):
                PY[par, eight(t * S), :] = flats[par][pl.ds((t * S + 1) * PR + S + j, S, stride=PR), :]
            y_copy(par).start()

    def receive(par, c, k):
        x_copy(par, k).wait()
        z_copy(par, k).wait()

        @pl.when(c == 0)
        def _():
            y_copy(par).wait()
            j = 136 * (1 - cy) + 7 * cy
            for t in range(16):
                flats[par][pl.ds((t * S + 1) * PR + j, S, stride=PR), :] = RY[par, eight(t * S), :]

    def spin(value, i):
        return pltpu.roll(value, (i - edge + 2 * W) & LAST, 1)

    def chunk(k, shift=0):
        return pl.ds(k * CR + shift, CR)

    def pack_group(buf, k, i0, count, first, cols):
        rows = chunk(k, S)
        for q in range(count):
            cols = jnp.where(lane == first + q, spin(buf[i0 + q + 1, rows, :], first + q), cols)
        return cols

    def pack_chunk(par, k):
        def step(t, cols):
            i0 = t * 2 * GI
            return pack_group(bufs[par], k, i0, 2 * GI, i0, cols)
        PK[par, chunk(k), :] = lax.fori_loop(0, N // (2 * GI), step, blank)

    def stencil_chunk(src, par, k, dst, visit, extra):
        ghost = RZ[par, chunk(k), :]
        ghosts = (jnp.where(even, ghost, 0.0), jnp.where(even, 0.0, ghost))
        rows, below, above = chunk(k, S), chunk(k, S - 1), chunk(k, S + 1)

        def side_sums(i0):
            for q in range(GI):
                c = src[i0 + q + 1, rows, :]
                g = pltpu.roll(ghosts[q & 1], (edge - i0 - q + W) & LAST, 1)
                KS[pl.ds(q * CR, CR), :] = jnp.where(lane0, g, pltpu.roll(c, 1, 1)) + jnp.where(
                    lane127, g, pltpu.roll(c, LAST, 1))

        def step(t, state):
            um, uc, cols, extra = state
            i0 = t * GI
            if dst is not None:
                cols = pack_group(dst, k, (i0 + N - GI) % N, GI, i0 - GI, cols)
            for q in range(GI):
                un = src[i0 + q + 2, rows, :]
                total = (um + un) + (src[i0 + q + 1, below, :] + src[i0 + q + 1, above, :]) + KS[pl.ds(q * CR, CR), :]
                extra = visit(t, i0, q, uc, total, extra)
                um, uc = uc, un
            side_sums((i0 + GI) % N)
            return um, uc, cols, extra
        side_sums(0)
        state = (src[0, rows, :], src[1, rows, :], blank, extra)
        _, _, cols, extra = lax.fori_loop(0, N // GI, step, state)
        if dst is not None:
            cols = pack_group(dst, k, N - GI, GI, N - GI, cols)
        return cols, extra

    def sweep_pass(par, first, last):
        src, dst = bufs[par], bufs[1 - par]

        @pl.loop(0, NC)
        def _(c):
            k = chunk_of(c)
            receive(par, c, k)

            def visit(t, i0, q, centre, total, extra):
                fs = F[i0 + q, chunk(k), :]
                if first:
                    fs = fs * F32(h2)
                    F[i0 + q, chunk(k), :] = fs
                dst[i0 + q + 1, chunk(k, S), :] = (3.0 * centre + (total + fs)) * ninth
                return extra
            cols, _ = stencil_chunk(src, par, k, None if last else dst, visit, ())
            if last:
                store(k).start()
            else:
                PK[1 - par, chunk(k), :] = cols
                send(1 - par, c, k)

    def store(k):
        return pltpu.make_async_copy(
            B.at[pl.ds(1, N), pl.ds(pl.multiple_of(S + k * CR, S), CR), :],
            out_hbm.at[:, pl.ds(pl.multiple_of(k * CR, S), CR), :], st.at[k])

    for k in range(NC):
        for cp in load(k):
            cp.wait()

    @pl.loop(0, NC)
    def _(c):
        k = chunk_of(c)
        pack_chunk(0, k)
        send(0, c, k)

    sweep_pass(0, True, False)
    sweep_pass(1, False, False)

    @pl.loop(0, NC)
    def _(c):
        k = chunk_of(c)
        receive(0, c, k)

        def visit(t, i0, q, centre, total, carry):
            low, mid = carry
            r = F[i0 + q, chunk(k), :] - 6.0 * centre + total
            if q % 2 == 0:
                return low, r
            Y[t * (GI // 2) + q // 2, chunk(k, S), :] = (low + r) + 2.0 * mid
            return r, mid
        _, lows = stencil_chunk(A, 0, k, None, visit, (blank, blank))
        Y[64, chunk(k, S), :] = lows[0]

    def restrict_j(src_plane, dst, dst_plane):
        base = src_plane * YR
        lo, mid, hi = (Y2[pl.ds(base + S + d, 64, stride=2), :] for d in (-1, 0, 1))
        dst[pl.ds(pl.multiple_of(dst_plane * XR, S), 64), :] = (lo + hi) + 2.0 * mid
        row = lax.broadcasted_iota(jnp.int32, (S, W), 0)
        dst[eight(pl.multiple_of(dst_plane * XR + 64, S)), :] = jnp.where(
            row == 0, pltpu.roll(Y2[eight(base + W), :], 1, 0), 0.0)

    @pl.loop(0, 64)
    def _(i):
        restrict_j(i, X2, i + 64 * cx)
    restrict_j(64, XP, 0)

    own = pl.ds(64 * cx, 64)
    cpx = [pltpu.make_async_remote_copy(src_ref=X.at[own], dst_ref=X.at[own], send_sem=cs.at[0], recv_sem=cr.at[0],
                                        device_id=px, device_id_type=MESH),
           pltpu.make_async_remote_copy(src_ref=XP, dst_ref=RXP, send_sem=cs.at[1], recv_sem=cr.at[1],
                                        device_id=px, device_id_type=MESH)]
    for cp in cpx:
        cp.start()
    for cp in cpx:
        cp.wait()
    for t in range(9):
        r = eight(t * S)
        X2[eight(64 * XR + t * S), :] += jnp.where(cx == 0, XP[r, :], RXP[r, :])

    @pl.loop(0, 13)
    def _(jo):
      for q in range(5):
        jc = jo * 5 + q
        TS[q, pl.ds(S, W), :] = jnp.transpose(X2[pl.ds(jc, W, stride=XR), :])
        base = (jc + L1.pj) * L1.nk + L1.kp
        lo, mid, hi = (TS[q, pl.ds(S + d, 64, stride=2), :] for d in (-1, 0, 1))
        G1[pl.ds(pl.multiple_of(base, S), 64), :] = ((lo + hi) + 2.0 * mid) * F32(1 / 16)
        G1[pl.ds(base + 64, 1), :] = TS[q, pl.ds(135, 1), :] * F32(1 / 16)

    def wide_exchange(L, G, RYl, SZl, RZl, s):
        cnt = L.h + 1
        js = (L.n - L.h) * (1 - cy)
        cp = pltpu.make_async_remote_copy(
            src_ref=G.at[pl.ds(pl.multiple_of((js + L.pj) * L.nk, S), cnt * L.nk), :], dst_ref=RYl,
            send_sem=cs.at[s], recv_sem=cr.at[s], device_id=py, device_id_type=MESH)
        cp.start()
        cp.wait()
        jd = (L.n * (1 - cy) - L.h * cy + L.pj) * L.nk

        @pl.loop(0, cnt)
        def _(p):
            r = pl.multiple_of(p * L.nk, S)
            G[pl.ds(pl.multiple_of(jd + r, S), L.nk), :] += RYl[pl.ds(r, L.nk), :]
        ks = (L.n - L.h) * (1 - cz) + L.kp
        kd = L.n * (1 - cz) - L.h * cz + L.kp
        jl = L.pj - L.h * cy

        @pl.loop(0, L.n + L.h)
        def _(p):
            SZl[pl.ds(p * cnt, cnt), :] = G[pl.ds((jl + p) * L.nk + ks, cnt), :]
        cp = pltpu.make_async_remote_copy(src_ref=SZl, dst_ref=RZl, send_sem=cs.at[s + 1], recv_sem=cr.at[s + 1],
                                          device_id=pz, device_id_type=MESH)
        cp.start()
        cp.wait()

        @pl.loop(0, L.n + L.h)
        def _(p):
            G[pl.ds((jl + p) * L.nk + kd, cnt), :] += RZl[pl.ds(p * cnt, cnt), :]
            G[pl.ds((jl + p) * L.nk + L.kp - 1 + (L.n + 1) * cz, 1), :] = zero[:1]
        G[pl.ds(pl.multiple_of((L.pj - 1 + (L.n + 1) * cy) * L.nk, S), L.nk), :] = jnp.zeros((L.nk, W), F32)

    def coarse_sum(L, src, r, count):
        lanes = lax.broadcasted_iota(jnp.int32, (count, W), 1)
        c = src[pl.ds(r, count), :]
        left = jnp.where(lanes == 0, 0.0, pltpu.roll(c, 1, 1))
        right = jnp.where(lanes == L.ni - 1, 0.0, pltpu.roll(c, LAST, 1))
        total = (src[pl.ds(r - L.nk, count), :] + src[pl.ds(r + L.nk, count), :]) + (
            src[pl.ds(r - 1, count), :] + src[pl.ds(r + 1, count), :]) + (left + right)
        return c, total

    def coarse_pass(L, src, visit):
        j0 = L.pj - (L.region - L.n) * cy
        k0 = L.kp - L.hb * cz
        count = L.n + L.hb

        @pl.loop(0, L.region // L.unroll)
        def _(po):
            for p in range(L.unroll):
                r = pl.multiple_of((j0 + po * L.unroll + p) * L.nk + k0, S)
                visit(pl.ds(r, count), *coarse_sum(L, src, r, count))

    def first_two(L, G, V):
        def visit(rows, c, total):
            V[rows, :] = (12.0 * c + total) * F32(1 / 81)
        coarse_pass(L, G, visit)

    def smooth(L, G, V, W_):
        def visit(rows, c, total):
            W_[rows, :] = (3.0 * c + (total + G[rows, :])) * ninth
        coarse_pass(L, V, visit)

    def weights(ni, up):
        a = lax.broadcasted_iota(jnp.int32, (W, W), 0)
        b = lax.broadcasted_iota(jnp.int32, (W, W), 1)
        if up:
            fine, coarse = b, a
            w = jnp.where(fine == 2 * coarse, 1.0, 0.0) + jnp.where(
                (fine == 2 * coarse + 1) | (fine == 2 * coarse - 1), 0.5, 0.0)
        else:
            fine, coarse = a, b
            w = jnp.where(fine == 2 * coarse, 2.0, 0.0) + jnp.where(
                (fine == 2 * coarse + 1) | (fine == 2 * coarse - 1), 1.0, 0.0)
        return jnp.where((coarse < ni) & (fine < 2 * ni), w, 0.0).astype(F32)

    def restrict_coarse(L, M, G, V, W_, Gc):
        @pl.loop(0, L.n // 4)
        def _(po):
            for p in range(4):
                r = pl.multiple_of((L.pj + po * 4 + p) * L.nk + L.kp, S)
                c, total = coarse_sum(L, V, r, L.n)
                W_[pl.ds(r, L.n), :] = G[pl.ds(r, L.n), :] - 6.0 * c + total
        for side in (L.pj - 1, L.pj + L.n, L.pj + L.n + 1):
            W_[pl.ds(side * L.nk, L.nk), :] = jnp.zeros((L.nk, W), F32)

        @pl.loop(0, L.n)
        def _(p):
            base = (L.pj + p) * L.nk + L.kp
            W_[eight(pl.multiple_of(base - S, S)), :] = zero
            W_[eight(pl.multiple_of(base + L.n, S)), :] = zero
        w = weights(M.ni, False)

        @pl.loop(0, M.n + 1)
        def _(p):
            base = (L.pj + 2 * p) * L.nk + L.kp
            rows = M.n + 4
            sums = []
            for dj in (-1, 0, 1):
                lo, mid, hi = (W_[pl.ds(base + dj * L.nk + d, rows, stride=2), :] for d in (-1, 0, 1))
                sums.append((lo + hi) + 2.0 * mid)
            T2[pl.ds(p * (M.n + S), rows), :] = (sums[0] + sums[2]) + 2.0 * sums[1]
        hr = M.n + S
        group = (M.n + 1) // (1 + 2 * (M.n // 32))

        @pl.loop(0, (M.n + 1) // group)
        def _(g):
            t0 = pl.multiple_of(g * group * hr, S)
            res = jnp.dot(T2[pl.ds(t0, group * hr), :], w, precision=HI, preferred_element_type=F32) * F32(1 / 16)
            for p in range(group):
                rb = (M.pj + g * group + p) * M.nk + M.kp
                Gc[pl.ds(pl.multiple_of(rb, S), M.n), :] = res[p * hr:p * hr + M.n]
                Gc[pl.ds(rb + M.n, 1), :] = res[p * hr + M.n:p * hr + M.n + 1]

    def prolong_coarse(L, M, V, e):
        w = weights(M.ni, True)
        extra = 3
        j0 = M.pj - extra * cy

        @pl.loop(0, (M.n + extra + 1) // M.group)
        def _(g):
            rows = pl.ds(pl.multiple_of((j0 + g * M.group) * M.nk, S), M.group * M.nk)
            E[rows, :] = jnp.dot(e[rows, :], w, precision=HI, preferred_element_type=F32)

        @pl.loop(0, M.n + extra)
        def _(p):
            jc = j0 + p - M.pj
            fb = (L.pj + 2 * jc) * L.nk + L.kp
            eb = (j0 + p) * M.nk + M.kp
            for kc, rows in ((0, M.n), (M.n * (1 - cz) - 4 * cz, 4)):
                a, b = E[pl.ds(eb + kc, rows), :], E[pl.ds(eb + kc + 1, rows), :]
                c, d = E[pl.ds(eb + M.nk + kc, rows), :], E[pl.ds(eb + M.nk + kc + 1, rows), :]
                ab = a + b
                f = fb + 2 * kc
                V[pl.ds(f, rows, stride=2), :] += a
                V[pl.ds(f + 1, rows, stride=2), :] += 0.5 * ab
                V[pl.ds(f + L.nk, rows, stride=2), :] += 0.5 * (a + c)
                V[pl.ds(f + L.nk + 1, rows, stride=2), :] += 0.25 * (ab + (c + d))

    wide_exchange(L1, G1, RY1, SZ1, RZ1, 2)
    first_two(L1, G1, V1)
    restrict_coarse(L1, L2, G1, V1, W1, G2)
    wide_exchange(L2, G2, RY2, SZ2, RZ2, 4)
    first_two(L2, G2, V2)
    restrict_coarse(L2, L3, G2, V2, W2, G3)
    wide_exchange(L3, G3, RY3, SZ3, RZ3, 6)
    first_two(L3, G3, V3)

    @pl.loop(0, 7)
    def _(s):
        smooth(L3, G3, V3, W3)
        smooth(L3, G3, W3, V3)
    prolong_coarse(L2, L3, V2, V3)
    smooth(L2, G2, V2, W2)
    smooth(L2, G2, W2, V2)
    prolong_coarse(L1, L2, V1, V2)
    smooth(L1, G1, V1, W1)
    smooth(L1, G1, W1, V1)

    @pl.loop(0, 13)
    def _(jo):
      for q in range(5):
        jc = jo * 5 + q
        base = (jc + L1.pj) * L1.nk + L1.kp
        a, b = V1[pl.ds(pl.multiple_of(base, S), 64), :], V1[pl.ds(base + 1, 64), :]
        TS[q, pl.ds(S, 64, stride=2), :] = a
        TS[q, pl.ds(S + 1, 64, stride=2), :] = 0.5 * (a + b)
        X2[pl.ds(jc, W, stride=XR), :] = jnp.transpose(TS[q, pl.ds(S, W), :])

    @pl.loop(0, NC)
    def _(c):
        k = chunk_of(c)

        @pl.loop(0, 64)
        def _(i):
            half = CR // 2
            xb = (i + 64 * cx) * XR + k * half
            a, b = X2[pl.ds(xb, half), :], X2[pl.ds(xb + 1, half), :]
            cc, d = X2[pl.ds(xb + XR, half), :], X2[pl.ds(xb + XR + 1, half), :]
            ab = a + b
            f = (2 * i + 1) * PR + S + k * CR
            for shift, value in ((0, a), (1, 0.5 * ab), (PR, 0.5 * (a + cc)), (PR + 1, 0.25 * (ab + (cc + d)))):
                rows = pl.ds(f + shift, half, stride=2)
                B2[rows, :] = A2[rows, :] + value
        pack_chunk(1, k)
        send(1, c, k)

    sweep_pass(1, False, False)
    sweep_pass(0, False, True)
    for k in range(NC):
        store(k).wait()


def solution(mesh):
    spec = P(('dp', 'sx'), 'sy', 'sz')

    def local(f, u):
        size = 2 * f.shape[1]
        h2 = 1.0 / float((size + 1) ** 2)
        vm = lambda *s: pltpu.VMEM(s, F32)
        scratch = [vm(130, PR, W), vm(130, PR, W), vm(N, N, W), vm(65, YR, W), vm(129, XR, W),
                   vm(XR, W), vm(XR, W), vm(5, 136, W), vm(GI * CR, W), vm(2, N, W), vm(2, N, W), vm(2, N, W), vm(2, N, W)]
        for L in LEVS:
            scratch += [vm(L.rows, W)] * 3
        scratch += [vm(max(L2.rows, L3.rows), W), vm(33 * 40, W)]
        for L in LEVS:
            z = up8((L.n + L.h) * (L.h + 1))
            scratch += [vm((L.h + 1) * L.nk, W), vm(z, W), vm(z, W)]
        dma = pltpu.SemaphoreType.DMA
        scratch += [dma((2, NC)), dma((NC,)), dma((2, NC)), dma((2, NC)), dma((2, NC)), dma((2, NC)), dma((2,)), dma((2,)),
                    dma((S,)), dma((S,))]
        return pl.pallas_call(
            functools.partial(body, h2),
            out_shape=jax.ShapeDtypeStruct(f.shape, F32),
            in_specs=[pl.BlockSpec(memory_space=pl.ANY)] * 2,
            out_specs=pl.BlockSpec(memory_space=pl.ANY),
            scratch_shapes=scratch,
            compiler_params=pltpu.CompilerParams(collective_id=0, has_side_effects=True, vmem_limit_bytes=67043328),
        )(f, u)

    def run(rhs_grid, u_start):
        return jax.shard_map(local, mesh=mesh, in_specs=(spec, spec), out_specs=spec, check_vma=False)(rhs_grid, u_start)
    return run
```

```python
import functools
import jax
import jax.numpy as jnp
from jax import lax
from jax.experimental import pallas as pl
from jax.experimental.pallas import tpu as pltpu
from jax.sharding import PartitionSpec as P

N = 128
PR = 144
NC = 4
XR = 72
CP = N // NC
GP = 4
GC = CP // GP
NG = N // GP
RB = 32
S, W = 8, 128
LAST = W - 1
MESH = pl.DeviceIdType.MESH
F32 = jnp.float32
HI = lax.Precision.HIGHEST


class Lev:
    def __init__(self, n, h, pj, kp, hb, ni, region, unroll, group):
        self.n, self.h, self.pj, self.kp, self.hb, self.ni = n, h, pj, kp, hb, ni
        self.region, self.unroll, self.group = region, unroll, group
        self.nk = n + 2 * kp
        self.planes = n + 2 * pj
        self.rows = self.planes * self.nk


L1 = Lev(64, 4, 6, 8, 8, 128, 68, 4, 1)
L2 = Lev(32, 5, 10, 8, 8, 64, 40, 8, 12)
L3 = Lev(16, 16, 18, 16, 16, 32, 32, 8, 10)
LEVS = (L1, L2, L3)


def up8(x):
    return (x + 7) // 8 * 8


def eight(r):
    return pl.ds(r, S)


def body(h2, f_hbm, u_hbm, out_hbm, A, B, AT, BT, F, X, XP, RXP, TS, KS, PZ, RZ, PY, RY,
         G2, V2, W2, G3, V3, W3, E, T2,
         RY1, SZ1, RZ1, RY2, SZ2, RZ2, RY3, SZ3, RZ3,
         ld, st, xs, xr, zs, zr, ys, yr, cs, cr):
    cx, cy, cz = lax.axis_index('sx'), lax.axis_index('sy'), lax.axis_index('sz')
    ninth = F32(1.0 / 9.0)
    px, py, pz = {'sx': 1 - cx}, {'sy': 1 - cy}, {'sz': 1 - cz}
    bufs = (A, B)

    def flat(ref):
        return ref.reshape(ref.shape[0] * ref.shape[1], ref.shape[2])

    A2, B2, X2 = flat(A), flat(B), flat(X)
    flats, turned = (A2, B2), (AT, BT)
    G1, V1, W1 = (AT.at[pl.ds(p * L1.rows, L1.rows), :] for p in range(3))

    def chunk_of(c):
        return c * cx + (NC - 1 - c) * (1 - cx)

    def block(i, shift=0, count=W):
        if isinstance(shift, int) and shift % S == 0:
            return pl.ds(pl.multiple_of(i * PR + S + shift, S), count)
        return pl.ds(i * PR + S + shift, count)

    def load(which, k):
        planes = pl.ds(k * CP, CP)
        src, dst = ((u_hbm, A.at[pl.ds(k * CP + 1, CP), pl.ds(S, W), :]), (f_hbm, F.at[planes]))[which]
        return pltpu.make_async_copy(src.at[planes], dst, ld.at[which, k])
    for which in range(2):
        for c in range(NC):
            load(which, chunk_of(c)).start()

    barrier = pltpu.get_barrier_semaphore()
    for p in (px, py, pz):
        pl.semaphore_signal(barrier, inc=1, device_id=p, device_id_type=MESH)
    pl.semaphore_wait(barrier, 3)

    zero = jnp.zeros((S, W), F32)

    def zero_rows(ref2, count):
        @pl.loop(0, count // 64)
        def _(t):
            ref2[pl.ds(pl.multiple_of(t * 64, 64), 64), :] = jnp.zeros((64, W), F32)
        if count % 64:
            ref2[pl.ds(count // 64 * 64, count % 64), :] = jnp.zeros((count % 64, W), F32)
    for ref in (G2, V2, W2, G3, V3, W3):
        zero_rows(ref, ref.shape[0])

    for buf in flats:
        buf[block(129 * cx, -S, PR), :] = jnp.zeros((PR, W), F32)
        for side in (-1, W):
            buf[pl.ds(PR + S + side, N, stride=PR), :] = jnp.zeros((N, W), F32)

    def zero_turned(buf, sides):
        for side in sides:
            buf[pl.ds(S + side, N, stride=PR), :] = jnp.zeros((N, W), F32)
    zero_turned(AT, (-1, W))
    zero_turned(BT, (-1, W))

    @pl.loop(0, XR // S)
    def _(t):
        X[W, eight(pl.multiple_of(t * S, S)), :] = zero
    for q in range(5):
        TS[q, eight(0), :] = zero

    def x_copy(par):
        return pltpu.make_async_remote_copy(
            src_ref=flats[par].at[block(W - LAST * cx), :], dst_ref=flats[par].at[block(129 * cx), :],
            send_sem=xs.at[par], recv_sem=xr.at[par], device_id=px, device_id_type=MESH)

    def side_copy(par, k, src, dst, ssem, rsem, to):
        planes = pl.ds(pl.multiple_of(k * CP, S), CP)
        return pltpu.make_async_remote_copy(
            src_ref=src.at[par, planes, :], dst_ref=dst.at[par, planes, :],
            send_sem=ssem.at[par, k], recv_sem=rsem.at[par, k], device_id=to, device_id_type=MESH)

    def side_copies(par, k):
        return side_copy(par, k, PY, RY, ys, yr, py), side_copy(par, k, PZ, RZ, zs, zr, pz)

    def send(par, k):
        planes = pl.ds(k * CP, CP)
        PY[par, planes, :] = flats[par][pl.ds((k * CP + 1) * PR + S + LAST * (1 - cy), CP, stride=PR), :]
        PZ[par, planes, :] = turned[par][pl.ds(k * CP * PR + S + LAST * (1 - cz), CP, stride=PR), :]
        for cp in side_copies(par, k):
            cp.start()

    def receive(par, k):
        for cp in side_copies(par, k):
            cp.wait()
        planes = pl.ds(k * CP, CP)
        flats[par][pl.ds((k * CP + 1) * PR + S + W - (W + 1) * cy, CP, stride=PR), :] = RY[par, planes, :]
        turned[par][pl.ds(k * CP * PR + S + W - (W + 1) * cz, CP, stride=PR), :] = RZ[par, planes, :]

    def place(g):
        return chunk_of(g // GC) * CP + g % GC * GP

    def turn(par, i0, count):
        for q in range(count):
            turned[par][block(i0 + q), :] = jnp.transpose(flats[par][block(i0 + q + 1), :])

    def side_sums(par, i0):
        for q in range(GP):
            KS[pl.ds(q * W, W), :] = jnp.transpose(turned[par][block(i0 + q, -1), :] + turned[par][block(i0 + q, 1), :])

    def after_chunk(g, done):
        @pl.when((g % GC == 0) & (g > 0))
        def _():
            done(g // GC - 1)

    def first_chunk(par, c):
        @pl.when(c == 0)
        def _():
            x_copy(par).start()

    def stencil_pass(par, visit, dst, done):
        src = flats[par]
        x_copy(par).wait()
        receive(par, chunk_of(0))
        side_sums(par, place(0))

        @pl.loop(0, NG)
        def _(g):
            @pl.when((g % GC == GC - 1) & (g < NG - 1))
            def _():
                receive(par, chunk_of(g // GC + 1))
            i0 = place(g)
            if dst is not None:
                turn(dst, place((g + NG - 1) % NG), GP)
            for t in range(W // RB):
                r = t * RB
                um, uc = src[block(i0, r, RB), :], src[block(i0 + 1, r, RB), :]
                for q in range(GP):
                    un = src[block(i0 + q + 2, r, RB), :]
                    total = (um + un) + (src[block(i0 + q + 1, r - 1, RB), :] + src[block(i0 + q + 1, r + 1, RB), :]) + KS[
                        pl.ds(q * W + r, RB), :]
                    visit(i0 + q, r, uc, total)
                    um, uc = uc, un
            side_sums(par, place((g + 1) % NG))
            if done is not None:
                after_chunk(g, done)
        if dst is not None:
            turn(dst, place(NG - 1), GP)
        if done is not None:
            done(NC - 1)

    def sweep_pass(par, first, last):
        if first:
            for k in range(NC):
                load(1, k).wait()

        def visit(i, r, centre, total):
            fs = F[i, pl.ds(r, RB), :]
            if first:
                fs = fs * F32(h2)
                F[i, pl.ds(r, RB), :] = fs
            flats[1 - par][block(i + 1, r, RB), :] = (3.0 * centre + (total + fs)) * ninth

        def done(c):
            k = chunk_of(c)
            if last:
                store(k).start()
            else:
                first_chunk(1 - par, c)
                send(1 - par, k)
        stencil_pass(par, visit, None if last else 1 - par, done)

    def store(k):
        return pltpu.make_async_copy(B.at[pl.ds(k * CP + 1, CP), pl.ds(S, W), :], out_hbm.at[pl.ds(k * CP, CP)], st.at[k])

    def start_level0():
        @pl.loop(0, NC)
        def _(c):
            k = chunk_of(c)
            load(0, k).wait()

            @pl.loop(0, CP // S)
            def _(t):
                turn(0, k * CP + t * S, S)
            first_chunk(0, c)
            send(0, k)

    def residual_pass():
        def visit(i, r, centre, total):
            BT[block(i, r, RB), :] = F[i, pl.ds(r, RB), :] - 6.0 * centre + total
        stencil_pass(0, visit, None, None)
        zero_turned(BT, (-1,))

    def restrict_planes(i, weights, dst, dst_plane):
        acc = None
        for di, w in weights:
            lo, mid, hi = (BT[pl.ds((i + di) * PR + S + d, 64, stride=2), :] for d in (-1, 0, 1))
            tail = BT[pl.ds((i + di) * PR + S + LAST, 1), :]
            pair = (lo + hi) + 2.0 * mid, tail
            pair = tuple(x if w == 1 else x * w for x in pair)
            acc = pair if acc is None else tuple(x + y for x, y in zip(acc, pair))
        dst[pl.ds(pl.multiple_of(dst_plane * XR, S), 64), :] = acc[0]
        dst[pl.ds(dst_plane * XR + 64, 1), :] = acc[1]

    def restrict_rows():
        restrict_planes(0, ((0, 2.0), (1, 1)), X2, 64 * cx)

        @pl.loop(1, 64)
        def _(i):
            restrict_planes(2 * i, ((-1, 1), (0, 2.0), (1, 1)), X2, i + 64 * cx)
        restrict_planes(LAST, ((0, 1),), XP, 0)

    def gather_chip():
        own = pl.ds(64 * cx, 64)
        cpx = [pltpu.make_async_remote_copy(src_ref=X.at[own], dst_ref=X.at[own], send_sem=cs.at[0], recv_sem=cr.at[0],
                                            device_id=px, device_id_type=MESH),
               pltpu.make_async_remote_copy(src_ref=XP, dst_ref=RXP, send_sem=cs.at[1], recv_sem=cr.at[1],
                                            device_id=px, device_id_type=MESH)]
        for cp in cpx:
            cp.start()
        zero_rows(AT, 3 * L1.rows)
        for cp in cpx:
            cp.wait()
        for t in range(9):
            r = eight(t * S)
            X2[eight(64 * XR + t * S), :] += jnp.where(cx == 0, XP[r, :], RXP[r, :])

    def to_level1():
        @pl.loop(0, 13)
        def _(jo):
          for q in range(5):
            jc = jo * 5 + q
            TS[q, pl.ds(S, W), :] = jnp.transpose(X2[pl.ds(jc, W, stride=XR), :])
            base = (jc + L1.pj) * L1.nk + L1.kp
            lo, mid, hi = (TS[q, pl.ds(S + d, 64, stride=2), :] for d in (-1, 0, 1))
            G1[pl.ds(pl.multiple_of(base, S), 64), :] = ((lo + hi) + 2.0 * mid) * F32(1 / 16)
            G1[pl.ds(base + 64, 1), :] = TS[q, pl.ds(135, 1), :] * F32(1 / 16)

    def wide_exchange(L, G, RYl, SZl, RZl, s):
        cnt = L.h + 1
        js = (L.n - L.h) * (1 - cy)
        cp = pltpu.make_async_remote_copy(
            src_ref=G.at[pl.ds(pl.multiple_of((js + L.pj) * L.nk, S), cnt * L.nk), :], dst_ref=RYl,
            send_sem=cs.at[s], recv_sem=cr.at[s], device_id=py, device_id_type=MESH)
        cp.start()
        cp.wait()
        jd = (L.n * (1 - cy) - L.h * cy + L.pj) * L.nk

        @pl.loop(0, cnt)
        def _(p):
            r = pl.multiple_of(p * L.nk, S)
            G[pl.ds(pl.multiple_of(jd + r, S), L.nk), :] += RYl[pl.ds(r, L.nk), :]
        ks = (L.n - L.h) * (1 - cz) + L.kp
        kd = L.n * (1 - cz) - L.h * cz + L.kp
        jl = L.pj - L.h * cy

        @pl.loop(0, L.n + L.h)
        def _(p):
            SZl[pl.ds(p * cnt, cnt), :] = G[pl.ds((jl + p) * L.nk + ks, cnt), :]
        cp = pltpu.make_async_remote_copy(src_ref=SZl, dst_ref=RZl, send_sem=cs.at[s + 1], recv_sem=cr.at[s + 1],
                                          device_id=pz, device_id_type=MESH)
        cp.start()
        cp.wait()

        @pl.loop(0, L.n + L.h)
        def _(p):
            G[pl.ds((jl + p) * L.nk + kd, cnt), :] += RZl[pl.ds(p * cnt, cnt), :]
            G[pl.ds((jl + p) * L.nk + L.kp - 1 + (L.n + 1) * cz, 1), :] = zero[:1]
        G[pl.ds(pl.multiple_of((L.pj - 1 + (L.n + 1) * cy) * L.nk, S), L.nk), :] = jnp.zeros((L.nk, W), F32)

    def coarse_sum(L, src, r, count):
        lanes = lax.broadcasted_iota(jnp.int32, (count, W), 1)
        c = src[pl.ds(r, count), :]
        left = jnp.where(lanes == 0, 0.0, pltpu.roll(c, 1, 1))
        right = jnp.where(lanes == L.ni - 1, 0.0, pltpu.roll(c, LAST, 1))
        total = (src[pl.ds(r - L.nk, count), :] + src[pl.ds(r + L.nk, count), :]) + (
            src[pl.ds(r - 1, count), :] + src[pl.ds(r + 1, count), :]) + (left + right)
        return c, total

    def coarse_pass(L, src, visit):
        j0 = L.pj - (L.region - L.n) * cy
        k0 = L.kp - L.hb * cz
        count = L.n + L.hb

        @pl.loop(0, L.region // L.unroll)
        def _(po):
            for p in range(L.unroll):
                r = pl.multiple_of((j0 + po * L.unroll + p) * L.nk + k0, S)
                visit(pl.ds(r, count), *coarse_sum(L, src, r, count))

    def first_two(L, G, V):
        def visit(rows, c, total):
            V[rows, :] = (12.0 * c + total) * F32(1 / 81)
        coarse_pass(L, G, visit)

    def smooth(L, G, V, W_):
        def visit(rows, c, total):
            W_[rows, :] = (3.0 * c + (total + G[rows, :])) * ninth
        coarse_pass(L, V, visit)

    def weights(ni, up):
        a = lax.broadcasted_iota(jnp.int32, (W, W), 0)
        b = lax.broadcasted_iota(jnp.int32, (W, W), 1)
        if up:
            fine, coarse = b, a
            w = jnp.where(fine == 2 * coarse, 1.0, 0.0) + jnp.where(
                (fine == 2 * coarse + 1) | (fine == 2 * coarse - 1), 0.5, 0.0)
        else:
            fine, coarse = a, b
            w = jnp.where(fine == 2 * coarse, 2.0, 0.0) + jnp.where(
                (fine == 2 * coarse + 1) | (fine == 2 * coarse - 1), 1.0, 0.0)
        return jnp.where((coarse < ni) & (fine < 2 * ni), w, 0.0).astype(F32)

    def restrict_coarse(L, M, G, V, W_, Gc):
        @pl.loop(0, L.n // 4)
        def _(po):
            for p in range(4):
                r = pl.multiple_of((L.pj + po * 4 + p) * L.nk + L.kp, S)
                c, total = coarse_sum(L, V, r, L.n)
                W_[pl.ds(r, L.n), :] = G[pl.ds(r, L.n), :] - 6.0 * c + total
        for side in (L.pj - 1, L.pj + L.n, L.pj + L.n + 1):
            W_[pl.ds(side * L.nk, L.nk), :] = jnp.zeros((L.nk, W), F32)

        @pl.loop(0, L.n)
        def _(p):
            base = (L.pj + p) * L.nk + L.kp
            W_[eight(pl.multiple_of(base - S, S)), :] = zero
            W_[eight(pl.multiple_of(base + L.n, S)), :] = zero
        w = weights(M.ni, False)

        @pl.loop(0, M.n + 1)
        def _(p):
            base = (L.pj + 2 * p) * L.nk + L.kp
            rows = M.n + 4
            sums = []
            for dj in (-1, 0, 1):
                lo, mid, hi = (W_[pl.ds(base + dj * L.nk + d, rows, stride=2), :] for d in (-1, 0, 1))
                sums.append((lo + hi) + 2.0 * mid)
            T2[pl.ds(p * (M.n + S), rows), :] = (sums[0] + sums[2]) + 2.0 * sums[1]
        hr = M.n + S
        group = (M.n + 1) // (1 + 2 * (M.n // 32))

        @pl.loop(0, (M.n + 1) // group)
        def _(g):
            t0 = pl.multiple_of(g * group * hr, S)
            res = jnp.dot(T2[pl.ds(t0, group * hr), :], w, precision=HI, preferred_element_type=F32) * F32(1 / 16)
            for p in range(group):
                rb = (M.pj + g * group + p) * M.nk + M.kp
                Gc[pl.ds(pl.multiple_of(rb, S), M.n), :] = res[p * hr:p * hr + M.n]
                Gc[pl.ds(rb + M.n, 1), :] = res[p * hr + M.n:p * hr + M.n + 1]

    def prolong_coarse(L, M, V, e):
        w = weights(M.ni, True)
        extra = 3
        j0 = M.pj - extra * cy

        @pl.loop(0, (M.n + extra + 1) // M.group)
        def _(g):
            rows = pl.ds(pl.multiple_of((j0 + g * M.group) * M.nk, S), M.group * M.nk)
            E[rows, :] = jnp.dot(e[rows, :], w, precision=HI, preferred_element_type=F32)

        @pl.loop(0, M.n + extra)
        def _(p):
            jc = j0 + p - M.pj
            fb = (L.pj + 2 * jc) * L.nk + L.kp
            eb = (j0 + p) * M.nk + M.kp
            for kc, rows in ((0, M.n), (M.n * (1 - cz) - 4 * cz, 4)):
                a, b = E[pl.ds(eb + kc, rows), :], E[pl.ds(eb + kc + 1, rows), :]
                c, d = E[pl.ds(eb + M.nk + kc, rows), :], E[pl.ds(eb + M.nk + kc + 1, rows), :]
                ab = a + b
                f = fb + 2 * kc
                V[pl.ds(f, rows, stride=2), :] += a
                V[pl.ds(f + 1, rows, stride=2), :] += 0.5 * ab
                V[pl.ds(f + L.nk, rows, stride=2), :] += 0.5 * (a + c)
                V[pl.ds(f + L.nk + 1, rows, stride=2), :] += 0.25 * (ab + (c + d))

    def from_level1():
        @pl.loop(0, 13)
        def _(jo):
          for q in range(5):
            jc = jo * 5 + q
            base = (jc + L1.pj) * L1.nk + L1.kp
            a, b = V1[pl.ds(pl.multiple_of(base, S), 64), :], V1[pl.ds(base + 1, 64), :]
            TS[q, pl.ds(S, 64, stride=2), :] = a
            TS[q, pl.ds(S + 1, 64, stride=2), :] = 0.5 * (a + b)
            X2[pl.ds(jc, W, stride=XR), :] = jnp.transpose(TS[q, pl.ds(S, W), :])

    def prolong_level0():
        zero_turned(AT, (-1, W))

        def done(c):
            first_chunk(1, c)
            send(1, chunk_of(c))

        @pl.loop(0, NG)
        def _(g):
            i0 = place(g)
            turn(1, place((g + NG - 1) % NG), GP)
            for q in range(GP // 2):
                half = W // 2
                xb = (i0 // 2 + q + half * cx) * XR
                a, b = X2[pl.ds(xb, half), :], X2[pl.ds(xb + 1, half), :]
                cc, d = X2[pl.ds(xb + XR, half), :], X2[pl.ds(xb + XR + 1, half), :]
                ab = a + b
                f = (i0 + 2 * q + 1) * PR + S
                for shift, value in ((0, a), (1, 0.5 * ab), (PR, 0.5 * (a + cc)), (PR + 1, 0.25 * (ab + (cc + d)))):
                    rows = pl.ds(f + shift, half, stride=2)
                    B2[rows, :] = A2[rows, :] + value
            after_chunk(g, done)
        turn(1, place(NG - 1), GP)
        done(NC - 1)

    def smooth_coarsest():
        @pl.loop(0, 7)
        def _(s):
            smooth(L3, G3, V3, W3)
            smooth(L3, G3, W3, V3)

    start_level0()
    sweep_pass(0, True, False)
    sweep_pass(1, False, False)
    residual_pass()
    restrict_rows()
    gather_chip()
    to_level1()
    wide_exchange(L1, G1, RY1, SZ1, RZ1, 2)
    first_two(L1, G1, V1)
    restrict_coarse(L1, L2, G1, V1, W1, G2)
    wide_exchange(L2, G2, RY2, SZ2, RZ2, 4)
    first_two(L2, G2, V2)
    restrict_coarse(L2, L3, G2, V2, W2, G3)
    wide_exchange(L3, G3, RY3, SZ3, RZ3, 6)
    first_two(L3, G3, V3)
    smooth_coarsest()
    prolong_coarse(L2, L3, V2, V3)
    smooth(L2, G2, V2, W2)
    smooth(L2, G2, W2, V2)
    prolong_coarse(L1, L2, V1, V2)
    smooth(L1, G1, V1, W1)
    smooth(L1, G1, W1, V1)
    from_level1()
    prolong_level0()
    sweep_pass(1, False, False)
    sweep_pass(0, False, True)
    for k in range(NC):
        store(k).wait()


def solution(mesh):
    spec = P(('dp', 'sx'), 'sy', 'sz')

    def local(f, u):
        size = 2 * f.shape[1]
        h2 = 1.0 / float((size + 1) ** 2)
        vm = lambda *s: pltpu.VMEM(s, F32)
        scratch = [vm(130, PR, W), vm(130, PR, W), vm(N * PR, W), vm(N * PR, W), vm(N, N, W), vm(129, XR, W),
                   vm(XR, W), vm(XR, W), vm(5, 136, W), vm(GP * W, W), vm(2, N, W), vm(2, N, W), vm(2, N, W), vm(2, N, W)]
        for L in LEVS[1:]:
            scratch += [vm(L.rows, W)] * 3
        scratch += [vm(max(L2.rows, L3.rows), W), vm(33 * 40, W)]
        for L in LEVS:
            z = up8((L.n + L.h) * (L.h + 1))
            scratch += [vm((L.h + 1) * L.nk, W), vm(z, W), vm(z, W)]
        dma = pltpu.SemaphoreType.DMA
        scratch += [dma((2, NC)), dma((NC,)), dma((2,)), dma((2,)), dma((2, NC)), dma((2, NC)), dma((2, NC)), dma((2, NC)),
                    dma((S,)), dma((S,))]
        return pl.pallas_call(
            functools.partial(body, h2),
            out_shape=jax.ShapeDtypeStruct(f.shape, F32),
            in_specs=[pl.BlockSpec(memory_space=pl.ANY)] * 2,
            out_specs=pl.BlockSpec(memory_space=pl.ANY),
            scratch_shapes=scratch,
            compiler_params=pltpu.CompilerParams(collective_id=0, has_side_effects=True, vmem_limit_bytes=67043328),
        )(f, u)

    def run(rhs_grid, u_start):
        return jax.shard_map(local, mesh=mesh, in_specs=(spec, spec), out_specs=spec, check_vma=False)(rhs_grid, u_start)
    return run
```

```python
import functools
import jax
import jax.numpy as jnp
from jax import lax
from jax.experimental import pallas as pl
from jax.experimental.pallas import tpu as pltpu
from jax.sharding import PartitionSpec as P

N = 128
PR = 144
NC = 4
XR = 72
CP = N // NC
GP = 4
GC = CP // GP
NG = N // GP
RB = 32
S, W = 8, 128
LAST = W - 1
MESH = pl.DeviceIdType.MESH
F32 = jnp.float32
HI = lax.Precision.HIGHEST


class Lev:
    def __init__(self, n, h, pj, kp, hb, ni, region, unroll, group):
        self.n, self.h, self.pj, self.kp, self.hb, self.ni = n, h, pj, kp, hb, ni
        self.region, self.unroll, self.group = region, unroll, group
        self.nk = n + 2 * kp
        self.planes = n + 2 * pj
        self.rows = self.planes * self.nk


L1 = Lev(64, 4, 6, 8, 8, 128, 68, 4, 1)
L2 = Lev(32, 5, 10, 8, 8, 64, 40, 8, 12)
L3 = Lev(16, 16, 18, 16, 16, 32, 32, 8, 10)
EXTRA = 3


def up8(x):
    return (x + 7) // 8 * 8


def eight(r):
    return pl.ds(r, S)


def body(h2, f_hbm, u_hbm, out_hbm, A, B, AT, BT, F, X, XP, RXP, TS, KS, PZ, RZ, PY, RY,
         G2, V2, W2, G3, V3, W3, E, T2,
         RY1, SZ1, RZ1, RY2, SZ2, RZ2, S3, R3,
         ld, st, xs, xr, zs, zr, ys, yr, cs, cr):
    cx, cy, cz = lax.axis_index('sx'), lax.axis_index('sy'), lax.axis_index('sz')
    ninth = F32(1.0 / 9.0)
    px, py, pz = {'sx': 1 - cx}, {'sy': 1 - cy}, {'sz': 1 - cz}
    pyz = {**py, **pz}

    def flat(ref):
        return ref.reshape(ref.shape[0] * ref.shape[1], ref.shape[2])

    A2, B2, X2 = flat(A), flat(B), flat(X)
    flats, turned = (A2, B2), (AT, BT)
    G1, V1, W1 = (AT.at[pl.ds(p * L1.rows, L1.rows), :] for p in range(3))

    def chunk_of(c):
        return c * cx + (NC - 1 - c) * (1 - cx)

    def block(i, shift=0, count=W):
        if isinstance(shift, int) and shift % S == 0:
            return pl.ds(pl.multiple_of(i * PR + S + shift, S), count)
        return pl.ds(i * PR + S + shift, count)

    def load(which, k):
        planes = pl.ds(k * CP, CP)
        src, dst = ((u_hbm, A.at[pl.ds(k * CP + 1, CP), pl.ds(S, W), :]), (f_hbm, F.at[planes]))[which]
        return pltpu.make_async_copy(src.at[planes], dst, ld.at[which, k])
    for which in range(2):
        for c in range(NC):
            load(which, chunk_of(c)).start()

    barrier = pltpu.get_barrier_semaphore()
    for p in (px, py, pz, pyz):
        pl.semaphore_signal(barrier, inc=1, device_id=p, device_id_type=MESH)
    pl.semaphore_wait(barrier, 4)

    zero = jnp.zeros((S, W), F32)

    def zero_rows(ref2, count):
        @pl.loop(0, count // 64)
        def _(t):
            ref2[pl.ds(pl.multiple_of(t * 64, 64), 64), :] = jnp.zeros((64, W), F32)
        if count % 64:
            ref2[pl.ds(count // 64 * 64, count % 64), :] = jnp.zeros((count % 64, W), F32)
    for ref in (G2, V2, W2, G3, V3, W3):
        zero_rows(ref, ref.shape[0])

    for buf in flats:
        buf[block(129 * cx, -S, PR), :] = jnp.zeros((PR, W), F32)
        for side in (-1, W):
            buf[pl.ds(PR + S + side, N, stride=PR), :] = jnp.zeros((N, W), F32)

    def zero_turned(buf, sides):
        for side in sides:
            buf[pl.ds(S + side, N, stride=PR), :] = jnp.zeros((N, W), F32)
    zero_turned(AT, (-1, W))
    zero_turned(BT, (-1, W))

    @pl.loop(0, XR // S)
    def _(t):
        X[W, eight(pl.multiple_of(t * S, S)), :] = zero
    for q in range(5):
        TS[q, eight(0), :] = zero

    def x_copy(par):
        return pltpu.make_async_remote_copy(
            src_ref=flats[par].at[block(W - LAST * cx), :], dst_ref=flats[par].at[block(129 * cx), :],
            send_sem=xs.at[par], recv_sem=xr.at[par], device_id=px, device_id_type=MESH)

    def side_copy(par, k, src, dst, ssem, rsem, to):
        planes = pl.ds(pl.multiple_of(k * CP, S), CP)
        return pltpu.make_async_remote_copy(
            src_ref=src.at[par, planes, :], dst_ref=dst.at[par, planes, :],
            send_sem=ssem.at[par, k], recv_sem=rsem.at[par, k], device_id=to, device_id_type=MESH)

    def side_copies(par, k):
        return side_copy(par, k, PY, RY, ys, yr, py), side_copy(par, k, PZ, RZ, zs, zr, pz)

    def send(par, k):
        planes = pl.ds(k * CP, CP)
        PY[par, planes, :] = flats[par][pl.ds((k * CP + 1) * PR + S + LAST * (1 - cy), CP, stride=PR), :]
        PZ[par, planes, :] = turned[par][pl.ds(k * CP * PR + S + LAST * (1 - cz), CP, stride=PR), :]
        for cp in side_copies(par, k):
            cp.start()

    def receive(par, k):
        for cp in side_copies(par, k):
            cp.wait()
        planes = pl.ds(k * CP, CP)
        flats[par][pl.ds((k * CP + 1) * PR + S + W - (W + 1) * cy, CP, stride=PR), :] = RY[par, planes, :]
        turned[par][pl.ds(k * CP * PR + S + W - (W + 1) * cz, CP, stride=PR), :] = RZ[par, planes, :]

    def place(g):
        return chunk_of(g // GC) * CP + g % GC * GP

    def turn(par, i0, count):
        for q in range(count):
            turned[par][block(i0 + q), :] = jnp.transpose(flats[par][block(i0 + q + 1), :])

    def side_sums(par, i0):
        for q in range(GP):
            KS[pl.ds(q * W, W), :] = jnp.transpose(turned[par][block(i0 + q, -1), :] + turned[par][block(i0 + q, 1), :])

    def after_chunk(g, done):
        @pl.when((g % GC == 0) & (g > 0))
        def _():
            done(g // GC - 1)

    def first_chunk(par, c):
        @pl.when(c == 0)
        def _():
            x_copy(par).start()

    def stencil_pass(par, visit, dst, done):
        src = flats[par]
        x_copy(par).wait()
        receive(par, chunk_of(0))
        side_sums(par, place(0))

        @pl.loop(0, NG)
        def _(g):
            @pl.when((g % GC == GC - 1) & (g < NG - 1))
            def _():
                receive(par, chunk_of(g // GC + 1))
            i0 = place(g)
            if dst is not None:
                turn(dst, place((g + NG - 1) % NG), GP)
            for t in range(W // RB):
                r = t * RB
                um, uc = src[block(i0, r, RB), :], src[block(i0 + 1, r, RB), :]
                for q in range(GP):
                    un = src[block(i0 + q + 2, r, RB), :]
                    total = (um + un) + (src[block(i0 + q + 1, r - 1, RB), :] + src[block(i0 + q + 1, r + 1, RB), :]) + KS[
                        pl.ds(q * W + r, RB), :]
                    visit(i0 + q, r, uc, total)
                    um, uc = uc, un
            side_sums(par, place((g + 1) % NG))
            if done is not None:
                after_chunk(g, done)
        if dst is not None:
            turn(dst, place(NG - 1), GP)
        if done is not None:
            done(NC - 1)

    def sweep_pass(par, first, last):
        if first:
            for k in range(NC):
                load(1, k).wait()

        def visit(i, r, centre, total):
            fs = F[i, pl.ds(r, RB), :]
            if first:
                fs = fs * F32(h2)
                F[i, pl.ds(r, RB), :] = fs
            flats[1 - par][block(i + 1, r, RB), :] = (3.0 * centre + (total + fs)) * ninth

        def done(c):
            k = chunk_of(c)
            if last:
                store(k).start()
            else:
                first_chunk(1 - par, c)
                send(1 - par, k)
        stencil_pass(par, visit, None if last else 1 - par, done)

    def store(k):
        return pltpu.make_async_copy(B.at[pl.ds(k * CP + 1, CP), pl.ds(S, W), :], out_hbm.at[pl.ds(k * CP, CP)], st.at[k])

    def start_level0():
        @pl.loop(0, NC)
        def _(c):
            k = chunk_of(c)
            load(0, k).wait()

            @pl.loop(0, CP // S)
            def _(t):
                turn(0, k * CP + t * S, S)
            first_chunk(0, c)
            send(0, k)

    def residual_pass():
        def visit(i, r, centre, total):
            BT[block(i, r, RB), :] = F[i, pl.ds(r, RB), :] - 6.0 * centre + total
        stencil_pass(0, visit, None, None)
        zero_turned(BT, (-1,))

    def restrict_planes(i, weights, dst, dst_plane):
        acc = None
        for di, w in weights:
            lo, mid, hi = (BT[pl.ds((i + di) * PR + S + d, 64, stride=2), :] for d in (-1, 0, 1))
            tail = BT[pl.ds((i + di) * PR + S + LAST, 1), :]
            pair = (lo + hi) + 2.0 * mid, tail
            pair = tuple(x if w == 1 else x * w for x in pair)
            acc = pair if acc is None else tuple(x + y for x, y in zip(acc, pair))
        dst[pl.ds(pl.multiple_of(dst_plane * XR, S), 64), :] = acc[0]
        dst[pl.ds(dst_plane * XR + 64, 1), :] = acc[1]

    def restrict_rows():
        restrict_planes(0, ((0, 2.0), (1, 1)), X2, 64 * cx)

        @pl.loop(1, 64)
        def _(i):
            restrict_planes(2 * i, ((-1, 1), (0, 2.0), (1, 1)), X2, i + 64 * cx)
        restrict_planes(LAST, ((0, 1),), XP, 0)

    def gather_chip():
        own = pl.ds(64 * cx, 64)
        cpx = [pltpu.make_async_remote_copy(src_ref=X.at[own], dst_ref=X.at[own], send_sem=cs.at[0], recv_sem=cr.at[0],
                                            device_id=px, device_id_type=MESH),
               pltpu.make_async_remote_copy(src_ref=XP, dst_ref=RXP, send_sem=cs.at[1], recv_sem=cr.at[1],
                                            device_id=px, device_id_type=MESH)]
        for cp in cpx:
            cp.start()
        zero_rows(AT, 3 * L1.rows)
        for cp in cpx:
            cp.wait()
        for t in range(9):
            r = eight(t * S)
            X2[eight(64 * XR + t * S), :] += jnp.where(cx == 0, XP[r, :], RXP[r, :])

    def to_level1():
        @pl.loop(0, 13)
        def _(jo):
          for q in range(5):
            jc = jo * 5 + q
            TS[q, pl.ds(S, W), :] = jnp.transpose(X2[pl.ds(jc, W, stride=XR), :])
            base = (jc + L1.pj) * L1.nk + L1.kp
            lo, mid, hi = (TS[q, pl.ds(S + d, 64, stride=2), :] for d in (-1, 0, 1))
            G1[pl.ds(pl.multiple_of(base, S), 64), :] = ((lo + hi) + 2.0 * mid) * F32(1 / 16)
            G1[pl.ds(base + 64, 1), :] = TS[q, pl.ds(135, 1), :] * F32(1 / 16)

    def wide_exchange(L, G, RYl, SZl, RZl, s):
        cnt = L.h + 1
        js = (L.n - L.h) * (1 - cy)
        cp = pltpu.make_async_remote_copy(
            src_ref=G.at[pl.ds(pl.multiple_of((js + L.pj) * L.nk, S), cnt * L.nk), :], dst_ref=RYl,
            send_sem=cs.at[s], recv_sem=cr.at[s], device_id=py, device_id_type=MESH)
        cp.start()
        cp.wait()
        jd = (L.n * (1 - cy) - L.h * cy + L.pj) * L.nk

        @pl.loop(0, cnt)
        def _(p):
            r = pl.multiple_of(p * L.nk, S)
            G[pl.ds(pl.multiple_of(jd + r, S), L.nk), :] += RYl[pl.ds(r, L.nk), :]
        ks = (L.n - L.h) * (1 - cz) + L.kp
        kd = L.n * (1 - cz) - L.h * cz + L.kp
        jl = L.pj - L.h * cy

        @pl.loop(0, L.n + L.h)
        def _(p):
            SZl[pl.ds(p * cnt, cnt), :] = G[pl.ds((jl + p) * L.nk + ks, cnt), :]
        cp = pltpu.make_async_remote_copy(src_ref=SZl, dst_ref=RZl, send_sem=cs.at[s + 1], recv_sem=cr.at[s + 1],
                                          device_id=pz, device_id_type=MESH)
        cp.start()
        cp.wait()

        @pl.loop(0, L.n + L.h)
        def _(p):
            G[pl.ds((jl + p) * L.nk + kd, cnt), :] += RZl[pl.ds(p * cnt, cnt), :]
            G[pl.ds((jl + p) * L.nk + L.kp - 1 + (L.n + 1) * cz, 1), :] = zero[:1]
        G[pl.ds(pl.multiple_of((L.pj - 1 + (L.n + 1) * cy) * L.nk, S), L.nk), :] = jnp.zeros((L.nk, W), F32)

    def coarse_sum(L, src, r, count):
        lanes = lax.broadcasted_iota(jnp.int32, (count, W), 1)
        c = src[pl.ds(r, count), :]
        left = jnp.where(lanes == 0, 0.0, pltpu.roll(c, 1, 1))
        right = jnp.where(lanes == L.ni - 1, 0.0, pltpu.roll(c, LAST, 1))
        total = (src[pl.ds(r - L.nk, count), :] + src[pl.ds(r + L.nk, count), :]) + (
            src[pl.ds(r - 1, count), :] + src[pl.ds(r + 1, count), :]) + (left + right)
        return c, total

    def coarse_pass(L, src, visit):
        j0 = L.pj - (L.region - L.n) * cy
        k0 = L.kp - L.hb * cz
        count = L.n + L.hb

        @pl.loop(0, L.region // L.unroll)
        def _(po):
            for p in range(L.unroll):
                r = pl.multiple_of((j0 + po * L.unroll + p) * L.nk + k0, S)
                visit(pl.ds(r, count), *coarse_sum(L, src, r, count))

    def first_two(L, G, V):
        def visit(rows, c, total):
            V[rows, :] = (12.0 * c + total) * F32(1 / 81)
        coarse_pass(L, G, visit)

    def smooth(L, G, V, W_):
        def visit(rows, c, total):
            W_[rows, :] = (3.0 * c + (total + G[rows, :])) * ninth
        coarse_pass(L, V, visit)

    def weights(ni, up, offset=0):
        a = lax.broadcasted_iota(jnp.int32, (W, W), 0)
        b = lax.broadcasted_iota(jnp.int32, (W, W), 1)
        fine, coarse = (b, a - offset) if up else (a, b - offset)
        near = (fine == 2 * coarse + 1) | (fine == 2 * coarse - 1)
        w = jnp.where(fine == 2 * coarse, 1.0, 0.0) + jnp.where(near, 0.5, 0.0)
        return jnp.where((coarse >= 0) & (coarse < ni) & (fine < 2 * ni), w if up else 2.0 * w, 0.0).astype(F32)

    def lane_dot(x, w):
        return jnp.dot(x, w, precision=HI, preferred_element_type=F32)

    def restrict_coarse(L, M, G, V, W_):
        @pl.loop(0, L.n // 4)
        def _(po):
            for p in range(4):
                r = pl.multiple_of((L.pj + po * 4 + p) * L.nk + L.kp, S)
                c, total = coarse_sum(L, V, r, L.n)
                W_[pl.ds(r, L.n), :] = G[pl.ds(r, L.n), :] - 6.0 * c + total
        for side in (L.pj - 1, L.pj + L.n, L.pj + L.n + 1):
            W_[pl.ds(side * L.nk, L.nk), :] = jnp.zeros((L.nk, W), F32)

        @pl.loop(0, L.n)
        def _(p):
            base = (L.pj + p) * L.nk + L.kp
            W_[eight(pl.multiple_of(base - S, S)), :] = zero
            W_[eight(pl.multiple_of(base + L.n, S)), :] = zero

        @pl.loop(0, M.n + 1)
        def _(p):
            base = (L.pj + 2 * p) * L.nk + L.kp
            rows = M.n + 4
            sums = []
            for dj in (-1, 0, 1):
                lo, mid, hi = (W_[pl.ds(base + dj * L.nk + d, rows, stride=2), :] for d in (-1, 0, 1))
                sums.append((lo + hi) + 2.0 * mid)
            T2[pl.ds(p * (M.n + S), rows), :] = (sums[0] + sums[2]) + 2.0 * sums[1]

    def restrict_lanes(M, Gc):
        hr = M.n + S
        group = 11
        w = weights(M.ni, False)

        @pl.loop(0, (M.n + 1) // group)
        def _(g):
            t0 = pl.multiple_of(g * group * hr, S)
            res = lane_dot(T2[pl.ds(t0, group * hr), :], w) * F32(1 / 16)
            for p in range(group):
                rb = (M.pj + g * group + p) * M.nk + M.kp
                Gc[pl.ds(pl.multiple_of(rb, S), M.n), :] = res[p * hr:p * hr + M.n]
                Gc[pl.ds(rb + M.n, 1), :] = res[p * hr + M.n:p * hr + M.n + 1]

    KR, KA = 48, 32

    def gather_coarsest():
        hr, cells = L3.n + S, L3.n + 1
        parts = [lane_dot(T2[pl.ds(p * S * hr, n * hr), :], weights(L3.ni, False, L3.ni * (2 * cy + p)))
                 for p, n in ((0, S), (1, S), (2, 1))]
        for p in range(S):
            x = parts[0][p * hr:p * hr + cells] + parts[1][p * hr:p * hr + cells]
            x = x + parts[2][:cells] if p == 0 else x
            S3[pl.ds(p * cells, cells), :] = x * F32(1 / 16)
        cps = [pltpu.make_async_remote_copy(src_ref=S3, dst_ref=R3.at[n], send_sem=cs.at[6 + n],
                                            recv_sem=cr.at[6 + n], device_id=to, device_id_type=MESH)
               for n, to in enumerate((py, pz, pyz))]
        for cp in cps:
            cp.start()
        for cp in cps:
            cp.wait()
        low, high = S + L3.n * cz, S + L3.n * (1 - cz)
        for p in range(S):
            rows = pl.ds(p * cells, cells)
            G3[pl.ds(p * KR + low, cells), :] += S3[rows, :] + R3[0, rows, :]
            G3[pl.ds(p * KR + high, cells), :] += R3[1, rows, :] + R3[2, rows, :]
            G3[pl.ds(p * KR + S + KA, 1), :] = zero[:1]

    def coarsest_pass(src, visit):
        lanes = lax.broadcasted_iota(jnp.int32, (KA, W), 1)
        cell = lanes % KA
        at = lambda p: pl.ds(p * KR + S, KA)
        for p in range(S):
            c = src[at(p), :]
            left = jnp.where(cell == 0, 0.0, pltpu.roll(c, 1, 1))
            right = jnp.where(cell == KA - 1, 0.0, pltpu.roll(c, LAST, 1))
            lo = src[at(p - 1), :] if p else jnp.where(lanes < KA, 0.0, pltpu.roll(src[at(S - 1), :], KA, 1))
            hi = src[at(p + 1), :] if p < S - 1 else jnp.where(lanes < W - KA, pltpu.roll(src[at(0), :], W - KA, 1), 0.0)
            total = (lo + hi) + (src[pl.ds(p * KR + S - 1, KA), :] + src[pl.ds(p * KR + S + 1, KA), :]) + (left + right)
            visit(at(p), c, total)

    def solve_coarsest():
        def first(rows, c, total):
            V3[rows, :] = (12.0 * c + total) * F32(1 / 81)
        coarsest_pass(G3, first)

        @pl.loop(0, 7)
        def _(s):
            for V, W_ in ((V3, W3), (W3, V3)):
                def visit(rows, c, total):
                    W_[rows, :] = (3.0 * c + (total + G3[rows, :])) * ninth
                coarsest_pass(V, visit)

    def spread_coarsest():
        def plane(j):
            return pl.ds(pl.multiple_of((L3.pj + j) * L3.nk + L3.kp - S, S), KA)
        E[plane(L3.n), :] = jnp.zeros((KA, W), F32)
        x = jnp.concatenate([V3[pl.ds(pl.multiple_of(p * KR + L3.n * cz, S), KA), :] for p in range(S)], axis=0)
        for q in (0, 1, 2 - 3 * cy):
            y = lane_dot(x, weights(L3.ni, True, L3.ni * (2 * cy + q)))
            for p in range(S):
                E[plane(q * S + p), :] = y[p * KA:p * KA + KA]

    def spread_lanes(M, e):
        w = weights(M.ni, True)
        j0 = M.pj - EXTRA * cy

        @pl.loop(0, (M.n + EXTRA + 1) // M.group)
        def _(g):
            rows = pl.ds(pl.multiple_of((j0 + g * M.group) * M.nk, S), M.group * M.nk)
            E[rows, :] = lane_dot(e[rows, :], w)

    def prolong_coarse(L, M, V):
        j0 = M.pj - EXTRA * cy

        @pl.loop(0, M.n + EXTRA)
        def _(p):
            jc = j0 + p - M.pj
            fb = (L.pj + 2 * jc) * L.nk + L.kp
            eb = (j0 + p) * M.nk + M.kp
            for kc, rows in ((0, M.n), (M.n * (1 - cz) - 4 * cz, 4)):
                a, b = E[pl.ds(eb + kc, rows), :], E[pl.ds(eb + kc + 1, rows), :]
                c, d = E[pl.ds(eb + M.nk + kc, rows), :], E[pl.ds(eb + M.nk + kc + 1, rows), :]
                ab = a + b
                f = fb + 2 * kc
                V[pl.ds(f, rows, stride=2), :] += a
                V[pl.ds(f + 1, rows, stride=2), :] += 0.5 * ab
                V[pl.ds(f + L.nk, rows, stride=2), :] += 0.5 * (a + c)
                V[pl.ds(f + L.nk + 1, rows, stride=2), :] += 0.25 * (ab + (c + d))

    def from_level1():
        @pl.loop(0, 13)
        def _(jo):
          for q in range(5):
            jc = jo * 5 + q
            base = (jc + L1.pj) * L1.nk + L1.kp
            a, b = V1[pl.ds(pl.multiple_of(base, S), 64), :], V1[pl.ds(base + 1, 64), :]
            TS[q, pl.ds(S, 64, stride=2), :] = a
            TS[q, pl.ds(S + 1, 64, stride=2), :] = 0.5 * (a + b)
            X2[pl.ds(jc, W, stride=XR), :] = jnp.transpose(TS[q, pl.ds(S, W), :])

    def prolong_level0():
        zero_turned(AT, (-1, W))

        def done(c):
            first_chunk(1, c)
            send(1, chunk_of(c))

        @pl.loop(0, NG)
        def _(g):
            i0 = place(g)
            turn(1, place((g + NG - 1) % NG), GP)
            for q in range(GP // 2):
                half = W // 2
                xb = (i0 // 2 + q + half * cx) * XR
                a, b = X2[pl.ds(xb, half), :], X2[pl.ds(xb + 1, half), :]
                cc, d = X2[pl.ds(xb + XR, half), :], X2[pl.ds(xb + XR + 1, half), :]
                ab = a + b
                f = (i0 + 2 * q + 1) * PR + S
                for shift, value in ((0, a), (1, 0.5 * ab), (PR, 0.5 * (a + cc)), (PR + 1, 0.25 * (ab + (cc + d)))):
                    rows = pl.ds(f + shift, half, stride=2)
                    B2[rows, :] = A2[rows, :] + value
            after_chunk(g, done)
        turn(1, place(NG - 1), GP)
        done(NC - 1)

    start_level0()
    sweep_pass(0, True, False)
    sweep_pass(1, False, False)
    residual_pass()
    restrict_rows()
    gather_chip()
    to_level1()
    wide_exchange(L1, G1, RY1, SZ1, RZ1, 2)
    first_two(L1, G1, V1)
    restrict_coarse(L1, L2, G1, V1, W1)
    restrict_lanes(L2, G2)
    wide_exchange(L2, G2, RY2, SZ2, RZ2, 4)
    first_two(L2, G2, V2)
    restrict_coarse(L2, L3, G2, V2, W2)
    gather_coarsest()
    solve_coarsest()
    spread_coarsest()
    prolong_coarse(L2, L3, V2)
    smooth(L2, G2, V2, W2)
    smooth(L2, G2, W2, V2)
    spread_lanes(L2, V2)
    prolong_coarse(L1, L2, V1)
    smooth(L1, G1, V1, W1)
    smooth(L1, G1, W1, V1)
    from_level1()
    prolong_level0()
    sweep_pass(1, False, False)
    sweep_pass(0, False, True)
    for k in range(NC):
        store(k).wait()


def solution(mesh):
    spec = P(('dp', 'sx'), 'sy', 'sz')

    def local(f, u):
        size = 2 * f.shape[1]
        h2 = 1.0 / float((size + 1) ** 2)
        vm = lambda *s: pltpu.VMEM(s, F32)
        scratch = [vm(130, PR, W), vm(130, PR, W), vm(N * PR, W), vm(N * PR, W), vm(N, N, W), vm(129, XR, W),
                   vm(XR, W), vm(XR, W), vm(5, 136, W), vm(GP * W, W), vm(2, N, W), vm(2, N, W), vm(2, N, W), vm(2, N, W)]
        scratch += [vm(L2.rows, W)] * 3 + [vm(S * 48, W)] * 3
        scratch += [vm(max(L2.rows, L3.rows), W), vm(33 * 40, W)]
        for L in (L1, L2):
            z = up8((L.n + L.h) * (L.h + 1))
            scratch += [vm((L.h + 1) * L.nk, W), vm(z, W), vm(z, W)]
        scratch += [vm(S * (L3.n + 1), W), vm(3, S * (L3.n + 1), W)]
        dma = pltpu.SemaphoreType.DMA
        scratch += [dma((2, NC)), dma((NC,)), dma((2,)), dma((2,)), dma((2, NC)), dma((2, NC)), dma((2, NC)), dma((2, NC)),
                    dma((S + 1,)), dma((S + 1,))]
        return pl.pallas_call(
            functools.partial(body, h2),
            out_shape=jax.ShapeDtypeStruct(f.shape, F32),
            in_specs=[pl.BlockSpec(memory_space=pl.ANY)] * 2,
            out_specs=pl.BlockSpec(memory_space=pl.ANY),
            scratch_shapes=scratch,
            compiler_params=pltpu.CompilerParams(collective_id=0, has_side_effects=True, vmem_limit_bytes=67043328),
        )(f, u)

    def run(rhs_grid, u_start):
        return jax.shard_map(local, mesh=mesh, in_specs=(spec, spec), out_specs=spec, check_vma=False)(rhs_grid, u_start)
    return run
```

```python
import functools
import jax
import jax.numpy as jnp
from jax import lax
from jax.experimental import pallas as pl
from jax.experimental.pallas import tpu as pltpu
from jax.sharding import PartitionSpec as P

N = 128
PR = 144
NC = 4
XR = 72
CP = N // NC
GP = 8
GC = CP // GP
NG = N // GP
RB = 32
S, W = 8, 128
LAST = W - 1
MESH = pl.DeviceIdType.MESH
F32 = jnp.float32
HI = lax.Precision.HIGHEST


class Lev:
    def __init__(self, n, h, pj, kp, hb, ni, region, unroll, group):
        self.n, self.h, self.pj, self.kp, self.hb, self.ni = n, h, pj, kp, hb, ni
        self.region, self.unroll, self.group = region, unroll, group
        self.nk = n + 2 * kp
        self.planes = n + 2 * pj
        self.rows = self.planes * self.nk


L1 = Lev(64, 4, 6, 8, 8, 128, 68, 4, 1)
L2 = Lev(32, 5, 10, 8, 8, 64, 40, 8, 12)
L3 = Lev(16, 16, 18, 16, 16, 32, 32, 8, 10)
EXTRA = 3


def up8(x):
    return (x + 7) // 8 * 8


def eight(r):
    return pl.ds(r, S)


def body(h2, f_hbm, u_hbm, out_hbm, A, B, AT, BT, F, X, XP, RXP, TS, KS, PZ, RZ, PY, RY,
         V1, W1, G2, V2, W2, G3, V3, W3,
         SY1, RY1, SZ1, RZ1, SD1, RD1, SY2, RY2, SZ2, RZ2, SD2, RD2, S3, R3,
         ld, st, xs, xr, zs, zr, ys, yr, cs, cr):
    cx, cy, cz = lax.axis_index('sx'), lax.axis_index('sy'), lax.axis_index('sz')
    ninth = F32(1.0 / 9.0)
    px, py, pz = {'sx': 1 - cx}, {'sy': 1 - cy}, {'sz': 1 - cz}
    pyz = {**py, **pz}

    def flat(ref):
        return ref.reshape(ref.shape[0] * ref.shape[1], ref.shape[2])

    A2, B2, X2 = flat(A), flat(B), flat(X)
    flats, turned = (A2, B2), (AT, BT)
    G1, T2 = AT.at[pl.ds(0, L1.rows), :], AT.at[pl.ds(L1.rows, 33 * 40), :]
    E = AT.at[pl.ds(L1.rows + 33 * 40, max(L2.rows, L3.rows)), :]

    def chunk_of(c):
        return c * cx + (NC - 1 - c) * (1 - cx)

    def block(i, shift=0, count=W):
        if isinstance(shift, int) and shift % S == 0:
            return pl.ds(pl.multiple_of(i * PR + S + shift, S), count)
        return pl.ds(i * PR + S + shift, count)

    def load(which, k):
        planes = pl.ds(k * CP, CP)
        src, dst = ((u_hbm, A.at[pl.ds(k * CP + 1, CP), pl.ds(S, W), :]), (f_hbm, F.at[planes]))[which]
        return pltpu.make_async_copy(src.at[planes], dst, ld.at[which, k])
    for which in range(2):
        for c in range(NC):
            load(which, chunk_of(c)).start()

    barrier = pltpu.get_barrier_semaphore()
    for p in (px, py, pz, pyz):
        pl.semaphore_signal(barrier, inc=1, device_id=p, device_id_type=MESH)
    pl.semaphore_wait(barrier, 4)

    zero = jnp.zeros((S, W), F32)

    def zero_rows(ref2, count):
        @pl.loop(0, count // 64)
        def _(t):
            ref2[pl.ds(pl.multiple_of(t * 64, 64), 64), :] = jnp.zeros((64, W), F32)
        if count % 64:
            ref2[pl.ds(count // 64 * 64, count % 64), :] = jnp.zeros((count % 64, W), F32)
    for ref in (V1, W1, G2, V2, W2, G3, V3, W3):
        zero_rows(ref, ref.shape[0])

    for buf in flats:
        buf[block(129 * cx, -S, PR), :] = jnp.zeros((PR, W), F32)
        for side in (-1, W):
            buf[pl.ds(PR + S + side, N, stride=PR), :] = jnp.zeros((N, W), F32)

    def zero_turned(buf, sides):
        for side in sides:
            buf[pl.ds(S + side, N, stride=PR), :] = jnp.zeros((N, W), F32)
    zero_turned(AT, (-1, W))
    zero_turned(BT, (-1, W))

    @pl.loop(0, XR // S)
    def _(t):
        X[W, eight(pl.multiple_of(t * S, S)), :] = zero
    for q in range(5):
        TS[q, eight(0), :] = zero

    def x_copy(par):
        return pltpu.make_async_remote_copy(
            src_ref=flats[par].at[block(W - LAST * cx), :], dst_ref=flats[par].at[block(129 * cx), :],
            send_sem=xs.at[par], recv_sem=xr.at[par], device_id=px, device_id_type=MESH)

    def side_copy(par, k, src, dst, ssem, rsem, to):
        planes = pl.ds(pl.multiple_of(k * CP, S), CP)
        return pltpu.make_async_remote_copy(
            src_ref=src.at[par, planes, :], dst_ref=dst.at[par, planes, :],
            send_sem=ssem.at[par, k], recv_sem=rsem.at[par, k], device_id=to, device_id_type=MESH)

    def side_copies(par, k):
        return side_copy(par, k, PY, RY, ys, yr, py), side_copy(par, k, PZ, RZ, zs, zr, pz)

    def send(par, k):
        planes = pl.ds(k * CP, CP)
        PY[par, planes, :] = flats[par][pl.ds((k * CP + 1) * PR + S + LAST * (1 - cy), CP, stride=PR), :]
        PZ[par, planes, :] = turned[par][pl.ds(k * CP * PR + S + LAST * (1 - cz), CP, stride=PR), :]
        for cp in side_copies(par, k):
            cp.start()

    def receive(par, k):
        for cp in side_copies(par, k):
            cp.wait()
        planes = pl.ds(k * CP, CP)
        flats[par][pl.ds((k * CP + 1) * PR + S + W - (W + 1) * cy, CP, stride=PR), :] = RY[par, planes, :]
        turned[par][pl.ds(k * CP * PR + S + W - (W + 1) * cz, CP, stride=PR), :] = RZ[par, planes, :]

    def place(g):
        return chunk_of(g // GC) * CP + g % GC * GP

    def turn(par, i0, count):
        for q in range(count):
            turned[par][block(i0 + q), :] = jnp.transpose(flats[par][block(i0 + q + 1), :])

    def side_sums(par, i0):
        for q in range(GP):
            KS[pl.ds(q * W, W), :] = jnp.transpose(turned[par][block(i0 + q, -1), :] + turned[par][block(i0 + q, 1), :])

    def after_chunk(g, done):
        @pl.when((g % GC == 0) & (g > 0))
        def _():
            done(g // GC - 1)

    def first_chunk(par, c):
        @pl.when(c == 0)
        def _():
            x_copy(par).start()

    def stencil_pass(par, visit, dst, done):
        src = flats[par]
        x_copy(par).wait()
        receive(par, chunk_of(0))
        side_sums(par, place(0))

        @pl.loop(0, NG)
        def _(g):
            @pl.when((g % GC == GC - 1) & (g < NG - 1))
            def _():
                receive(par, chunk_of(g // GC + 1))
            i0 = place(g)
            if dst is not None:
                turn(dst, place((g + NG - 1) % NG), GP)
            for t in range(W // RB):
                r = t * RB
                um, uc = src[block(i0, r, RB), :], src[block(i0 + 1, r, RB), :]
                for q in range(GP):
                    un = src[block(i0 + q + 2, r, RB), :]
                    total = (um + un) + (src[block(i0 + q + 1, r - 1, RB), :] + src[block(i0 + q + 1, r + 1, RB), :]) + KS[
                        pl.ds(q * W + r, RB), :]
                    visit(i0 + q, r, uc, total)
                    um, uc = uc, un
            side_sums(par, place((g + 1) % NG))
            if done is not None:
                after_chunk(g, done)
        if dst is not None:
            turn(dst, place(NG - 1), GP)
        if done is not None:
            done(NC - 1)

    def sweep_pass(par, first, last):
        if first:
            for k in range(NC):
                load(1, k).wait()

        def visit(i, r, centre, total):
            fs = F[i, pl.ds(r, RB), :]
            if first:
                fs = fs * F32(h2)
                F[i, pl.ds(r, RB), :] = fs
            flats[1 - par][block(i + 1, r, RB), :] = (3.0 * centre + (total + fs)) * ninth

        def done(c):
            k = chunk_of(c)
            if last:
                store(k).start()
            else:
                first_chunk(1 - par, c)
                send(1 - par, k)
        stencil_pass(par, visit, None if last else 1 - par, done)

    def store(k):
        return pltpu.make_async_copy(B.at[pl.ds(k * CP + 1, CP), pl.ds(S, W), :], out_hbm.at[pl.ds(k * CP, CP)], st.at[k])

    def start_level0():
        @pl.loop(0, NC)
        def _(c):
            k = chunk_of(c)
            load(0, k).wait()

            @pl.loop(0, CP // S)
            def _(t):
                turn(0, k * CP + t * S, S)
            first_chunk(0, c)
            send(0, k)

    def residual_pass():
        def visit(i, r, centre, total):
            BT[block(i, r, RB), :] = F[i, pl.ds(r, RB), :] - 6.0 * centre + total
        stencil_pass(0, visit, None, None)
        zero_turned(BT, (-1,))

    def restrict_planes(i, weights, dst, dst_plane, jc, count):
        acc = None
        for di, w in weights:
            base = (i + di) * PR + S + 2 * jc
            lo, mid, hi = (BT[pl.ds(base + d, count, stride=2), :] for d in (-1, 0, 1))
            tail = BT[pl.ds(base - 1, 1), :]
            pair = (lo + hi) + 2.0 * mid if count > 1 else tail
            pair = pair if w == 1 else pair * w
            acc = pair if acc is None else acc + pair
        dst[pl.ds(dst_plane * XR + jc, count), :] = acc

    def restrict_rows(jc, count):
        restrict_planes(0, ((0, 2.0), (1, 1)), X2, 64 * cx, jc, count)

        @pl.loop(1, 64)
        def _(i):
            restrict_planes(2 * i, ((-1, 1), (0, 2.0), (1, 1)), X2, i + 64 * cx, jc, count)

    JP = (24, 24, 16)

    def to_level1():
        spans = []
        for m, count in enumerate(JP):
            jc = sum(JP[:m])
            pieces = ((jc, count),) if m < 2 else ((jc, count), (jc + count, 1))
            spans.append((jc, pieces))
        for jc, pieces in spans:
            for piece in pieces:
                restrict_planes(LAST, ((0, 1),), XP, 0, *piece)
        own = pl.ds(64 * cx, 64)
        whole = [pltpu.make_async_remote_copy(src_ref=XP, dst_ref=RXP, send_sem=cs.at[3], recv_sem=cr.at[3],
                                              device_id=px, device_id_type=MESH)]
        whole[0].start()
        for m, (jc, pieces) in enumerate(spans):
            for piece in pieces:
                restrict_rows(*piece)
            part = X.at[own, pl.ds(jc, JP[0]), :]
            whole.append(pltpu.make_async_remote_copy(src_ref=part, dst_ref=part, send_sem=cs.at[m], recv_sem=cr.at[m],
                                                      device_id=px, device_id_type=MESH))
            whole[-1].start()
        zero_rows(AT, L1.rows)
        whole[0].wait()

        def tile(jc, q):
            TS[q, pl.ds(S, W), :] = jnp.transpose(X2[pl.ds(jc, W, stride=XR), :])
            base = (jc + L1.pj) * L1.nk + L1.kp
            lo, mid, hi = (TS[q, pl.ds(S + d, 64, stride=2), :] for d in (-1, 0, 1))
            G1[pl.ds(pl.multiple_of(base, S), 64), :] = ((lo + hi) + 2.0 * mid) * F32(1 / 16)
            G1[pl.ds(base + 64, 1), :] = TS[q, pl.ds(135, 1), :] * F32(1 / 16)

        for m, (jc, pieces) in enumerate(spans):
            whole[m + 1].wait()
            rows = pl.ds(jc, JP[0])
            X2[pl.ds(64 * XR + jc, JP[0]), :] += jnp.where(cx == 0, XP[rows, :], RXP[rows, :])

            @pl.loop(0, JP[m] // 4)
            def _(jo):
                for q in range(4):
                    tile(jc + jo * 4 + q, q)
        tile(64, 4)

    def wide_exchange(L, G, SY, RY_, SZ, RZ_, SD, RD, s):
        cnt, wide = L.h, L.n + S
        js, ks = (L.n + 1 - cnt) * (1 - cy) + L.pj, (L.n + 1 - cnt) * (1 - cz) + L.kp
        jd, kd = L.n * (1 - cy) + (1 - cnt) * cy + L.pj, L.n * (1 - cz) + (1 - cnt) * cz + L.kp
        for p in range(cnt):
            SY[pl.ds(p * wide, wide), :] = G[pl.ds(pl.multiple_of((js + p) * L.nk + L.kp, S), wide), :]
            SD[pl.ds(p * S, cnt), :] = G[pl.ds((js + p) * L.nk + ks, cnt), :]
        cps = [pltpu.make_async_remote_copy(src_ref=src, dst_ref=dst, send_sem=cs.at[s + n], recv_sem=cr.at[s + n],
                                            device_id=to, device_id_type=MESH)
               for n, (src, dst, to) in enumerate(((SY, RY_, py), (SD, RD, pyz), (SZ, RZ_, pz)))]
        cps[0].start()
        cps[1].start()

        @pl.loop(0, L.n + 1)
        def _(p):
            SZ[pl.ds(p * cnt, cnt), :] = G[pl.ds((L.pj + p) * L.nk + ks, cnt), :]
        cps[2].start()
        for cp in cps:
            cp.wait()
        for p in range(cnt):
            G[pl.ds(pl.multiple_of((jd + p) * L.nk + L.kp, S), wide), :] += RY_[pl.ds(p * wide, wide), :]
            G[pl.ds((jd + p) * L.nk + kd, cnt), :] += RD[pl.ds(p * S, cnt), :]

        @pl.loop(0, L.n + 1)
        def _(p):
            G[pl.ds((L.pj + p) * L.nk + kd, cnt), :] += RZ_[pl.ds(p * cnt, cnt), :]
        last = L.kp - 1 + (L.n + 1) * cz

        @pl.loop(0, L.region)
        def _(p):
            G[pl.ds((L.pj - (L.region - L.n) * cy + p) * L.nk + last, 1), :] = zero[:1]
        G[pl.ds(pl.multiple_of((L.pj - 1 + (L.n + 1) * cy) * L.nk, S), L.nk), :] = jnp.zeros((L.nk, W), F32)

    def coarse_pass(L, src, visit, own=False):
        j0 = L.pj if own else L.pj - (L.region - L.n) * cy
        k0 = L.kp if own else L.kp - L.hb * cz
        count = L.n if own else L.n + L.hb
        groups = (L.n if own else L.region) // L.unroll
        lanes = lax.broadcasted_iota(jnp.int32, (count, W), 1)

        def place(g, p):
            return pl.multiple_of((j0 + g * L.unroll + p) * L.nk + k0, S)

        def sides(g):
            out = []
            for p in range(L.unroll):
                c = src[pl.ds(place(g, p), count), :]
                out.append(jnp.where(lanes == 0, 0.0, pltpu.roll(c, 1, 1)) + jnp.where(
                    lanes == L.ni - 1, 0.0, pltpu.roll(c, LAST, 1)))
            return out

        def keep(sums):
            for p in range(L.unroll):
                KS[pl.ds(p * count, count), :] = sums[p]
        keep(sides(0))

        @pl.loop(0, groups)
        def _(g):
            later = sides((g + 1) % groups)
            for p in range(L.unroll):
                r = place(g, p)
                total = (src[pl.ds(r - L.nk, count), :] + src[pl.ds(r + L.nk, count), :]) + (
                    src[pl.ds(r - 1, count), :] + src[pl.ds(r + 1, count), :]) + KS[pl.ds(p * count, count), :]
                visit(pl.ds(r, count), src[pl.ds(r, count), :], total)
            keep(later)

    def first_two(L, G, V):
        def visit(rows, c, total):
            V[rows, :] = (12.0 * c + total) * F32(1 / 81)
        coarse_pass(L, G, visit)

    def smooth(L, G, V, W_):
        def visit(rows, c, total):
            W_[rows, :] = (3.0 * c + (total + G[rows, :])) * ninth
        coarse_pass(L, V, visit)

    def weights(ni, up, offset=0):
        a = lax.broadcasted_iota(jnp.int32, (W, W), 0)
        b = lax.broadcasted_iota(jnp.int32, (W, W), 1)
        fine, coarse = (b, a - offset) if up else (a, b - offset)
        near = (fine == 2 * coarse + 1) | (fine == 2 * coarse - 1)
        w = jnp.where(fine == 2 * coarse, 1.0, 0.0) + jnp.where(near, 0.5, 0.0)
        return jnp.where((coarse >= 0) & (coarse < ni) & (fine < 2 * ni), w if up else 2.0 * w, 0.0).astype(F32)

    def lane_dot(x, w):
        return jnp.dot(x, w, precision=HI, preferred_element_type=F32)

    def restrict_coarse(L, M, G, V, W_):
        def visit(rows, c, total):
            W_[rows, :] = G[rows, :] - 6.0 * c + total
        coarse_pass(L, V, visit, True)
        for side in (L.pj - 1, L.pj + L.n, L.pj + L.n + 1):
            W_[pl.ds(side * L.nk, L.nk), :] = jnp.zeros((L.nk, W), F32)

        @pl.loop(0, L.n)
        def _(p):
            base = (L.pj + p) * L.nk + L.kp
            W_[eight(pl.multiple_of(base - S, S)), :] = zero
            W_[eight(pl.multiple_of(base + L.n, S)), :] = zero

        @pl.loop(0, M.n + 1)
        def _(p):
            base = (L.pj + 2 * p) * L.nk + L.kp
            rows = M.n + 4
            sums = []
            for dj in (-1, 0, 1):
                lo, mid, hi = (W_[pl.ds(base + dj * L.nk + d, rows, stride=2), :] for d in (-1, 0, 1))
                sums.append((lo + hi) + 2.0 * mid)
            T2[pl.ds(p * (M.n + S), rows), :] = (sums[0] + sums[2]) + 2.0 * sums[1]

    def restrict_lanes(M, Gc):
        hr = M.n + S
        group = 11
        w = weights(M.ni, False)

        @pl.loop(0, (M.n + 1) // group)
        def _(g):
            t0 = pl.multiple_of(g * group * hr, S)
            res = lane_dot(T2[pl.ds(t0, group * hr), :], w) * F32(1 / 16)
            for p in range(group):
                rb = (M.pj + g * group + p) * M.nk + M.kp
                Gc[pl.ds(pl.multiple_of(rb, S), M.n), :] = res[p * hr:p * hr + M.n]
                Gc[pl.ds(rb + M.n, 1), :] = res[p * hr + M.n:p * hr + M.n + 1]

    KR, KA = 48, 32

    def gather_coarsest():
        hr, cells = L3.n + S, L3.n + 1
        parts = [lane_dot(T2[pl.ds(p * S * hr, n * hr), :], weights(L3.ni, False, L3.ni * (2 * cy + p)))
                 for p, n in ((0, S), (1, S), (2, 1))]
        for p in range(S):
            x = parts[0][p * hr:p * hr + cells] + parts[1][p * hr:p * hr + cells]
            x = x + parts[2][:cells] if p == 0 else x
            S3[pl.ds(p * cells, cells), :] = x * F32(1 / 16)
        cps = [pltpu.make_async_remote_copy(src_ref=S3, dst_ref=R3.at[n], send_sem=cs.at[10 + n],
                                            recv_sem=cr.at[10 + n], device_id=to, device_id_type=MESH)
               for n, to in enumerate((py, pz, pyz))]
        for cp in cps:
            cp.start()
        for cp in cps:
            cp.wait()
        low, high = S + L3.n * cz, S + L3.n * (1 - cz)
        for p in range(S):
            rows = pl.ds(p * cells, cells)
            G3[pl.ds(p * KR + low, cells), :] += S3[rows, :] + R3[0, rows, :]
            G3[pl.ds(p * KR + high, cells), :] += R3[1, rows, :] + R3[2, rows, :]
            G3[pl.ds(p * KR + S + KA, 1), :] = zero[:1]

    def coarsest_pass(src, visit):
        lanes = lax.broadcasted_iota(jnp.int32, (KA, W), 1)
        cell = lanes % KA
        at = lambda p: pl.ds(p * KR + S, KA)
        for p in range(S):
            c = src[at(p), :]
            left = jnp.where(cell == 0, 0.0, pltpu.roll(c, 1, 1))
            right = jnp.where(cell == KA - 1, 0.0, pltpu.roll(c, LAST, 1))
            lo = src[at(p - 1), :] if p else jnp.where(lanes < KA, 0.0, pltpu.roll(src[at(S - 1), :], KA, 1))
            hi = src[at(p + 1), :] if p < S - 1 else jnp.where(lanes < W - KA, pltpu.roll(src[at(0), :], W - KA, 1), 0.0)
            total = (lo + hi) + (src[pl.ds(p * KR + S - 1, KA), :] + src[pl.ds(p * KR + S + 1, KA), :]) + (left + right)
            visit(at(p), c, total)

    def solve_coarsest():
        def first(rows, c, total):
            V3[rows, :] = (12.0 * c + total) * F32(1 / 81)
        coarsest_pass(G3, first)

        @pl.loop(0, 7)
        def _(s):
            for V, W_ in ((V3, W3), (W3, V3)):
                def visit(rows, c, total):
                    W_[rows, :] = (3.0 * c + (total + G3[rows, :])) * ninth
                coarsest_pass(V, visit)

    def spread_coarsest():
        def plane(j):
            return pl.ds(pl.multiple_of((L3.pj + j) * L3.nk + L3.kp - S, S), KA)
        E[plane(L3.n), :] = jnp.zeros((KA, W), F32)
        x = jnp.concatenate([V3[pl.ds(pl.multiple_of(p * KR + L3.n * cz, S), KA), :] for p in range(S)], axis=0)
        for q in (0, 1, 2 - 3 * cy):
            y = lane_dot(x, weights(L3.ni, True, L3.ni * (2 * cy + q)))
            for p in range(S):
                E[plane(q * S + p), :] = y[p * KA:p * KA + KA]

    def spread_lanes(M, e):
        w = weights(M.ni, True)
        j0 = M.pj - EXTRA * cy

        @pl.loop(0, (M.n + EXTRA + 1) // M.group)
        def _(g):
            rows = pl.ds(pl.multiple_of((j0 + g * M.group) * M.nk, S), M.group * M.nk)
            E[rows, :] = lane_dot(e[rows, :], w)

    def prolong_coarse(L, M, V):
        j0 = M.pj - EXTRA * cy

        @pl.loop(0, M.n + EXTRA)
        def _(p):
            jc = j0 + p - M.pj
            fb = (L.pj + 2 * jc) * L.nk + L.kp
            eb = (j0 + p) * M.nk + M.kp
            for kc, rows in ((0, M.n), (M.n * (1 - cz) - 4 * cz, 4)):
                a, b = E[pl.ds(eb + kc, rows), :], E[pl.ds(eb + kc + 1, rows), :]
                c, d = E[pl.ds(eb + M.nk + kc, rows), :], E[pl.ds(eb + M.nk + kc + 1, rows), :]
                ab = a + b
                f = fb + 2 * kc
                V[pl.ds(f, rows, stride=2), :] += a
                V[pl.ds(f + 1, rows, stride=2), :] += 0.5 * ab
                V[pl.ds(f + L.nk, rows, stride=2), :] += 0.5 * (a + c)
                V[pl.ds(f + L.nk + 1, rows, stride=2), :] += 0.25 * (ab + (c + d))

    def from_level1():
        @pl.loop(0, 13)
        def _(jo):
          for q in range(5):
            jc = jo * 5 + q
            base = (jc + L1.pj) * L1.nk + L1.kp
            a, b = V1[pl.ds(pl.multiple_of(base, S), 64), :], V1[pl.ds(base + 1, 64), :]
            TS[q, pl.ds(S, 64, stride=2), :] = a
            TS[q, pl.ds(S + 1, 64, stride=2), :] = 0.5 * (a + b)
            X2[pl.ds(jc, W, stride=XR), :] = jnp.transpose(TS[q, pl.ds(S, W), :])

    def prolong_level0():
        zero_turned(AT, (-1, W))

        def done(c):
            first_chunk(1, c)
            send(1, chunk_of(c))

        @pl.loop(0, NG)
        def _(g):
            i0 = place(g)
            turn(1, place((g + NG - 1) % NG), GP)
            for q in range(GP // 2):
                half = W // 2
                xb = (i0 // 2 + q + half * cx) * XR
                a, b = X2[pl.ds(xb, half), :], X2[pl.ds(xb + 1, half), :]
                cc, d = X2[pl.ds(xb + XR, half), :], X2[pl.ds(xb + XR + 1, half), :]
                ab = a + b
                f = (i0 + 2 * q + 1) * PR + S
                for shift, value in ((0, a), (1, 0.5 * ab), (PR, 0.5 * (a + cc)), (PR + 1, 0.25 * (ab + (cc + d)))):
                    rows = pl.ds(f + shift, half, stride=2)
                    B2[rows, :] = A2[rows, :] + value
            after_chunk(g, done)
        turn(1, place(NG - 1), GP)
        done(NC - 1)

    start_level0()
    sweep_pass(0, True, False)
    sweep_pass(1, False, False)
    residual_pass()
    to_level1()
    wide_exchange(L1, G1, SY1, RY1, SZ1, RZ1, SD1, RD1, 4)
    first_two(L1, G1, V1)
    restrict_coarse(L1, L2, G1, V1, W1)
    restrict_lanes(L2, G2)
    wide_exchange(L2, G2, SY2, RY2, SZ2, RZ2, SD2, RD2, 7)
    first_two(L2, G2, V2)
    restrict_coarse(L2, L3, G2, V2, W2)
    gather_coarsest()
    solve_coarsest()
    spread_coarsest()
    prolong_coarse(L2, L3, V2)
    smooth(L2, G2, V2, W2)
    smooth(L2, G2, W2, V2)
    spread_lanes(L2, V2)
    prolong_coarse(L1, L2, V1)
    smooth(L1, G1, V1, W1)
    smooth(L1, G1, W1, V1)
    from_level1()
    prolong_level0()
    sweep_pass(1, False, False)
    sweep_pass(0, False, True)
    for k in range(NC):
        store(k).wait()


def solution(mesh):
    spec = P(('dp', 'sx'), 'sy', 'sz')

    def local(f, u):
        size = 2 * f.shape[1]
        h2 = 1.0 / float((size + 1) ** 2)
        vm = lambda *s: pltpu.VMEM(s, F32)
        scratch = [vm(130, PR, W), vm(130, PR, W), vm(N * PR, W), vm(N * PR, W), vm(N, N, W), vm(129, XR, W),
                   vm(XR, W), vm(XR, W), vm(5, 136, W), vm(GP * W, W), vm(2, N, W), vm(2, N, W), vm(2, N, W), vm(2, N, W)]
        scratch += [vm(L1.rows, W)] * 2 + [vm(L2.rows, W)] * 3 + [vm(S * 48, W)] * 3
        for L in (L1, L2):
            z = up8((L.n + 1) * L.h)
            scratch += [vm(L.h * (L.n + S), W)] * 2 + [vm(z, W)] * 2 + [vm(L.h * S, W)] * 2
        scratch += [vm(S * (L3.n + 1), W), vm(3, S * (L3.n + 1), W)]
        dma = pltpu.SemaphoreType.DMA
        scratch += [dma((2, NC)), dma((NC,)), dma((2,)), dma((2,)), dma((2, NC)), dma((2, NC)), dma((2, NC)), dma((2, NC)),
                    dma((13,)), dma((13,))]
        return pl.pallas_call(
            functools.partial(body, h2),
            out_shape=jax.ShapeDtypeStruct(f.shape, F32),
            in_specs=[pl.BlockSpec(memory_space=pl.ANY)] * 2,
            out_specs=pl.BlockSpec(memory_space=pl.ANY),
            scratch_shapes=scratch,
            compiler_params=pltpu.CompilerParams(collective_id=0, has_side_effects=True, vmem_limit_bytes=67043328),
        )(f, u)

    def run(rhs_grid, u_start):
        return jax.shard_map(local, mesh=mesh, in_specs=(spec, spec), out_specs=spec, check_vma=False)(rhs_grid, u_start)
    return run
```

```python
import functools
import jax
import jax.numpy as jnp
from jax import lax
from jax.experimental import pallas as pl
from jax.experimental.pallas import tpu as pltpu
from jax.sharding import PartitionSpec as P

N = 128
PR = 144
NC = 4
XR = 72
CP = N // NC
GP = 8
GC = CP // GP
NG = N // GP
RB = 32
S, W = 8, 128
LAST = W - 1
MESH = pl.DeviceIdType.MESH
F32 = jnp.float32
HI = lax.Precision.HIGHEST


class Lev:
    def __init__(self, n, h, pj, kp, hb, ni, region, unroll, group):
        self.n, self.h, self.pj, self.kp, self.hb, self.ni = n, h, pj, kp, hb, ni
        self.region, self.unroll, self.group = region, unroll, group
        self.size_own = 16
        self.nk = n + 2 * kp
        self.planes = n + 2 * pj
        self.rows = self.planes * self.nk


L1 = Lev(64, 4, 6, 8, 8, 128, 68, 17, 1)
L2 = Lev(32, 5, 10, 8, 8, 64, 40, 20, 12)
L3 = Lev(16, 16, 18, 16, 16, 32, 32, 8, 10)
EXTRA = 3


def up8(x):
    return (x + 7) // 8 * 8


def eight(r):
    return pl.ds(r, S)


def body(h2, f_hbm, u_hbm, B, A, AT, BT, F, X, XP, RXP, TS, KS, PZ, RZ, PY, RY,
         V1, W1, G2, V2, W2, G3, V3, W3,
         SY1, RY1, SZ1, RZ1, SD1, RD1, SY2, RY2, SZ2, RZ2, SD2, RD2, S3, R3,
         ld, xs, xr, zs, zr, ys, yr, cs, cr):
    cx, cy, cz = lax.axis_index('sx'), lax.axis_index('sy'), lax.axis_index('sz')
    ninth = F32(1.0 / 9.0)
    px, py, pz = {'sx': 1 - cx}, {'sy': 1 - cy}, {'sz': 1 - cz}
    pyz = {**py, **pz}

    def flat(ref):
        return ref.reshape(ref.shape[0] * ref.shape[1], ref.shape[2])

    A2, B2, X2 = flat(A), flat(B), flat(X)
    flats, turned = (A2, B2), (AT, BT)
    G1, T2 = AT.at[pl.ds(0, L1.rows), :], AT.at[pl.ds(L1.rows, 33 * 40), :]
    E = AT.at[pl.ds(L1.rows + 33 * 40, max(L2.rows, L3.rows)), :]

    def chunk_of(c):
        return c * cx + (NC - 1 - c) * (1 - cx)

    def block(i, shift=0, count=W):
        if isinstance(shift, int) and shift % S == 0:
            return pl.ds(pl.multiple_of(i * PR + S + shift, S), count)
        return pl.ds(i * PR + S + shift, count)

    def load(which, k):
        planes = pl.ds(k * CP, CP)
        src, dst = ((u_hbm, A.at[pl.ds(k * CP + 1, CP), pl.ds(S, W), :]), (f_hbm, F.at[planes]))[which]
        return pltpu.make_async_copy(src.at[planes], dst, ld.at[which, k])
    for c in range(NC):
        load(0, chunk_of(c)).start()

    barrier = pltpu.get_barrier_semaphore()
    for p in (px, py, pz, pyz):
        pl.semaphore_signal(barrier, inc=1, device_id=p, device_id_type=MESH)
    pl.semaphore_wait(barrier, 4)

    zero = jnp.zeros((S, W), F32)

    def zero_rows(ref2, count):
        @pl.loop(0, count // 64)
        def _(t):
            ref2[pl.ds(pl.multiple_of(t * 64, 64), 64), :] = jnp.zeros((64, W), F32)
        if count % 64:
            ref2[pl.ds(count // 64 * 64, count % 64), :] = jnp.zeros((count % 64, W), F32)
    for ref in (V1, W1, G2, V2, W2, G3, V3, W3):
        zero_rows(ref, ref.shape[0])

    for buf in flats:
        buf[block(129 * cx, -S, PR), :] = jnp.zeros((PR, W), F32)
        for side in (-1, W):
            buf[pl.ds(PR + S + side, N, stride=PR), :] = jnp.zeros((N, W), F32)

    def zero_turned(buf, sides):
        for side in sides:
            buf[pl.ds(S + side, N, stride=PR), :] = jnp.zeros((N, W), F32)
    zero_turned(AT, (-1, W))
    zero_turned(BT, (-1, W))

    @pl.loop(0, XR // S)
    def _(t):
        X[W, eight(pl.multiple_of(t * S, S)), :] = zero
    for q in range(5):
        TS[q, eight(0), :] = zero

    def x_copy(par):
        return pltpu.make_async_remote_copy(
            src_ref=flats[par].at[block(W - LAST * cx), :], dst_ref=flats[par].at[block(129 * cx), :],
            send_sem=xs.at[par], recv_sem=xr.at[par], device_id=px, device_id_type=MESH)

    def side_copy(par, k, src, dst, ssem, rsem, to):
        planes = pl.ds(pl.multiple_of(k * CP, S), CP)
        return pltpu.make_async_remote_copy(
            src_ref=src.at[par, planes, :], dst_ref=dst.at[par, planes, :],
            send_sem=ssem.at[par, k], recv_sem=rsem.at[par, k], device_id=to, device_id_type=MESH)

    def side_copies(par, k):
        return side_copy(par, k, PY, RY, ys, yr, py), side_copy(par, k, PZ, RZ, zs, zr, pz)

    def send(par, k):
        planes = pl.ds(k * CP, CP)
        PY[par, planes, :] = flats[par][pl.ds((k * CP + 1) * PR + S + LAST * (1 - cy), CP, stride=PR), :]
        PZ[par, planes, :] = turned[par][pl.ds(k * CP * PR + S + LAST * (1 - cz), CP, stride=PR), :]
        for cp in side_copies(par, k):
            cp.start()

    def receive(par, k):
        for cp in side_copies(par, k):
            cp.wait()
        planes = pl.ds(k * CP, CP)
        flats[par][pl.ds((k * CP + 1) * PR + S + W - (W + 1) * cy, CP, stride=PR), :] = RY[par, planes, :]
        turned[par][pl.ds(k * CP * PR + S + W - (W + 1) * cz, CP, stride=PR), :] = RZ[par, planes, :]

    def place(g):
        return chunk_of(g // GC) * CP + g % GC * GP

    def turn(par, i0, count):
        for q in range(count):
            turned[par][block(i0 + q), :] = jnp.transpose(flats[par][block(i0 + q + 1), :])

    def side_sums(par, i0):
        for q in range(GP):
            KS[pl.ds(q * W, W), :] = jnp.transpose(turned[par][block(i0 + q, -1), :] + turned[par][block(i0 + q, 1), :])

    def after_chunk(g, done):
        @pl.when((g % GC == 0) & (g > 0))
        def _():
            done(g // GC - 1)

    def first_chunk(par, c):
        @pl.when(c == 0)
        def _():
            x_copy(par).start()

    def stencil_pass(par, visit, dst, done, arrive=None):
        src = flats[par]
        x_copy(par).wait()
        receive(par, chunk_of(0))
        side_sums(par, place(0))
        if arrive is not None:
            arrive(chunk_of(0))

        @pl.loop(0, NG)
        def _(g):
            @pl.when((g % GC == GC - 1) & (g < NG - 1))
            def _():
                receive(par, chunk_of(g // GC + 1))
                if arrive is not None:
                    arrive(chunk_of(g // GC + 1))
            i0 = place(g)
            if dst is not None:
                turn(dst, place((g + NG - 1) % NG), GP)
            for t in range(W // RB):
                r = t * RB
                um, uc = src[block(i0, r, RB), :], src[block(i0 + 1, r, RB), :]
                for q in range(GP):
                    un = src[block(i0 + q + 2, r, RB), :]
                    total = (um + un) + (src[block(i0 + q + 1, r - 1, RB), :] + src[block(i0 + q + 1, r + 1, RB), :]) + KS[
                        pl.ds(q * W + r, RB), :]
                    visit(i0 + q, r, uc, total)
                    um, uc = uc, un
            side_sums(par, place((g + 1) % NG))
            if done is not None:
                after_chunk(g, done)
        if dst is not None:
            turn(dst, place(NG - 1), GP)
        if done is not None:
            done(NC - 1)

    def sweep_pass(par, first, last):
        def visit(i, r, centre, total):
            fs = F[i, pl.ds(r, RB), :]
            if first:
                fs = fs * F32(h2)
                F[i, pl.ds(r, RB), :] = fs
            flats[1 - par][block(i + 1, r, RB), :] = (3.0 * centre + (total + fs)) * ninth

        def done(c):
            k = chunk_of(c)
            first_chunk(1 - par, c)
            send(1 - par, k)
        stencil_pass(par, visit, None if last else 1 - par, None if last else done,
                     (lambda k: load(1, k).wait()) if first else None)

    def start_level0():
        @pl.loop(0, NC)
        def _(c):
            k = chunk_of(c)
            load(0, k).wait()
            load(1, k).start()

            @pl.loop(0, CP // S)
            def _(t):
                turn(0, k * CP + t * S, S)
            first_chunk(0, c)
            send(0, k)

    def residual_pass():
        def visit(i, r, centre, total):
            BT[block(i, r, RB), :] = F[i, pl.ds(r, RB), :] - 6.0 * centre + total
        stencil_pass(0, visit, None, None)
        zero_turned(BT, (-1,))

    def restrict_planes(i, weights, dst, dst_plane, jc, count):
        acc = None
        for di, w in weights:
            base = (i + di) * PR + S + 2 * jc
            lo, mid, hi = (BT[pl.ds(base + d, count, stride=2), :] for d in (-1, 0, 1))
            tail = BT[pl.ds(base - 1, 1), :]
            pair = (lo + hi) + 2.0 * mid if count > 1 else tail
            pair = pair if w == 1 else pair * w
            acc = pair if acc is None else acc + pair
        dst[pl.ds(dst_plane * XR + jc, count), :] = acc

    def restrict_rows(jc, count):
        restrict_planes(0, ((0, 2.0), (1, 1)), X2, 64 * cx, jc, count)

        @pl.loop(1, 64)
        def _(i):
            restrict_planes(2 * i, ((-1, 1), (0, 2.0), (1, 1)), X2, i + 64 * cx, jc, count)

    JP = (24, 24, 16)

    def to_level1():
        spans = []
        for m, count in enumerate(JP):
            jc = sum(JP[:m])
            pieces = ((jc, count),) if m < 2 else ((jc, count), (jc + count, 1))
            spans.append((jc, pieces))
        for jc, pieces in spans:
            for piece in pieces:
                restrict_planes(LAST, ((0, 1),), XP, 0, *piece)
        own = pl.ds(64 * cx, 64)
        whole = [pltpu.make_async_remote_copy(src_ref=XP, dst_ref=RXP, send_sem=cs.at[3], recv_sem=cr.at[3],
                                              device_id=px, device_id_type=MESH)]
        whole[0].start()
        for m, (jc, pieces) in enumerate(spans):
            for piece in pieces:
                restrict_rows(*piece)
            part = X.at[own, pl.ds(jc, JP[0]), :]
            whole.append(pltpu.make_async_remote_copy(src_ref=part, dst_ref=part, send_sem=cs.at[m], recv_sem=cr.at[m],
                                                      device_id=px, device_id_type=MESH))
            whole[-1].start()
        zero_rows(AT, L1.rows)
        whole[0].wait()

        def tile(jc, q):
            TS[q, pl.ds(S, W), :] = jnp.transpose(X2[pl.ds(jc, W, stride=XR), :])
            base = (jc + L1.pj) * L1.nk + L1.kp
            lo, mid, hi = (TS[q, pl.ds(S + d, 64, stride=2), :] for d in (-1, 0, 1))
            G1[pl.ds(pl.multiple_of(base, S), 64), :] = ((lo + hi) + 2.0 * mid) * F32(1 / 16)
            G1[pl.ds(base + 64, 1), :] = TS[q, pl.ds(135, 1), :] * F32(1 / 16)

        for m, (jc, pieces) in enumerate(spans):
            whole[m + 1].wait()
            rows = pl.ds(jc, JP[0])
            X2[pl.ds(64 * XR + jc, JP[0]), :] += jnp.where(cx == 0, XP[rows, :], RXP[rows, :])

            @pl.loop(0, JP[m] // 4)
            def _(jo):
                for q in range(4):
                    tile(jc + jo * 4 + q, q)
        tile(64, 4)

    def wide_exchange(L, G, SY, RY_, SZ, RZ_, SD, RD, s):
        cnt, wide = L.h, L.n + S
        js, ks = (L.n + 1 - cnt) * (1 - cy) + L.pj, (L.n + 1 - cnt) * (1 - cz) + L.kp
        jd, kd = L.n * (1 - cy) + (1 - cnt) * cy + L.pj, L.n * (1 - cz) + (1 - cnt) * cz + L.kp
        for p in range(cnt):
            SY[pl.ds(p * wide, wide), :] = G[pl.ds(pl.multiple_of((js + p) * L.nk + L.kp, S), wide), :]
            SD[pl.ds(p * S, cnt), :] = G[pl.ds((js + p) * L.nk + ks, cnt), :]
        cps = [pltpu.make_async_remote_copy(src_ref=src, dst_ref=dst, send_sem=cs.at[s + n], recv_sem=cr.at[s + n],
                                            device_id=to, device_id_type=MESH)
               for n, (src, dst, to) in enumerate(((SY, RY_, py), (SD, RD, pyz), (SZ, RZ_, pz)))]
        cps[0].start()
        cps[1].start()

        @pl.loop(0, L.n + 1)
        def _(p):
            SZ[pl.ds(p * cnt, cnt), :] = G[pl.ds((L.pj + p) * L.nk + ks, cnt), :]
        cps[2].start()
        for cp in cps:
            cp.wait()
        for p in range(cnt):
            G[pl.ds(pl.multiple_of((jd + p) * L.nk + L.kp, S), wide), :] += RY_[pl.ds(p * wide, wide), :]
            G[pl.ds((jd + p) * L.nk + kd, cnt), :] += RD[pl.ds(p * S, cnt), :]

        @pl.loop(0, L.n + 1)
        def _(p):
            G[pl.ds((L.pj + p) * L.nk + kd, cnt), :] += RZ_[pl.ds(p * cnt, cnt), :]
        last = L.kp - 1 + (L.n + 1) * cz

        @pl.loop(0, L.region)
        def _(p):
            G[pl.ds((L.pj - (L.region - L.n) * cy + p) * L.nk + last, 1), :] = zero[:1]
        G[pl.ds(pl.multiple_of((L.pj - 1 + (L.n + 1) * cy) * L.nk, S), L.nk), :] = jnp.zeros((L.nk, W), F32)

    def coarse_pass(L, src, visit, own=False):
        j0 = L.pj if own else L.pj - (L.region - L.n) * cy
        k0 = L.kp if own else L.kp - L.hb * cz
        count = L.n if own else L.n + L.hb
        planes = L.n if own else L.region
        size = L.size_own if own else L.unroll
        groups = planes // size
        lanes = lax.broadcasted_iota(jnp.int32, (count, W), 1)

        def place(g, p):
            return pl.multiple_of((j0 + g * size + p) * L.nk + k0, S)

        def sides(g):
            out = []
            for p in range(size):
                c = src[pl.ds(place(g, p), count), :]
                out.append(jnp.where(lanes == 0, 0.0, pltpu.roll(c, 1, 1)) + jnp.where(
                    lanes == L.ni - 1, 0.0, pltpu.roll(c, LAST, 1)))
            return out

        def keep(sums):
            for p in range(size):
                KS[pl.ds(p * count, count), :] = sums[p]
        keep(sides(0))

        @pl.loop(0, groups)
        def _(g):
            later = sides((g + 1) % groups)
            for p in range(size):
                r = place(g, p)
                total = (src[pl.ds(r - L.nk, count), :] + src[pl.ds(r + L.nk, count), :]) + (
                    src[pl.ds(r - 1, count), :] + src[pl.ds(r + 1, count), :]) + KS[pl.ds(p * count, count), :]
                visit(pl.ds(r, count), src[pl.ds(r, count), :], total)
            keep(later)

    def first_two(L, G, V):
        def visit(rows, c, total):
            V[rows, :] = (12.0 * c + total) * F32(1 / 81)
        coarse_pass(L, G, visit)

    def smooth(L, G, V, W_):
        def visit(rows, c, total):
            W_[rows, :] = (3.0 * c + (total + G[rows, :])) * ninth
        coarse_pass(L, V, visit)

    def weights(ni, up, offset=0):
        a = lax.broadcasted_iota(jnp.int32, (W, W), 0)
        b = lax.broadcasted_iota(jnp.int32, (W, W), 1)
        fine, coarse = (b, a - offset) if up else (a, b - offset)
        near = (fine == 2 * coarse + 1) | (fine == 2 * coarse - 1)
        w = jnp.where(fine == 2 * coarse, 1.0, 0.0) + jnp.where(near, 0.5, 0.0)
        return jnp.where((coarse >= 0) & (coarse < ni) & (fine < 2 * ni), w if up else 2.0 * w, 0.0).astype(F32)

    def lane_dot(x, w):
        return jnp.dot(x, w, precision=HI, preferred_element_type=F32)

    def restrict_coarse(L, M, G, V, W_):
        def visit(rows, c, total):
            W_[rows, :] = G[rows, :] - 6.0 * c + total
        coarse_pass(L, V, visit, True)
        for side in (L.pj - 1, L.pj + L.n, L.pj + L.n + 1):
            W_[pl.ds(side * L.nk, L.nk), :] = jnp.zeros((L.nk, W), F32)

        @pl.loop(0, L.n)
        def _(p):
            base = (L.pj + p) * L.nk + L.kp
            W_[eight(pl.multiple_of(base - S, S)), :] = zero
            W_[eight(pl.multiple_of(base + L.n, S)), :] = zero

        @pl.loop(0, M.n + 1)
        def _(p):
            base = (L.pj + 2 * p) * L.nk + L.kp
            rows = M.n + 4
            sums = []
            for dj in (-1, 0, 1):
                lo, mid, hi = (W_[pl.ds(base + dj * L.nk + d, rows, stride=2), :] for d in (-1, 0, 1))
                sums.append((lo + hi) + 2.0 * mid)
            T2[pl.ds(p * (M.n + S), rows), :] = (sums[0] + sums[2]) + 2.0 * sums[1]

    def restrict_lanes(M, Gc):
        hr = M.n + S
        group = 11
        w = weights(M.ni, False)

        @pl.loop(0, (M.n + 1) // group)
        def _(g):
            t0 = pl.multiple_of(g * group * hr, S)
            res = lane_dot(T2[pl.ds(t0, group * hr), :], w) * F32(1 / 16)
            for p in range(group):
                rb = (M.pj + g * group + p) * M.nk + M.kp
                Gc[pl.ds(pl.multiple_of(rb, S), M.n), :] = res[p * hr:p * hr + M.n]
                Gc[pl.ds(rb + M.n, 1), :] = res[p * hr + M.n:p * hr + M.n + 1]

    KR, KA = 48, 32

    def gather_coarsest():
        hr, cells = L3.n + S, L3.n + 1
        parts = [lane_dot(T2[pl.ds(p * S * hr, n * hr), :], weights(L3.ni, False, L3.ni * (2 * cy + p)))
                 for p, n in ((0, S), (1, S), (2, 1))]
        for p in range(S):
            x = parts[0][p * hr:p * hr + cells] + parts[1][p * hr:p * hr + cells]
            x = x + parts[2][:cells] if p == 0 else x
            S3[pl.ds(p * cells, cells), :] = x * F32(1 / 16)
        cps = [pltpu.make_async_remote_copy(src_ref=S3, dst_ref=R3.at[n], send_sem=cs.at[10 + n],
                                            recv_sem=cr.at[10 + n], device_id=to, device_id_type=MESH)
               for n, to in enumerate((py, pz, pyz))]
        for cp in cps:
            cp.start()
        for cp in cps:
            cp.wait()
        low, high = S + L3.n * cz, S + L3.n * (1 - cz)
        for p in range(S):
            rows = pl.ds(p * cells, cells)
            G3[pl.ds(p * KR + low, cells), :] += S3[rows, :] + R3[0, rows, :]
            G3[pl.ds(p * KR + high, cells), :] += R3[1, rows, :] + R3[2, rows, :]
            G3[pl.ds(p * KR + S + KA, 1), :] = zero[:1]

    def coarsest_pass(src, visit):
        lanes = lax.broadcasted_iota(jnp.int32, (KA, W), 1)
        cell = lanes % KA
        at = lambda p: pl.ds(p * KR + S, KA)
        for p in range(S):
            c = src[at(p), :]
            left = jnp.where(cell == 0, 0.0, pltpu.roll(c, 1, 1))
            right = jnp.where(cell == KA - 1, 0.0, pltpu.roll(c, LAST, 1))
            lo = src[at(p - 1), :] if p else jnp.where(lanes < KA, 0.0, pltpu.roll(src[at(S - 1), :], KA, 1))
            hi = src[at(p + 1), :] if p < S - 1 else jnp.where(lanes < W - KA, pltpu.roll(src[at(0), :], W - KA, 1), 0.0)
            total = (lo + hi) + (src[pl.ds(p * KR + S - 1, KA), :] + src[pl.ds(p * KR + S + 1, KA), :]) + (left + right)
            visit(at(p), c, total)

    def solve_coarsest():
        def first(rows, c, total):
            V3[rows, :] = (12.0 * c + total) * F32(1 / 81)
        coarsest_pass(G3, first)

        @pl.loop(0, 7)
        def _(s):
            for V, W_ in ((V3, W3), (W3, V3)):
                def visit(rows, c, total):
                    W_[rows, :] = (3.0 * c + (total + G3[rows, :])) * ninth
                coarsest_pass(V, visit)

    def spread_coarsest():
        def plane(j):
            return pl.ds(pl.multiple_of((L3.pj + j) * L3.nk + L3.kp - S, S), KA)
        E[plane(L3.n), :] = jnp.zeros((KA, W), F32)
        x = jnp.concatenate([V3[pl.ds(pl.multiple_of(p * KR + L3.n * cz, S), KA), :] for p in range(S)], axis=0)
        for q in (0, 1, 2 - 3 * cy):
            y = lane_dot(x, weights(L3.ni, True, L3.ni * (2 * cy + q)))
            for p in range(S):
                E[plane(q * S + p), :] = y[p * KA:p * KA + KA]

    def spread_lanes(M, e):
        w = weights(M.ni, True)
        j0 = M.pj - EXTRA * cy

        @pl.loop(0, (M.n + EXTRA + 1) // M.group)
        def _(g):
            rows = pl.ds(pl.multiple_of((j0 + g * M.group) * M.nk, S), M.group * M.nk)
            E[rows, :] = lane_dot(e[rows, :], w)

    def prolong_coarse(L, M, V):
        j0 = M.pj - EXTRA * cy

        @pl.loop(0, M.n + EXTRA)
        def _(p):
            jc = j0 + p - M.pj
            fb = (L.pj + 2 * jc) * L.nk + L.kp
            eb = (j0 + p) * M.nk + M.kp
            for kc, rows in ((0, M.n), (M.n * (1 - cz) - 4 * cz, 4)):
                a, b = E[pl.ds(eb + kc, rows), :], E[pl.ds(eb + kc + 1, rows), :]
                c, d = E[pl.ds(eb + M.nk + kc, rows), :], E[pl.ds(eb + M.nk + kc + 1, rows), :]
                ab = a + b
                f = fb + 2 * kc
                V[pl.ds(f, rows, stride=2), :] += a
                V[pl.ds(f + 1, rows, stride=2), :] += 0.5 * ab
                V[pl.ds(f + L.nk, rows, stride=2), :] += 0.5 * (a + c)
                V[pl.ds(f + L.nk + 1, rows, stride=2), :] += 0.25 * (ab + (c + d))

    def from_level1():
        @pl.loop(0, 13)
        def _(jo):
          for q in range(5):
            jc = jo * 5 + q
            base = (jc + L1.pj) * L1.nk + L1.kp
            a, b = V1[pl.ds(pl.multiple_of(base, S), 64), :], V1[pl.ds(base + 1, 64), :]
            TS[q, pl.ds(S, 64, stride=2), :] = a
            TS[q, pl.ds(S + 1, 64, stride=2), :] = 0.5 * (a + b)
            X2[pl.ds(jc, W, stride=XR), :] = jnp.transpose(TS[q, pl.ds(S, W), :])

    def prolong_level0():
        zero_turned(AT, (-1, W))

        def done(c):
            first_chunk(1, c)
            send(1, chunk_of(c))

        @pl.loop(0, NG)
        def _(g):
            i0 = place(g)
            turn(1, place((g + NG - 1) % NG), GP)
            for q in range(GP // 2):
                half = W // 2
                xb = (i0 // 2 + q + half * cx) * XR
                a, b = X2[pl.ds(xb, half), :], X2[pl.ds(xb + 1, half), :]
                cc, d = X2[pl.ds(xb + XR, half), :], X2[pl.ds(xb + XR + 1, half), :]
                ab = a + b
                f = (i0 + 2 * q + 1) * PR + S
                for shift, value in ((0, a), (1, 0.5 * ab), (PR, 0.5 * (a + cc)), (PR + 1, 0.25 * (ab + (cc + d)))):
                    rows = pl.ds(f + shift, half, stride=2)
                    B2[rows, :] = A2[rows, :] + value
            after_chunk(g, done)
        turn(1, place(NG - 1), GP)
        done(NC - 1)

    start_level0()
    sweep_pass(0, True, False)
    sweep_pass(1, False, False)
    residual_pass()
    to_level1()
    wide_exchange(L1, G1, SY1, RY1, SZ1, RZ1, SD1, RD1, 4)
    first_two(L1, G1, V1)
    restrict_coarse(L1, L2, G1, V1, W1)
    restrict_lanes(L2, G2)
    wide_exchange(L2, G2, SY2, RY2, SZ2, RZ2, SD2, RD2, 7)
    first_two(L2, G2, V2)
    restrict_coarse(L2, L3, G2, V2, W2)
    gather_coarsest()
    solve_coarsest()
    spread_coarsest()
    prolong_coarse(L2, L3, V2)
    smooth(L2, G2, V2, W2)
    smooth(L2, G2, W2, V2)
    spread_lanes(L2, V2)
    prolong_coarse(L1, L2, V1)
    smooth(L1, G1, V1, W1)
    smooth(L1, G1, W1, V1)
    from_level1()
    prolong_level0()
    sweep_pass(1, False, False)
    sweep_pass(0, False, True)


def solution(mesh):
    spec = P(('dp', 'sx'), 'sy', 'sz')

    def local(f, u):
        size = 2 * f.shape[1]
        h2 = 1.0 / float((size + 1) ** 2)
        vm = lambda *s: pltpu.VMEM(s, F32)
        scratch = [vm(130, PR, W), vm(N * PR, W), vm(N * PR, W), vm(N, N, W), vm(129, XR, W),
                   vm(XR, W), vm(XR, W), vm(5, 136, W), vm(17 * 72, W), vm(2, N, W), vm(2, N, W), vm(2, N, W), vm(2, N, W)]
        scratch += [vm(L1.rows, W)] * 2 + [vm(L2.rows, W)] * 3 + [vm(S * 48, W)] * 3
        for L in (L1, L2):
            z = up8((L.n + 1) * L.h)
            scratch += [vm(L.h * (L.n + S), W)] * 2 + [vm(z, W)] * 2 + [vm(L.h * S, W)] * 2
        scratch += [vm(S * (L3.n + 1), W), vm(3, S * (L3.n + 1), W)]
        dma = pltpu.SemaphoreType.DMA
        scratch += [dma((2, NC)), dma((2,)), dma((2,)), dma((2, NC)), dma((2, NC)), dma((2, NC)), dma((2, NC)),
                    dma((13,)), dma((13,))]
        out = pl.pallas_call(
            functools.partial(body, h2),
            out_shape=vm(130, PR, W),
            in_specs=[pl.BlockSpec(memory_space=pl.ANY)] * 2,
            out_specs=pl.BlockSpec(memory_space=pltpu.VMEM),
            scratch_shapes=scratch,
            compiler_params=pltpu.CompilerParams(collective_id=0, has_side_effects=True, vmem_limit_bytes=67043328 - 130 * PR * W * 4),
        )(f, u)
        return out[1:N + 1, S:S + W]

    def run(rhs_grid, u_start):
        return jax.shard_map(local, mesh=mesh, in_specs=(spec, spec), out_specs=spec, check_vma=False)(rhs_grid, u_start)
    return run
```

```python
import functools
import math
import jax
import jax.numpy as jnp
from jax import lax
from jax.experimental import pallas as pl
from jax.experimental.pallas import tpu as pltpu
from jax.sharding import PartitionSpec as P

N = 128
PR = 144
NC = 4
XR = 72
CP = N // NC
GP = 8
GC = CP // GP
NG = N // GP
RB = 32
S, W = 8, 128
LAST = W - 1
MESH = pl.DeviceIdType.MESH
F32 = jnp.float32
HI = lax.Precision.HIGHEST


class Lev:
    def __init__(self, n, h, pj, kp, hb, ni, region, unroll, group):
        self.n, self.h, self.pj, self.kp, self.hb, self.ni = n, h, pj, kp, hb, ni
        self.region, self.unroll, self.group = region, unroll, group
        self.size_own = 16
        self.nk = n + 2 * kp
        self.planes = n + 2 * pj
        self.rows = self.planes * self.nk


L1 = Lev(64, 4, 6, 8, 8, 128, 68, 17, 1)
L2 = Lev(32, 5, 10, 8, 8, 64, 40, 20, 12)
L3 = Lev(16, 16, 18, 16, 16, 32, 32, 8, 10)
EXTRA = 3


def up8(x):
    return (x + 7) // 8 * 8


def eight(r):
    return pl.ds(r, S)


def body(h2, f_hbm, u_hbm, B, A, AT, F, BT, X, XP, RXP, TS, KS, PZ, RZ, PY, RY,
         V1, W1, G2, V2, W2, G3, V3, W3,
         SY1, RY1, SZ1, RZ1, SD1, RD1, SY2, RY2, SZ2, RZ2, SD2, RD2, S3, R3,
         ld, xs, xr, zs, zr, ys, yr, cs, cr):
    cx, cy, cz = lax.axis_index('sx'), lax.axis_index('sy'), lax.axis_index('sz')
    ninth = F32(1.0 / 9.0)
    px, py, pz = {'sx': 1 - cx}, {'sy': 1 - cy}, {'sz': 1 - cz}
    pyz = {**py, **pz}

    def flat(ref):
        return ref.reshape(ref.shape[0] * ref.shape[1], ref.shape[2])

    A2, B2, X2 = flat(A), flat(B), flat(X)
    flats, turned = (A2, B2), (AT, BT)
    G1, T2 = AT.at[pl.ds(0, L1.rows), :], AT.at[pl.ds(L1.rows, 33 * 40), :]
    E = AT.at[pl.ds(L1.rows + 33 * 40, max(L2.rows, L3.rows)), :]

    def chunk_of(c):
        return c * cx + (NC - 1 - c) * (1 - cx)

    def block(i, shift=0, count=W):
        if isinstance(shift, int) and shift % S == 0:
            return pl.ds(pl.multiple_of(i * PR + S + shift, S), count)
        return pl.ds(i * PR + S + shift, count)

    def load(which, k):
        planes = pl.ds(k * CP, CP)
        src, dst = ((u_hbm, A.at[pl.ds(k * CP + 1, CP), pl.ds(S, W), :]), (f_hbm, F.at[planes]))[which]
        return pltpu.make_async_copy(src.at[planes], dst, ld.at[which, k])
    for c in range(NC):
        load(0, chunk_of(c)).start()

    barrier = pltpu.get_barrier_semaphore()
    for p in (px, py, pz, pyz):
        pl.semaphore_signal(barrier, inc=1, device_id=p, device_id_type=MESH)
    pl.semaphore_wait(barrier, 4)

    zero = jnp.zeros((S, W), F32)

    def zero_rows(ref2, count):
        @pl.loop(0, count // 64)
        def _(t):
            ref2[pl.ds(pl.multiple_of(t * 64, 64), 64), :] = jnp.zeros((64, W), F32)
        if count % 64:
            ref2[pl.ds(count // 64 * 64, count % 64), :] = jnp.zeros((count % 64, W), F32)
    for ref in (V1, W1, G2, V2, W2, G3, V3, W3):
        zero_rows(ref, ref.shape[0])

    for buf in flats:
        buf[block(129 * cx, -S, PR), :] = jnp.zeros((PR, W), F32)
        for side in (-1, W):
            buf[pl.ds(PR + S + side, N, stride=PR), :] = jnp.zeros((N, W), F32)

    def zero_turned(buf, sides):
        for side in sides:
            buf[pl.ds(S + side, N, stride=PR), :] = jnp.zeros((N, W), F32)
    zero_turned(AT, (-1, W))
    zero_turned(BT, (-1, W))

    @pl.loop(0, XR // S)
    def _(t):
        X[W, eight(pl.multiple_of(t * S, S)), :] = zero
    for q in range(5):
        TS[q, eight(0), :] = zero

    def x_copy(par):
        return pltpu.make_async_remote_copy(
            src_ref=flats[par].at[block(W - LAST * cx), :], dst_ref=flats[par].at[block(129 * cx), :],
            send_sem=xs.at[par], recv_sem=xr.at[par], device_id=px, device_id_type=MESH)

    def side_copy(par, k, src, dst, ssem, rsem, to):
        planes = pl.ds(pl.multiple_of(k * CP, S), CP)
        return pltpu.make_async_remote_copy(
            src_ref=src.at[par, planes, :], dst_ref=dst.at[par, planes, :],
            send_sem=ssem.at[par, k], recv_sem=rsem.at[par, k], device_id=to, device_id_type=MESH)

    def side_copies(par, k):
        return side_copy(par, k, PY, RY, ys, yr, py), side_copy(par, k, PZ, RZ, zs, zr, pz)

    def send(par, k):
        planes = pl.ds(k * CP, CP)
        PY[par, planes, :] = flats[par][pl.ds((k * CP + 1) * PR + S + LAST * (1 - cy), CP, stride=PR), :]
        PZ[par, planes, :] = turned[par][pl.ds(k * CP * PR + S + LAST * (1 - cz), CP, stride=PR), :]
        for cp in side_copies(par, k):
            cp.start()

    def receive(par, k):
        for cp in side_copies(par, k):
            cp.wait()
        planes = pl.ds(k * CP, CP)
        flats[par][pl.ds((k * CP + 1) * PR + S + W - (W + 1) * cy, CP, stride=PR), :] = RY[par, planes, :]
        turned[par][pl.ds(k * CP * PR + S + W - (W + 1) * cz, CP, stride=PR), :] = RZ[par, planes, :]

    def place(g):
        return chunk_of(g // GC) * CP + g % GC * GP

    def turn(par, i0, count):
        for q in range(count):
            turned[par][block(i0 + q), :] = jnp.transpose(flats[par][block(i0 + q + 1), :])

    def side_sums(par, i0):
        for q in range(GP):
            KS[pl.ds(q * W, W), :] = jnp.transpose(turned[par][block(i0 + q, -1), :] + turned[par][block(i0 + q, 1), :])

    def after_chunk(g, done):
        @pl.when((g % GC == 0) & (g > 0))
        def _():
            done(g // GC - 1)

    def first_chunk(par, c):
        @pl.when(c == 0)
        def _():
            x_copy(par).start()

    def stencil_pass(par, visit, dst, done, arrive=None, groups=NG):
        src = flats[par]
        x_copy(par).wait()
        receive(par, chunk_of(0))
        side_sums(par, place(0))
        if arrive is not None:
            arrive(chunk_of(0))

        @pl.loop(0, groups)
        def _(g):
            @pl.when((g % GC == GC - 1) & (g < groups - 1))
            def _():
                receive(par, chunk_of(g // GC + 1))
                if arrive is not None:
                    arrive(chunk_of(g // GC + 1))
            i0 = place(g)
            if dst is not None:
                turn(dst, place((g + NG - 1) % NG), GP)
            for t in range(W // RB):
                r = t * RB
                um, uc = src[block(i0, r, RB), :], src[block(i0 + 1, r, RB), :]
                for q in range(GP):
                    un = src[block(i0 + q + 2, r, RB), :]
                    total = (um + un) + (src[block(i0 + q + 1, r - 1, RB), :] + src[block(i0 + q + 1, r + 1, RB), :]) + KS[
                        pl.ds(q * W + r, RB), :]
                    visit(i0 + q, r, uc, total)
                    um, uc = uc, un
            side_sums(par, place((g + 1) % NG))
            if done is not None:
                after_chunk(g, done)
        if dst is not None:
            turn(dst, place(NG - 1), GP)
        if done is not None:
            done(NC - 1)

    def sweep_pass(par, first, last):
        def visit(i, r, centre, total):
            fs = F[i, pl.ds(r, RB), :]
            if first:
                fs = fs * F32(h2)
                F[i, pl.ds(r, RB), :] = fs
            flats[1 - par][block(i + 1, r, RB), :] = (3.0 * centre + (total + fs)) * ninth

        def done(c):
            k = chunk_of(c)
            first_chunk(1 - par, c)
            send(1 - par, k)
        stencil_pass(par, visit, None if last else 1 - par, None if last else done,
                     (lambda k: load(1, k).wait()) if first else None, NG // 2 if last else NG)

    def start_level0():
        @pl.loop(0, NC)
        def _(c):
            k = chunk_of(c)
            load(0, k).wait()
            load(1, k).start()

            @pl.loop(0, CP // S)
            def _(t):
                turn(0, k * CP + t * S, S)
            first_chunk(0, c)
            send(0, k)

    def residual_pass():
        def visit(i, r, centre, total):
            BT[block(i, r, RB), :] = F[i, pl.ds(r, RB), :] - 6.0 * centre + total
        stencil_pass(0, visit, None, None)
        zero_turned(BT, (-1,))

    def restrict_planes(i, weights, dst, dst_plane, jc, count):
        acc = None
        for di, w in weights:
            base = (i + di) * PR + S + 2 * jc
            lo, mid, hi = (BT[pl.ds(base + d, count, stride=2), :] for d in (-1, 0, 1))
            tail = BT[pl.ds(base - 1, 1), :]
            pair = (lo + hi) + 2.0 * mid if count > 1 else tail
            pair = pair if w == 1 else pair * w
            acc = pair if acc is None else acc + pair
        dst[pl.ds(dst_plane * XR + jc, count), :] = acc

    def restrict_rows(jc, count):
        restrict_planes(0, ((0, 2.0), (1, 1)), X2, 64 * cx, jc, count)

        @pl.loop(1, 64)
        def _(i):
            restrict_planes(2 * i, ((-1, 1), (0, 2.0), (1, 1)), X2, i + 64 * cx, jc, count)

    JP = (24, 24, 16)

    def to_level1():
        spans = []
        for m, count in enumerate(JP):
            jc = sum(JP[:m])
            pieces = ((jc, count),) if m < 2 else ((jc, count), (jc + count, 1))
            spans.append((jc, pieces))
        for jc, pieces in spans:
            for piece in pieces:
                restrict_planes(LAST, ((0, 1),), XP, 0, *piece)
        own = pl.ds(64 * cx, 64)
        whole = [pltpu.make_async_remote_copy(src_ref=XP, dst_ref=RXP, send_sem=cs.at[3], recv_sem=cr.at[3],
                                              device_id=px, device_id_type=MESH)]
        whole[0].start()
        for m, (jc, pieces) in enumerate(spans):
            for piece in pieces:
                restrict_rows(*piece)
            part = X.at[own, pl.ds(jc, JP[0]), :]
            whole.append(pltpu.make_async_remote_copy(src_ref=part, dst_ref=part, send_sem=cs.at[m], recv_sem=cr.at[m],
                                                      device_id=px, device_id_type=MESH))
            whole[-1].start()
        zero_rows(AT, L1.rows)
        whole[0].wait()

        def tile(jc, q):
            TS[q, pl.ds(S, W), :] = jnp.transpose(X2[pl.ds(jc, W, stride=XR), :])
            base = (jc + L1.pj) * L1.nk + L1.kp
            lo, mid, hi = (TS[q, pl.ds(S + d, 64, stride=2), :] for d in (-1, 0, 1))
            G1[pl.ds(pl.multiple_of(base, S), 64), :] = ((lo + hi) + 2.0 * mid) * F32(1 / 16)
            G1[pl.ds(base + 64, 1), :] = TS[q, pl.ds(135, 1), :] * F32(1 / 16)

        for m, (jc, pieces) in enumerate(spans):
            whole[m + 1].wait()
            rows = pl.ds(jc, JP[0])
            X2[pl.ds(64 * XR + jc, JP[0]), :] += jnp.where(cx == 0, XP[rows, :], RXP[rows, :])

            @pl.loop(0, JP[m] // 4)
            def _(jo):
                for q in range(4):
                    tile(jc + jo * 4 + q, q)
        tile(64, 4)

    def wide_exchange(L, G, SY, RY_, SZ, RZ_, SD, RD, s):
        cnt, wide = L.h, L.n + S
        js, ks = (L.n + 1 - cnt) * (1 - cy) + L.pj, (L.n + 1 - cnt) * (1 - cz) + L.kp
        jd, kd = L.n * (1 - cy) + (1 - cnt) * cy + L.pj, L.n * (1 - cz) + (1 - cnt) * cz + L.kp
        for p in range(cnt):
            SY[pl.ds(p * wide, wide), :] = G[pl.ds(pl.multiple_of((js + p) * L.nk + L.kp, S), wide), :]
            SD[pl.ds(p * S, cnt), :] = G[pl.ds((js + p) * L.nk + ks, cnt), :]
        cps = [pltpu.make_async_remote_copy(src_ref=src, dst_ref=dst, send_sem=cs.at[s + n], recv_sem=cr.at[s + n],
                                            device_id=to, device_id_type=MESH)
               for n, (src, dst, to) in enumerate(((SY, RY_, py), (SD, RD, pyz), (SZ, RZ_, pz)))]
        cps[0].start()
        cps[1].start()

        @pl.loop(0, L.n + 1)
        def _(p):
            SZ[pl.ds(p * cnt, cnt), :] = G[pl.ds((L.pj + p) * L.nk + ks, cnt), :]
        cps[2].start()
        for cp in cps:
            cp.wait()
        for p in range(cnt):
            G[pl.ds(pl.multiple_of((jd + p) * L.nk + L.kp, S), wide), :] += RY_[pl.ds(p * wide, wide), :]
            G[pl.ds((jd + p) * L.nk + kd, cnt), :] += RD[pl.ds(p * S, cnt), :]

        @pl.loop(0, L.n + 1)
        def _(p):
            G[pl.ds((L.pj + p) * L.nk + kd, cnt), :] += RZ_[pl.ds(p * cnt, cnt), :]
        last = L.kp - 1 + (L.n + 1) * cz

        @pl.loop(0, L.region)
        def _(p):
            G[pl.ds((L.pj - (L.region - L.n) * cy + p) * L.nk + last, 1), :] = zero[:1]
        G[pl.ds(pl.multiple_of((L.pj - 1 + (L.n + 1) * cy) * L.nk, S), L.nk), :] = jnp.zeros((L.nk, W), F32)

    def coarse_pass(L, src, visit, own=False):
        j0 = L.pj if own else L.pj - (L.region - L.n) * cy
        k0 = L.kp if own else L.kp - L.hb * cz
        count = L.n if own else L.n + L.hb
        planes = L.n if own else L.region
        size = L.size_own if own else L.unroll
        groups = planes // size
        lanes = lax.broadcasted_iota(jnp.int32, (count, W), 1)

        def place(g, p):
            return pl.multiple_of((j0 + g * size + p) * L.nk + k0, S)

        def sides(g):
            out = []
            for p in range(size):
                c = src[pl.ds(place(g, p), count), :]
                out.append(jnp.where(lanes == 0, 0.0, pltpu.roll(c, 1, 1)) + jnp.where(
                    lanes == L.ni - 1, 0.0, pltpu.roll(c, LAST, 1)))
            return out

        def keep(sums):
            for p in range(size):
                KS[pl.ds(p * count, count), :] = sums[p]
        keep(sides(0))

        @pl.loop(0, groups)
        def _(g):
            later = sides((g + 1) % groups)
            for p in range(size):
                r = place(g, p)
                total = (src[pl.ds(r - L.nk, count), :] + src[pl.ds(r + L.nk, count), :]) + (
                    src[pl.ds(r - 1, count), :] + src[pl.ds(r + 1, count), :]) + KS[pl.ds(p * count, count), :]
                visit(pl.ds(r, count), src[pl.ds(r, count), :], total)
            keep(later)

    def first_two(L, G, V):
        def visit(rows, c, total):
            V[rows, :] = (12.0 * c + total) * F32(1 / 81)
        coarse_pass(L, G, visit)

    def smooth(L, G, V, W_):
        def visit(rows, c, total):
            W_[rows, :] = (3.0 * c + (total + G[rows, :])) * ninth
        coarse_pass(L, V, visit)

    def weights(ni, up, offset=0):
        a = lax.broadcasted_iota(jnp.int32, (W, W), 0)
        b = lax.broadcasted_iota(jnp.int32, (W, W), 1)
        fine, coarse = (b, a - offset) if up else (a, b - offset)
        near = (fine == 2 * coarse + 1) | (fine == 2 * coarse - 1)
        w = jnp.where(fine == 2 * coarse, 1.0, 0.0) + jnp.where(near, 0.5, 0.0)
        return jnp.where((coarse >= 0) & (coarse < ni) & (fine < 2 * ni), w if up else 2.0 * w, 0.0).astype(F32)

    def lane_dot(x, w):
        return jnp.dot(x, w, precision=HI, preferred_element_type=F32)

    def restrict_coarse(L, M, G, V, W_):
        def visit(rows, c, total):
            W_[rows, :] = G[rows, :] - 6.0 * c + total
        coarse_pass(L, V, visit, True)
        for side in (L.pj - 1, L.pj + L.n, L.pj + L.n + 1):
            W_[pl.ds(side * L.nk, L.nk), :] = jnp.zeros((L.nk, W), F32)

        @pl.loop(0, L.n)
        def _(p):
            base = (L.pj + p) * L.nk + L.kp
            W_[eight(pl.multiple_of(base - S, S)), :] = zero
            W_[eight(pl.multiple_of(base + L.n, S)), :] = zero

        @pl.loop(0, M.n + 1)
        def _(p):
            base = (L.pj + 2 * p) * L.nk + L.kp
            rows = M.n + 4
            sums = []
            for dj in (-1, 0, 1):
                lo, mid, hi = (W_[pl.ds(base + dj * L.nk + d, rows, stride=2), :] for d in (-1, 0, 1))
                sums.append((lo + hi) + 2.0 * mid)
            T2[pl.ds(p * (M.n + S), rows), :] = (sums[0] + sums[2]) + 2.0 * sums[1]

    def restrict_lanes(M, Gc):
        hr = M.n + S
        group = 11
        w = weights(M.ni, False)

        @pl.loop(0, (M.n + 1) // group)
        def _(g):
            t0 = pl.multiple_of(g * group * hr, S)
            res = lane_dot(T2[pl.ds(t0, group * hr), :], w) * F32(1 / 16)
            for p in range(group):
                rb = (M.pj + g * group + p) * M.nk + M.kp
                Gc[pl.ds(pl.multiple_of(rb, S), M.n), :] = res[p * hr:p * hr + M.n]
                Gc[pl.ds(rb + M.n, 1), :] = res[p * hr + M.n:p * hr + M.n + 1]

    KR, KA = 48, 32

    def gather_coarsest():
        hr, cells = L3.n + S, L3.n + 1
        parts = [lane_dot(T2[pl.ds(p * S * hr, n * hr), :], weights(L3.ni, False, L3.ni * (2 * cy + p)))
                 for p, n in ((0, S), (1, S), (2, 1))]
        for p in range(S):
            x = parts[0][p * hr:p * hr + cells] + parts[1][p * hr:p * hr + cells]
            x = x + parts[2][:cells] if p == 0 else x
            S3[pl.ds(p * cells, cells), :] = x * F32(1 / 16)
        cps = [pltpu.make_async_remote_copy(src_ref=S3, dst_ref=R3.at[n], send_sem=cs.at[10 + n],
                                            recv_sem=cr.at[10 + n], device_id=to, device_id_type=MESH)
               for n, to in enumerate((py, pz, pyz))]
        for cp in cps:
            cp.start()
        for cp in cps:
            cp.wait()
        low, high = S + L3.n * cz, S + L3.n * (1 - cz)
        for p in range(S):
            rows = pl.ds(p * cells, cells)
            G3[pl.ds(p * KR + low, cells), :] += S3[rows, :] + R3[0, rows, :]
            G3[pl.ds(p * KR + high, cells), :] += R3[1, rows, :] + R3[2, rows, :]
            G3[pl.ds(p * KR + S + KA, 1), :] = zero[:1]

    def coarsest_pass(src, visit):
        lanes = lax.broadcasted_iota(jnp.int32, (KA, W), 1)
        cell = lanes % KA
        at = lambda p: pl.ds(p * KR + S, KA)
        for p in range(S):
            c = src[at(p), :]
            left = jnp.where(cell == 0, 0.0, pltpu.roll(c, 1, 1))
            right = jnp.where(cell == KA - 1, 0.0, pltpu.roll(c, LAST, 1))
            lo = src[at(p - 1), :] if p else jnp.where(lanes < KA, 0.0, pltpu.roll(src[at(S - 1), :], KA, 1))
            hi = src[at(p + 1), :] if p < S - 1 else jnp.where(lanes < W - KA, pltpu.roll(src[at(0), :], W - KA, 1), 0.0)
            total = (lo + hi) + (src[pl.ds(p * KR + S - 1, KA), :] + src[pl.ds(p * KR + S + 1, KA), :]) + (left + right)
            visit(at(p), c, total)

    def solve_coarsest():
        def first(rows, c, total):
            V3[rows, :] = (12.0 * c + total) * F32(1 / 81)
        coarsest_pass(G3, first)

        @pl.loop(0, 7)
        def _(s):
            for V, W_ in ((V3, W3), (W3, V3)):
                def visit(rows, c, total):
                    W_[rows, :] = (3.0 * c + (total + G3[rows, :])) * ninth
                coarsest_pass(V, visit)

    def spread_coarsest():
        def plane(j):
            return pl.ds(pl.multiple_of((L3.pj + j) * L3.nk + L3.kp - S, S), KA)
        E[plane(L3.n), :] = jnp.zeros((KA, W), F32)
        x = jnp.concatenate([V3[pl.ds(pl.multiple_of(p * KR + L3.n * cz, S), KA), :] for p in range(S)], axis=0)
        for q in (0, 1, 2 - 3 * cy):
            y = lane_dot(x, weights(L3.ni, True, L3.ni * (2 * cy + q)))
            for p in range(S):
                E[plane(q * S + p), :] = y[p * KA:p * KA + KA]

    def spread_lanes(M, e):
        w = weights(M.ni, True)
        j0 = M.pj - EXTRA * cy

        @pl.loop(0, (M.n + EXTRA + 1) // M.group)
        def _(g):
            rows = pl.ds(pl.multiple_of((j0 + g * M.group) * M.nk, S), M.group * M.nk)
            E[rows, :] = lane_dot(e[rows, :], w)

    def prolong_coarse(L, M, V):
        j0 = M.pj - EXTRA * cy

        @pl.loop(0, M.n + EXTRA)
        def _(p):
            jc = j0 + p - M.pj
            fb = (L.pj + 2 * jc) * L.nk + L.kp
            eb = (j0 + p) * M.nk + M.kp
            for kc, rows in ((0, M.n), (M.n * (1 - cz) - 4 * cz, 4)):
                a, b = E[pl.ds(eb + kc, rows), :], E[pl.ds(eb + kc + 1, rows), :]
                c, d = E[pl.ds(eb + M.nk + kc, rows), :], E[pl.ds(eb + M.nk + kc + 1, rows), :]
                ab = a + b
                f = fb + 2 * kc
                V[pl.ds(f, rows, stride=2), :] += a
                V[pl.ds(f + 1, rows, stride=2), :] += 0.5 * ab
                V[pl.ds(f + L.nk, rows, stride=2), :] += 0.5 * (a + c)
                V[pl.ds(f + L.nk + 1, rows, stride=2), :] += 0.25 * (ab + (c + d))

    def from_level1():
        @pl.loop(0, 13)
        def _(jo):
          for q in range(5):
            jc = jo * 5 + q
            base = (jc + L1.pj) * L1.nk + L1.kp
            a, b = V1[pl.ds(pl.multiple_of(base, S), 64), :], V1[pl.ds(base + 1, 64), :]
            TS[q, pl.ds(S, 64, stride=2), :] = a
            TS[q, pl.ds(S + 1, 64, stride=2), :] = 0.5 * (a + b)
            X2[pl.ds(jc, W, stride=XR), :] = jnp.transpose(TS[q, pl.ds(S, W), :])

    def prolong_level0():
        zero_turned(AT, (-1, W))

        def done(c):
            first_chunk(1, c)
            send(1, chunk_of(c))

        @pl.loop(0, NG)
        def _(g):
            i0 = place(g)
            turn(1, place((g + NG - 1) % NG), GP)
            for q in range(GP // 2):
                half = W // 2
                xb = (i0 // 2 + q + half * cx) * XR
                a, b = X2[pl.ds(xb, half), :], X2[pl.ds(xb + 1, half), :]
                cc, d = X2[pl.ds(xb + XR, half), :], X2[pl.ds(xb + XR + 1, half), :]
                ab = a + b
                f = (i0 + 2 * q + 1) * PR + S
                for shift, value in ((0, a), (1, 0.5 * ab), (PR, 0.5 * (a + cc)), (PR + 1, 0.25 * (ab + (cc + d)))):
                    rows = pl.ds(f + shift, half, stride=2)
                    B2[rows, :] = A2[rows, :] + value
            after_chunk(g, done)
        turn(1, place(NG - 1), GP)
        done(NC - 1)

    start_level0()
    sweep_pass(0, True, False)
    sweep_pass(1, False, False)
    residual_pass()
    to_level1()
    wide_exchange(L1, G1, SY1, RY1, SZ1, RZ1, SD1, RD1, 4)
    first_two(L1, G1, V1)
    restrict_coarse(L1, L2, G1, V1, W1)
    restrict_lanes(L2, G2)
    wide_exchange(L2, G2, SY2, RY2, SZ2, RZ2, SD2, RD2, 7)
    first_two(L2, G2, V2)
    restrict_coarse(L2, L3, G2, V2, W2)
    gather_coarsest()
    solve_coarsest()
    spread_coarsest()
    prolong_coarse(L2, L3, V2)
    smooth(L2, G2, V2, W2)
    smooth(L2, G2, W2, V2)
    spread_lanes(L2, V2)
    prolong_coarse(L1, L2, V1)
    smooth(L1, G1, V1, W1)
    smooth(L1, G1, W1, V1)
    from_level1()
    prolong_level0()
    sweep_pass(1, False, False)
    sweep_pass(0, False, True)
    for c in range(NC // 2, NC):
        receive(0, chunk_of(c))


def close(B, A, AT, F, out_hbm, O, KS, sems):
    cx = lax.axis_index('sx')

    def chunk_of(c):
        return c * cx + (NC - 1 - c) * (1 - cx)

    def place(g):
        return chunk_of(g // GC) * CP + g % GC * GP

    def rows(i, shift=0, count=W):
        return pl.ds(i * PR + S + shift, count)

    def store(c):
        planes = pl.ds(chunk_of(c) * CP, CP)
        src = B.at[pl.ds(chunk_of(c) * CP + 1, CP), pl.ds(S, W), :] if c < NC // 2 else O.at[pl.ds((c - NC // 2) * CP, CP)]
        return pltpu.make_async_copy(src, out_hbm.at[planes], sems.at[c])
    for c in range(NC // 2):
        store(c).start()
    src = A.reshape(A.shape[0] * PR, W)

    def side_sums(i0):
        for q in range(GP):
            KS[pl.ds(q * W, W), :] = jnp.transpose(AT[rows(i0 + q, -1), :] + AT[rows(i0 + q, 1), :])
    side_sums(place(NG // 2))
    for c in range(NC // 2, NC):
        @pl.loop(c * GC, (c + 1) * GC)
        def _(g):
            i0 = place(g)
            for t in range(W // RB):
                r = t * RB
                um, uc = src[rows(i0, r, RB), :], src[rows(i0 + 1, r, RB), :]
                for q in range(GP):
                    un = src[rows(i0 + q + 2, r, RB), :]
                    total = (um + un) + (src[rows(i0 + q + 1, r - 1, RB), :] + src[rows(i0 + q + 1, r + 1, RB), :]) + KS[
                        pl.ds(q * W + r, RB), :]
                    new = (3.0 * uc + (total + F[i0 + q, pl.ds(r, RB), :])) * F32(1 / 9)
                    O[(g - NG // 2) * GP + q, pl.ds(r, RB), :] = new
                    um, uc = uc, un
            side_sums(place((g + 1) % NG))
        store(c).start()
    for c in range(NC):
        store(c).wait()


def solution(mesh):
    spec = P(('dp', 'sx'), 'sy', 'sz')

    def local(f, u):
        size = 2 * f.shape[1]
        h2 = 1.0 / float((size + 1) ** 2)
        vm = lambda *s: pltpu.VMEM(s, F32)
        scratch = [vm(N * PR, W), vm(129, XR, W),
                   vm(XR, W), vm(XR, W), vm(5, 136, W), vm(17 * 72, W), vm(2, N, W), vm(2, N, W), vm(2, N, W), vm(2, N, W)]
        scratch += [vm(L1.rows, W)] * 2 + [vm(L2.rows, W)] * 3 + [vm(S * 48, W)] * 3
        for L in (L1, L2):
            z = up8((L.n + 1) * L.h)
            scratch += [vm(L.h * (L.n + S), W)] * 2 + [vm(z, W)] * 2 + [vm(L.h * S, W)] * 2
        scratch += [vm(S * (L3.n + 1), W), vm(3, S * (L3.n + 1), W)]
        dma = pltpu.SemaphoreType.DMA
        scratch += [dma((2, NC)), dma((2,)), dma((2,)), dma((2, NC)), dma((2, NC)), dma((2, NC)), dma((2, NC)),
                    dma((13,)), dma((13,))]
        resident = [vm(130, PR, W), vm(130, PR, W), vm(N * PR, W), vm(N, N, W)]
        used = 4 * sum(math.prod(x.shape) for x in resident)
        kept = pl.pallas_call(
            functools.partial(body, h2),
            out_shape=resident,
            in_specs=[pl.BlockSpec(memory_space=pl.ANY)] * 2,
            out_specs=[pl.BlockSpec(memory_space=pltpu.VMEM)] * len(resident),
            scratch_shapes=scratch,
            compiler_params=pltpu.CompilerParams(collective_id=0, has_side_effects=True, vmem_limit_bytes=67043328 - used),
        )(f, u)
        kept = [pltpu.with_memory_space_constraint(x, pltpu.VMEM) for x in kept]
        return pl.pallas_call(
            close,
            out_shape=jax.ShapeDtypeStruct(f.shape, F32),
            in_specs=[pl.BlockSpec(memory_space=pltpu.VMEM)] * len(kept),
            out_specs=pl.BlockSpec(memory_space=pl.ANY),
            scratch_shapes=[vm(N // 2, N, W), vm(GP * W, W), dma((NC,))],
            compiler_params=pltpu.CompilerParams(vmem_limit_bytes=67043328 - used),
        )(*kept)

    def run(rhs_grid, u_start):
        return jax.shard_map(local, mesh=mesh, in_specs=(spec, spec), out_specs=spec, check_vma=False)(rhs_grid, u_start)
    return run
```

```python
import functools
import math
import jax
import jax.numpy as jnp
from jax import lax
from jax.experimental import pallas as pl
from jax.experimental.pallas import tpu as pltpu
from jax.sharding import PartitionSpec as P

N = 128
PR = 144
NC = 4
XR = 72
CP = N // NC
GP = 16
GC = CP // GP
NG = N // GP
RB = 32
S, W = 8, 128
LAST = W - 1
MESH = pl.DeviceIdType.MESH
F32 = jnp.float32
HI = lax.Precision.HIGHEST


class Lev:
    def __init__(self, n, h, pj, kp, hb, ni, region, unroll, group):
        self.n, self.h, self.pj, self.kp, self.hb, self.ni = n, h, pj, kp, hb, ni
        self.region, self.unroll, self.group = region, unroll, group
        self.size_own = 16
        self.nk = n + 2 * kp
        self.planes = n + 2 * pj
        self.rows = self.planes * self.nk


L1 = Lev(64, 4, 6, 8, 8, 128, 68, 17, 1)
L2 = Lev(32, 5, 10, 8, 8, 64, 40, 20, 12)
L3 = Lev(16, 16, 18, 16, 16, 32, 32, 8, 10)
EXTRA = 3


def up8(x):
    return (x + 7) // 8 * 8


def eight(r):
    return pl.ds(r, S)


def body(h2, f_hbm, u_hbm, B, A, AT, F, BT, X, XP, RXP, TS, KS, PZ, RZ, PY, RY,
         V1, W1, G2, V2, W2, G3, V3, W3,
         SY1, RY1, SZ1, RZ1, SD1, RD1, SY2, RY2, SZ2, RZ2, SD2, RD2, S3, R3,
         ld, xs, xr, zs, zr, ys, yr, cs, cr):
    cx, cy, cz = lax.axis_index('sx'), lax.axis_index('sy'), lax.axis_index('sz')
    ninth = F32(1.0 / 9.0)
    px, py, pz = {'sx': 1 - cx}, {'sy': 1 - cy}, {'sz': 1 - cz}
    pyz = {**py, **pz}

    def flat(ref):
        return ref.reshape(ref.shape[0] * ref.shape[1], ref.shape[2])

    A2, B2, X2 = flat(A), flat(B), flat(X)
    flats, turned = (A2, B2), (AT, BT)
    G1, T2 = AT.at[pl.ds(0, L1.rows), :], AT.at[pl.ds(L1.rows, 33 * 40), :]
    E = AT.at[pl.ds(L1.rows + 33 * 40, max(L2.rows, L3.rows)), :]

    def chunk_of(c):
        return c * cx + (NC - 1 - c) * (1 - cx)

    def block(i, shift=0, count=W):
        if isinstance(shift, int) and shift % S == 0:
            return pl.ds(pl.multiple_of(i * PR + S + shift, S), count)
        return pl.ds(i * PR + S + shift, count)

    def load(which, k):
        planes = pl.ds(k * CP, CP)
        src, dst = ((u_hbm, A.at[pl.ds(k * CP + 1, CP), pl.ds(S, W), :]), (f_hbm, F.at[planes]))[which]
        return pltpu.make_async_copy(src.at[planes], dst, ld.at[which, k])
    for c in range(NC):
        load(0, chunk_of(c)).start()

    barrier = pltpu.get_barrier_semaphore()
    for p in (px, py, pz, pyz):
        pl.semaphore_signal(barrier, inc=1, device_id=p, device_id_type=MESH)
    pl.semaphore_wait(barrier, 4)

    zero = jnp.zeros((S, W), F32)

    def zero_rows(ref2, count):
        @pl.loop(0, count // 64)
        def _(t):
            ref2[pl.ds(pl.multiple_of(t * 64, 64), 64), :] = jnp.zeros((64, W), F32)
        if count % 64:
            ref2[pl.ds(count // 64 * 64, count % 64), :] = jnp.zeros((count % 64, W), F32)
    for ref in (V1, W1, G2, V2, W2, G3, V3, W3):
        zero_rows(ref, ref.shape[0])

    for buf in flats:
        buf[block(129 * cx, -S, PR), :] = jnp.zeros((PR, W), F32)
        for side in (-1, W):
            buf[pl.ds(PR + S + side, N, stride=PR), :] = jnp.zeros((N, W), F32)

    def zero_turned(buf, sides):
        for side in sides:
            buf[pl.ds(S + side, N, stride=PR), :] = jnp.zeros((N, W), F32)
    zero_turned(AT, (-1, W))
    zero_turned(BT, (-1, W))

    @pl.loop(0, XR // S)
    def _(t):
        X[W, eight(pl.multiple_of(t * S, S)), :] = zero
    for q in range(5):
        TS[q, eight(0), :] = zero

    def x_copy(par):
        return pltpu.make_async_remote_copy(
            src_ref=flats[par].at[block(W - LAST * cx), :], dst_ref=flats[par].at[block(129 * cx), :],
            send_sem=xs.at[par], recv_sem=xr.at[par], device_id=px, device_id_type=MESH)

    def side_copy(par, k, src, dst, ssem, rsem, to):
        planes = pl.ds(pl.multiple_of(k * CP, S), CP)
        return pltpu.make_async_remote_copy(
            src_ref=src.at[par, planes, :], dst_ref=dst.at[par, planes, :],
            send_sem=ssem.at[par, k], recv_sem=rsem.at[par, k], device_id=to, device_id_type=MESH)

    def side_copies(par, k):
        return side_copy(par, k, PY, RY, ys, yr, py), side_copy(par, k, PZ, RZ, zs, zr, pz)

    def send(par, k):
        planes = pl.ds(k * CP, CP)
        PY[par, planes, :] = flats[par][pl.ds((k * CP + 1) * PR + S + LAST * (1 - cy), CP, stride=PR), :]
        PZ[par, planes, :] = turned[par][pl.ds(k * CP * PR + S + LAST * (1 - cz), CP, stride=PR), :]
        for cp in side_copies(par, k):
            cp.start()

    def receive(par, k):
        for cp in side_copies(par, k):
            cp.wait()
        planes = pl.ds(k * CP, CP)
        flats[par][pl.ds((k * CP + 1) * PR + S + W - (W + 1) * cy, CP, stride=PR), :] = RY[par, planes, :]
        turned[par][pl.ds(k * CP * PR + S + W - (W + 1) * cz, CP, stride=PR), :] = RZ[par, planes, :]

    def place(g):
        return chunk_of(g // GC) * CP + g % GC * GP

    def turn(par, i0, count):
        base = pl.multiple_of(i0 * PR, S)
        for q in range(count):
            turned[par][pl.ds(base + (q * PR + S), W), :] = jnp.transpose(flats[par][pl.ds(base + ((q + 1) * PR + S), W), :])

    def side_sums(par, i0):
        base = pl.multiple_of(i0 * PR, S)
        for q in range(GP):
            lo, hi = (turned[par][pl.ds(base + (q * PR + S + d), W), :] for d in (-1, 1))
            KS[pl.ds(q * W, W), :] = jnp.transpose(lo + hi)

    def after_chunk(g, done):
        @pl.when((g % GC == 0) & (g > 0))
        def _():
            done(g // GC - 1)

    def first_chunk(par, c):
        @pl.when(c == 0)
        def _():
            x_copy(par).start()

    def stencil_pass(par, visit, dst, done, arrive=None, groups=NG):
        src = flats[par]
        x_copy(par).wait()
        receive(par, chunk_of(0))
        side_sums(par, place(0))
        if arrive is not None:
            arrive(chunk_of(0))

        @pl.loop(0, groups)
        def _(g):
            @pl.when((g % GC == GC - 1) & (g < groups - 1))
            def _():
                receive(par, chunk_of(g // GC + 1))
                if arrive is not None:
                    arrive(chunk_of(g // GC + 1))
            i0 = place(g)
            if dst is not None:
                turn(dst, place((g + NG - 1) % NG), GP)
            base = pl.multiple_of(i0 * PR, S)

            def at(q, r):
                return pl.ds(base + (q * PR + S + r), RB)
            for t in range(W // RB):
                r = t * RB
                um, uc = src[at(0, r), :], src[at(1, r), :]
                for q in range(GP):
                    un = src[at(q + 2, r), :]
                    total = (um + un) + (src[at(q + 1, r - 1), :] + src[at(q + 1, r + 1), :]) + KS[pl.ds(q * W + r, RB), :]
                    visit(i0, at, q, r, uc, total)
                    um, uc = uc, un
            side_sums(par, place((g + 1) % NG))
            if done is not None:
                after_chunk(g, done)
        if dst is not None:
            turn(dst, place(NG - 1), GP)
        if done is not None:
            done(NC - 1)

    def sweep_pass(par, first, last):
        def visit(i0, at, q, r, centre, total):
            fs = F[i0 + q, pl.ds(r, RB), :]
            if first:
                fs = fs * F32(h2)
                F[i0 + q, pl.ds(r, RB), :] = fs
            flats[1 - par][at(q + 1, r), :] = (3.0 * centre + (total + fs)) * ninth

        def done(c):
            k = chunk_of(c)
            first_chunk(1 - par, c)
            send(1 - par, k)
        stencil_pass(par, visit, None if last else 1 - par, None if last else done,
                     (lambda k: load(1, k).wait()) if first else None, NG // 2 if last else NG)

    def start_level0():
        @pl.loop(0, NC)
        def _(c):
            k = chunk_of(c)
            load(0, k).wait()
            load(1, k).start()

            @pl.loop(0, CP // S)
            def _(t):
                turn(0, k * CP + t * S, S)
            first_chunk(0, c)
            send(0, k)

    def residual_pass():
        def visit(i0, at, q, r, centre, total):
            BT[at(q, r), :] = F[i0 + q, pl.ds(r, RB), :] - 6.0 * centre + total
        stencil_pass(0, visit, None, None)
        zero_turned(BT, (-1, W, W + 1))

    def restrict_rows(jc, count):
        def line(plane):
            lo, mid, hi = (BT[pl.ds(plane * PR + S + 2 * jc + d, count, stride=2), :] for d in (-1, 0, 1))
            return (lo + hi) + 2.0 * mid

        def put(i, value):
            X2[pl.ds((i + 64 * cx) * XR + jc, count), :] = value

        def step(t, last):
            for q in range(3):
                i = 1 + t * 3 + q
                odd = line(2 * i + 1)
                put(i, (last + odd) + 2.0 * line(2 * i))
                last = odd
            return last
        odd = line(1)
        put(0, odd + 2.0 * line(0))
        XP[pl.ds(jc, count), :] = lax.fori_loop(0, 21, step, odd)

    JP = (24, 24, 17)

    def to_level1():
        own = pl.ds(64 * cx, 64)
        copies = []
        for m, count in enumerate(JP):
            jc = m * JP[0]
            restrict_rows(jc, count)
            part, rows = X.at[own, pl.ds(jc, JP[0]), :], pl.ds(jc, JP[0])
            pair = [pltpu.make_async_remote_copy(src_ref=src, dst_ref=dst, send_sem=cs.at[2 * m + n], recv_sem=cr.at[2 * m + n],
                                                 device_id=px, device_id_type=MESH)
                    for n, (src, dst) in enumerate(((XP.at[rows, :], RXP.at[rows, :]), (part, part)))]
            for cp in pair:
                cp.start()
            copies.append(pair)
        zero_rows(AT, L1.rows)

        def tile(jc, q):
            TS[q, pl.ds(S, W), :] = jnp.transpose(X2[pl.ds(jc, W, stride=XR), :])
            base = (jc + L1.pj) * L1.nk + L1.kp
            lo, mid, hi = (TS[q, pl.ds(S + d, 64, stride=2), :] for d in (-1, 0, 1))
            G1[pl.ds(pl.multiple_of(base, S), 64), :] = ((lo + hi) + 2.0 * mid) * F32(1 / 16)
            G1[pl.ds(base + 64, 1), :] = TS[q, pl.ds(135, 1), :] * F32(1 / 16)

        for m, pair in enumerate(copies):
            for cp in pair:
                cp.wait()
            jc = m * JP[0]
            rows = pl.ds(jc, JP[0])
            X2[pl.ds(64 * XR + jc, JP[0]), :] += jnp.where(cx == 0, XP[rows, :], RXP[rows, :])

            @pl.loop(0, JP[m] // 4)
            def _(jo):
                for q in range(4):
                    tile(jc + jo * 4 + q, q)
        tile(64, 4)

    def wide_exchange(L, G, SY, RY_, SZ, RZ_, SD, RD, s):
        cnt, wide = L.h, L.n + S
        js, ks = (L.n + 1 - cnt) * (1 - cy) + L.pj, (L.n + 1 - cnt) * (1 - cz) + L.kp
        jd, kd = L.n * (1 - cy) + (1 - cnt) * cy + L.pj, L.n * (1 - cz) + (1 - cnt) * cz + L.kp
        for p in range(cnt):
            SY[pl.ds(p * wide, wide), :] = G[pl.ds(pl.multiple_of((js + p) * L.nk + L.kp, S), wide), :]
            SD[pl.ds(p * S, cnt), :] = G[pl.ds((js + p) * L.nk + ks, cnt), :]
        cps = [pltpu.make_async_remote_copy(src_ref=src, dst_ref=dst, send_sem=cs.at[s + n], recv_sem=cr.at[s + n],
                                            device_id=to, device_id_type=MESH)
               for n, (src, dst, to) in enumerate(((SY, RY_, py), (SD, RD, pyz), (SZ, RZ_, pz)))]
        cps[0].start()
        cps[1].start()

        @pl.loop(0, L.n + 1)
        def _(p):
            SZ[pl.ds(p * cnt, cnt), :] = G[pl.ds((L.pj + p) * L.nk + ks, cnt), :]
        cps[2].start()
        for cp in cps:
            cp.wait()
        for p in range(cnt):
            G[pl.ds(pl.multiple_of((jd + p) * L.nk + L.kp, S), wide), :] += RY_[pl.ds(p * wide, wide), :]
            G[pl.ds((jd + p) * L.nk + kd, cnt), :] += RD[pl.ds(p * S, cnt), :]

        @pl.loop(0, L.n + 1)
        def _(p):
            G[pl.ds((L.pj + p) * L.nk + kd, cnt), :] += RZ_[pl.ds(p * cnt, cnt), :]
        last = L.kp - 1 + (L.n + 1) * cz

        @pl.loop(0, L.region)
        def _(p):
            G[pl.ds((L.pj - (L.region - L.n) * cy + p) * L.nk + last, 1), :] = zero[:1]
        G[pl.ds(pl.multiple_of((L.pj - 1 + (L.n + 1) * cy) * L.nk, S), L.nk), :] = jnp.zeros((L.nk, W), F32)

    def coarse_pass(L, src, visit, own=False):
        j0 = L.pj if own else L.pj - (L.region - L.n) * cy
        k0 = L.kp if own else L.kp - L.hb * cz
        count = L.n if own else L.n + L.hb
        planes = L.n if own else L.region
        size = L.size_own if own else L.unroll
        groups = planes // size
        lanes = lax.broadcasted_iota(jnp.int32, (count, W), 1)

        def place(g):
            return pl.multiple_of((j0 + g * size) * L.nk + k0, S)

        def sides(g):
            out = []
            base = place(g)
            for p in range(size):
                c = src[pl.ds(base + p * L.nk, count), :]
                out.append(jnp.where(lanes == 0, 0.0, pltpu.roll(c, 1, 1)) + jnp.where(
                    lanes == L.ni - 1, 0.0, pltpu.roll(c, LAST, 1)))
            return out

        def keep(sums):
            for p in range(size):
                KS[pl.ds(p * count, count), :] = sums[p]
        keep(sides(0))

        @pl.loop(0, groups)
        def _(g):
            later = sides((g + 1) % groups)
            base = place(g)
            for p in range(size):
                lo, hi, below, above, c = (src[pl.ds(base + (p * L.nk + d), count), :] for d in (-L.nk, L.nk, -1, 1, 0))
                visit(pl.ds(base + p * L.nk, count), c, (lo + hi) + (below + above) + KS[pl.ds(p * count, count), :])
            keep(later)

    def first_two(L, G, V):
        def visit(rows, c, total):
            V[rows, :] = (12.0 * c + total) * F32(1 / 81)
        coarse_pass(L, G, visit)

    def smooth(L, G, V, W_):
        def visit(rows, c, total):
            W_[rows, :] = (3.0 * c + (total + G[rows, :])) * ninth
        coarse_pass(L, V, visit)

    def weights(ni, up, offset=0):
        a = lax.broadcasted_iota(jnp.int32, (W, W), 0)
        b = lax.broadcasted_iota(jnp.int32, (W, W), 1)
        fine, coarse = (b, a - offset) if up else (a, b - offset)
        near = (fine == 2 * coarse + 1) | (fine == 2 * coarse - 1)
        w = jnp.where(fine == 2 * coarse, 1.0, 0.0) + jnp.where(near, 0.5, 0.0)
        return jnp.where((coarse >= 0) & (coarse < ni) & (fine < 2 * ni), w if up else 2.0 * w, 0.0).astype(F32)

    def lane_dot(x, w):
        return jnp.dot(x, w, precision=HI, preferred_element_type=F32)

    def restrict_coarse(L, M, G, V, W_):
        def visit(rows, c, total):
            W_[rows, :] = G[rows, :] - 6.0 * c + total
        coarse_pass(L, V, visit, True)
        for side in (L.pj - 1, L.pj + L.n, L.pj + L.n + 1):
            W_[pl.ds(side * L.nk, L.nk), :] = jnp.zeros((L.nk, W), F32)

        @pl.loop(0, L.n)
        def _(p):
            base = (L.pj + p) * L.nk + L.kp
            W_[eight(pl.multiple_of(base - S, S)), :] = zero
            W_[eight(pl.multiple_of(base + L.n, S)), :] = zero

        @pl.loop(0, M.n + 1)
        def _(p):
            base = (L.pj + 2 * p) * L.nk + L.kp
            rows = M.n + 4
            sums = []
            for dj in (-1, 0, 1):
                lo, mid, hi = (W_[pl.ds(base + dj * L.nk + d, rows, stride=2), :] for d in (-1, 0, 1))
                sums.append((lo + hi) + 2.0 * mid)
            T2[pl.ds(p * (M.n + S), rows), :] = (sums[0] + sums[2]) + 2.0 * sums[1]

    def restrict_lanes(M, Gc):
        hr = M.n + S
        group = 11
        w = weights(M.ni, False)

        @pl.loop(0, (M.n + 1) // group)
        def _(g):
            t0 = pl.multiple_of(g * group * hr, S)
            res = lane_dot(T2[pl.ds(t0, group * hr), :], w) * F32(1 / 16)
            for p in range(group):
                rb = (M.pj + g * group + p) * M.nk + M.kp
                Gc[pl.ds(pl.multiple_of(rb, S), M.n), :] = res[p * hr:p * hr + M.n]
                Gc[pl.ds(rb + M.n, 1), :] = res[p * hr + M.n:p * hr + M.n + 1]

    KR, KA = 48, 32

    def gather_coarsest():
        hr, cells = L3.n + S, L3.n + 1
        parts = [lane_dot(T2[pl.ds(p * S * hr, n * hr), :], weights(L3.ni, False, L3.ni * (2 * cy + p)))
                 for p, n in ((0, S), (1, S), (2, 1))]
        for p in range(S):
            x = parts[0][p * hr:p * hr + cells] + parts[1][p * hr:p * hr + cells]
            x = x + parts[2][:cells] if p == 0 else x
            S3[pl.ds(p * cells, cells), :] = x * F32(1 / 16)
        cps = [pltpu.make_async_remote_copy(src_ref=S3, dst_ref=R3.at[n], send_sem=cs.at[12 + n],
                                            recv_sem=cr.at[12 + n], device_id=to, device_id_type=MESH)
               for n, to in enumerate((py, pz, pyz))]
        for cp in cps:
            cp.start()
        for cp in cps:
            cp.wait()
        low, high = S + L3.n * cz, S + L3.n * (1 - cz)
        for p in range(S):
            rows = pl.ds(p * cells, cells)
            G3[pl.ds(p * KR + low, cells), :] += S3[rows, :] + R3[0, rows, :]
            G3[pl.ds(p * KR + high, cells), :] += R3[1, rows, :] + R3[2, rows, :]
            G3[pl.ds(p * KR + S + KA, 1), :] = zero[:1]

    def coarsest_pass(src, visit):
        lanes = lax.broadcasted_iota(jnp.int32, (KA, W), 1)
        cell = lanes % KA
        at = lambda p: pl.ds(p * KR + S, KA)
        for p in range(S):
            c = src[at(p), :]
            left = jnp.where(cell == 0, 0.0, pltpu.roll(c, 1, 1))
            right = jnp.where(cell == KA - 1, 0.0, pltpu.roll(c, LAST, 1))
            lo = src[at(p - 1), :] if p else jnp.where(lanes < KA, 0.0, pltpu.roll(src[at(S - 1), :], KA, 1))
            hi = src[at(p + 1), :] if p < S - 1 else jnp.where(lanes < W - KA, pltpu.roll(src[at(0), :], W - KA, 1), 0.0)
            total = (lo + hi) + (src[pl.ds(p * KR + S - 1, KA), :] + src[pl.ds(p * KR + S + 1, KA), :]) + (left + right)
            visit(at(p), c, total)

    def solve_coarsest():
        def first(rows, c, total):
            V3[rows, :] = (12.0 * c + total) * F32(1 / 81)
        coarsest_pass(G3, first)

        @pl.loop(0, 7)
        def _(s):
            for V, W_ in ((V3, W3), (W3, V3)):
                def visit(rows, c, total):
                    W_[rows, :] = (3.0 * c + (total + G3[rows, :])) * ninth
                coarsest_pass(V, visit)

    def spread_coarsest():
        def plane(j):
            return pl.ds(pl.multiple_of((L3.pj + j) * L3.nk + L3.kp - S, S), KA)
        E[plane(L3.n), :] = jnp.zeros((KA, W), F32)
        x = jnp.concatenate([V3[pl.ds(pl.multiple_of(p * KR + L3.n * cz, S), KA), :] for p in range(S)], axis=0)
        for q in (0, 1, 2 - 3 * cy):
            y = lane_dot(x, weights(L3.ni, True, L3.ni * (2 * cy + q)))
            for p in range(S):
                E[plane(q * S + p), :] = y[p * KA:p * KA + KA]

    def spread_lanes(M, e):
        w = weights(M.ni, True)
        j0 = M.pj - EXTRA * cy

        @pl.loop(0, (M.n + EXTRA + 1) // M.group)
        def _(g):
            rows = pl.ds(pl.multiple_of((j0 + g * M.group) * M.nk, S), M.group * M.nk)
            E[rows, :] = lane_dot(e[rows, :], w)

    def prolong_coarse(L, M, V):
        j0 = M.pj - EXTRA * cy

        @pl.loop(0, M.n + EXTRA)
        def _(p):
            jc = j0 + p - M.pj
            fb = (L.pj + 2 * jc) * L.nk + L.kp
            eb = (j0 + p) * M.nk + M.kp
            for kc, rows in ((0, M.n), (M.n * (1 - cz) - 4 * cz, 4)):
                a, b = E[pl.ds(eb + kc, rows), :], E[pl.ds(eb + kc + 1, rows), :]
                c, d = E[pl.ds(eb + M.nk + kc, rows), :], E[pl.ds(eb + M.nk + kc + 1, rows), :]
                ab = a + b
                f = fb + 2 * kc
                V[pl.ds(f, rows, stride=2), :] += a
                V[pl.ds(f + 1, rows, stride=2), :] += 0.5 * ab
                V[pl.ds(f + L.nk, rows, stride=2), :] += 0.5 * (a + c)
                V[pl.ds(f + L.nk + 1, rows, stride=2), :] += 0.25 * (ab + (c + d))

    def from_level1():
        @pl.loop(0, 13)
        def _(jo):
          for q in range(5):
            jc = jo * 5 + q
            base = (jc + L1.pj) * L1.nk + L1.kp
            a, b = V1[pl.ds(pl.multiple_of(base, S), 64), :], V1[pl.ds(base + 1, 64), :]
            TS[q, pl.ds(S, 64, stride=2), :] = a
            TS[q, pl.ds(S + 1, 64, stride=2), :] = 0.5 * (a + b)
            X2[pl.ds(jc, W, stride=XR), :] = jnp.transpose(TS[q, pl.ds(S, W), :])

    def prolong_level0():
        zero_turned(AT, (-1, W))

        def done(c):
            first_chunk(1, c)
            send(1, chunk_of(c))

        @pl.loop(0, NG)
        def _(g):
            i0 = place(g)
            turn(1, place((g + NG - 1) % NG), GP)
            for q in range(GP // 2):
                half = W // 2
                xb = (i0 // 2 + q + half * cx) * XR
                a, b = X2[pl.ds(xb, half), :], X2[pl.ds(xb + 1, half), :]
                cc, d = X2[pl.ds(xb + XR, half), :], X2[pl.ds(xb + XR + 1, half), :]
                ab = a + b
                f = (i0 + 2 * q + 1) * PR + S
                for shift, value in ((0, a), (1, 0.5 * ab), (PR, 0.5 * (a + cc)), (PR + 1, 0.25 * (ab + (cc + d)))):
                    rows = pl.ds(f + shift, half, stride=2)
                    B2[rows, :] = A2[rows, :] + value
            after_chunk(g, done)
        turn(1, place(NG - 1), GP)
        done(NC - 1)

    start_level0()
    sweep_pass(0, True, False)
    sweep_pass(1, False, False)
    residual_pass()
    to_level1()
    wide_exchange(L1, G1, SY1, RY1, SZ1, RZ1, SD1, RD1, 6)
    first_two(L1, G1, V1)
    restrict_coarse(L1, L2, G1, V1, W1)
    restrict_lanes(L2, G2)
    wide_exchange(L2, G2, SY2, RY2, SZ2, RZ2, SD2, RD2, 9)
    first_two(L2, G2, V2)
    restrict_coarse(L2, L3, G2, V2, W2)
    gather_coarsest()
    solve_coarsest()
    spread_coarsest()
    prolong_coarse(L2, L3, V2)
    smooth(L2, G2, V2, W2)
    smooth(L2, G2, W2, V2)
    spread_lanes(L2, V2)
    prolong_coarse(L1, L2, V1)
    smooth(L1, G1, V1, W1)
    smooth(L1, G1, W1, V1)
    from_level1()
    prolong_level0()
    sweep_pass(1, False, False)
    sweep_pass(0, False, True)
    for c in range(NC // 2, NC):
        receive(0, chunk_of(c))


def close(B, A, AT, F, out_hbm, O, KS, sems):
    cx = lax.axis_index('sx')

    def chunk_of(c):
        return c * cx + (NC - 1 - c) * (1 - cx)

    def place(g):
        return chunk_of(g // GC) * CP + g % GC * GP

    def rows(i, shift=0, count=W):
        return pl.ds(i * PR + S + shift, count)

    def store(c):
        planes = pl.ds(chunk_of(c) * CP, CP)
        src = B.at[pl.ds(chunk_of(c) * CP + 1, CP), pl.ds(S, W), :] if c < NC // 2 else O.at[pl.ds((c - NC // 2) * CP, CP)]
        return pltpu.make_async_copy(src, out_hbm.at[planes], sems.at[c])
    for c in range(NC // 2):
        store(c).start()
    src = A.reshape(A.shape[0] * PR, W)

    def side_sums(i0):
        for q in range(GP):
            KS[pl.ds(q * W, W), :] = jnp.transpose(AT[rows(i0 + q, -1), :] + AT[rows(i0 + q, 1), :])
    side_sums(place(NG // 2))
    for c in range(NC // 2, NC):
        @pl.loop(c * GC, (c + 1) * GC)
        def _(g):
            i0 = place(g)
            base = pl.multiple_of(i0 * PR, S)

            def at(q, r):
                return pl.ds(base + (q * PR + S + r), RB)
            for t in range(W // RB):
                r = t * RB
                um, uc = src[at(0, r), :], src[at(1, r), :]
                for q in range(GP):
                    un = src[at(q + 2, r), :]
                    total = (um + un) + (src[at(q + 1, r - 1), :] + src[at(q + 1, r + 1), :]) + KS[pl.ds(q * W + r, RB), :]
                    new = (3.0 * uc + (total + F[i0 + q, pl.ds(r, RB), :])) * F32(1 / 9)
                    O[(g - NG // 2) * GP + q, pl.ds(r, RB), :] = new
                    um, uc = uc, un
            side_sums(place((g + 1) % NG))
        store(c).start()
    for c in range(NC):
        store(c).wait()


def solution(mesh):
    spec = P(('dp', 'sx'), 'sy', 'sz')

    def local(f, u):
        size = 2 * f.shape[1]
        h2 = 1.0 / float((size + 1) ** 2)
        vm = lambda *s: pltpu.VMEM(s, F32)
        scratch = [vm(N * PR, W), vm(129, XR, W),
                   vm(XR, W), vm(XR, W), vm(5, 136, W), vm(GP * W, W), vm(2, N, W), vm(2, N, W), vm(2, N, W), vm(2, N, W)]
        scratch += [vm(L1.rows, W)] * 2 + [vm(L2.rows, W)] * 3 + [vm(S * 48, W)] * 3
        for L in (L1, L2):
            z = up8((L.n + 1) * L.h)
            scratch += [vm(L.h * (L.n + S), W)] * 2 + [vm(z, W)] * 2 + [vm(L.h * S, W)] * 2
        scratch += [vm(S * (L3.n + 1), W), vm(3, S * (L3.n + 1), W)]
        dma = pltpu.SemaphoreType.DMA
        scratch += [dma((2, NC)), dma((2,)), dma((2,)), dma((2, NC)), dma((2, NC)), dma((2, NC)), dma((2, NC)),
                    dma((15,)), dma((15,))]
        resident = [vm(130, PR, W), vm(130, PR, W), vm(N * PR, W), vm(N, N, W)]
        used = 4 * sum(math.prod(x.shape) for x in resident)
        kept = pl.pallas_call(
            functools.partial(body, h2),
            out_shape=resident,
            in_specs=[pl.BlockSpec(memory_space=pl.ANY)] * 2,
            out_specs=[pl.BlockSpec(memory_space=pltpu.VMEM)] * len(resident),
            scratch_shapes=scratch,
            compiler_params=pltpu.CompilerParams(collective_id=0, has_side_effects=True, vmem_limit_bytes=67043328 - used),
        )(f, u)
        kept = [pltpu.with_memory_space_constraint(x, pltpu.VMEM) for x in kept]
        return pl.pallas_call(
            close,
            out_shape=jax.ShapeDtypeStruct(f.shape, F32),
            in_specs=[pl.BlockSpec(memory_space=pltpu.VMEM)] * len(kept),
            out_specs=pl.BlockSpec(memory_space=pl.ANY),
            scratch_shapes=[vm(N // 2, N, W), vm(GP * W, W), dma((NC,))],
            compiler_params=pltpu.CompilerParams(vmem_limit_bytes=67043328 - used),
        )(*kept)

    def run(rhs_grid, u_start):
        return jax.shard_map(local, mesh=mesh, in_specs=(spec, spec), out_specs=spec, check_vma=False)(rhs_grid, u_start)
    return run
```

```python
import functools
import math
import jax
import jax.numpy as jnp
from jax import lax
from jax.experimental import pallas as pl
from jax.experimental.pallas import tpu as pltpu
from jax.sharding import PartitionSpec as P

N = 128
PR = 144
NC = 8
XR = 72
CP = N // NC
GP = 16
GC = CP // GP
NG = N // GP
RB = 32
S, W = 8, 128
LAST = W - 1
MESH = pl.DeviceIdType.MESH
F32 = jnp.float32
HI = lax.Precision.HIGHEST


class Lev:
    def __init__(self, n, h, pj, kp, hb, ni, region, unroll, group):
        self.n, self.h, self.pj, self.kp, self.hb, self.ni = n, h, pj, kp, hb, ni
        self.region, self.unroll, self.group = region, unroll, group
        self.size_own = 16
        self.nk = n + 2 * kp
        self.planes = n + 2 * pj
        self.rows = self.planes * self.nk


L1 = Lev(64, 4, 6, 8, 8, 128, 68, 17, 1)
L2 = Lev(32, 5, 10, 8, 8, 64, 40, 20, 12)
L3 = Lev(16, 16, 18, 16, 16, 32, 32, 8, 10)
EXTRA = 3


def up8(x):
    return (x + 7) // 8 * 8


def eight(r):
    return pl.ds(r, S)


def body(h2, f_hbm, u_hbm, B, A, AT, F, BT, X, XP, RXP, TS, KS, PZ, RZ, PY, RY,
         V1, W1, G2, V2, W2, G3, V3, W3,
         SY1, RY1, SZ1, RZ1, SD1, RD1, SY2, RY2, SZ2, RZ2, SD2, RD2, S3, R3,
         ld, xs, xr, zs, zr, ys, yr, cs, cr):
    cx, cy, cz = lax.axis_index('sx'), lax.axis_index('sy'), lax.axis_index('sz')
    ninth = F32(1.0 / 9.0)
    px, py, pz = {'sx': 1 - cx}, {'sy': 1 - cy}, {'sz': 1 - cz}
    pyz = {**py, **pz}

    def flat(ref):
        return ref.reshape(ref.shape[0] * ref.shape[1], ref.shape[2])

    A2, B2, X2 = flat(A), flat(B), flat(X)
    flats, turned = (A2, B2), (AT, BT)
    G1, T2 = AT.at[pl.ds(0, L1.rows), :], AT.at[pl.ds(L1.rows, 33 * 40), :]
    E = AT.at[pl.ds(L1.rows + 33 * 40, max(L2.rows, L3.rows)), :]

    def chunk_of(c):
        return c * cx + (NC - 1 - c) * (1 - cx)

    def block(i, shift=0, count=W):
        if isinstance(shift, int) and shift % S == 0:
            return pl.ds(pl.multiple_of(i * PR + S + shift, S), count)
        return pl.ds(i * PR + S + shift, count)

    def load(which, k):
        planes = pl.ds(k * CP, CP)
        src, dst = ((u_hbm, A.at[pl.ds(k * CP + 1, CP), pl.ds(S, W), :]), (f_hbm, F.at[planes]))[which]
        return pltpu.make_async_copy(src.at[planes], dst, ld.at[which, k])
    for c in range(NC):
        load(0, chunk_of(c)).start()

    barrier = pltpu.get_barrier_semaphore()
    for p in (px, py, pz, pyz):
        pl.semaphore_signal(barrier, inc=1, device_id=p, device_id_type=MESH)
    pl.semaphore_wait(barrier, 4)

    zero = jnp.zeros((S, W), F32)

    def zero_rows(ref2, count):
        @pl.loop(0, count // 64)
        def _(t):
            ref2[pl.ds(pl.multiple_of(t * 64, 64), 64), :] = jnp.zeros((64, W), F32)
        if count % 64:
            ref2[pl.ds(count // 64 * 64, count % 64), :] = jnp.zeros((count % 64, W), F32)
    for ref in (V1, W1, G2, V2, W2, G3, V3, W3):
        zero_rows(ref, ref.shape[0])

    for buf in flats:
        buf[block(129 * cx, -S, PR), :] = jnp.zeros((PR, W), F32)
        for side in (-1, W):
            buf[pl.ds(PR + S + side, N, stride=PR), :] = jnp.zeros((N, W), F32)

    def zero_turned(buf, sides):
        for side in sides:
            buf[pl.ds(S + side, N, stride=PR), :] = jnp.zeros((N, W), F32)
    zero_turned(AT, (-1, W))
    zero_turned(BT, (-1, W))

    @pl.loop(0, XR // S)
    def _(t):
        X[W, eight(pl.multiple_of(t * S, S)), :] = zero
    for q in range(5):
        TS[q, eight(0), :] = zero

    def x_copy(par):
        return pltpu.make_async_remote_copy(
            src_ref=flats[par].at[block(W - LAST * cx), :], dst_ref=flats[par].at[block(129 * cx), :],
            send_sem=xs.at[par], recv_sem=xr.at[par], device_id=px, device_id_type=MESH)

    def side_copy(par, k, src, dst, ssem, rsem, to):
        planes = pl.ds(pl.multiple_of(k * CP, S), CP)
        return pltpu.make_async_remote_copy(
            src_ref=src.at[par, planes, :], dst_ref=dst.at[par, planes, :],
            send_sem=ssem.at[par, k], recv_sem=rsem.at[par, k], device_id=to, device_id_type=MESH)

    def side_copies(par, k):
        return side_copy(par, k, PY, RY, ys, yr, py), side_copy(par, k, PZ, RZ, zs, zr, pz)

    def send(par, k):
        planes = pl.ds(k * CP, CP)
        PY[par, planes, :] = flats[par][pl.ds((k * CP + 1) * PR + S + LAST * (1 - cy), CP, stride=PR), :]
        PZ[par, planes, :] = turned[par][pl.ds(k * CP * PR + S + LAST * (1 - cz), CP, stride=PR), :]
        for cp in side_copies(par, k):
            cp.start()

    def receive(par, k):
        for cp in side_copies(par, k):
            cp.wait()
        planes = pl.ds(k * CP, CP)
        flats[par][pl.ds((k * CP + 1) * PR + S + W - (W + 1) * cy, CP, stride=PR), :] = RY[par, planes, :]
        turned[par][pl.ds(k * CP * PR + S + W - (W + 1) * cz, CP, stride=PR), :] = RZ[par, planes, :]

    def place(g):
        return chunk_of(g // GC) * CP + g % GC * GP

    def turn(par, i0, count):
        base = pl.multiple_of(i0 * PR, S)
        for q in range(count):
            turned[par][pl.ds(base + (q * PR + S), W), :] = jnp.transpose(flats[par][pl.ds(base + ((q + 1) * PR + S), W), :])

    def side_sums(par, i0):
        base = pl.multiple_of(i0 * PR, S)
        for q in range(GP):
            lo, hi = (turned[par][pl.ds(base + (q * PR + S + d), W), :] for d in (-1, 1))
            KS[pl.ds(q * W, W), :] = jnp.transpose(lo + hi)

    def after_chunk(g, done):
        @pl.when((g % GC == 0) & (g > 0))
        def _():
            done(g // GC - 1)

    def first_chunk(par, c):
        @pl.when(c == 0)
        def _():
            x_copy(par).start()

    def stencil_pass(par, visit, dst, done, arrive=None, groups=NG):
        src = flats[par]
        x_copy(par).wait()
        receive(par, chunk_of(0))
        side_sums(par, place(0))
        if arrive is not None:
            arrive(chunk_of(0))

        @pl.loop(0, groups)
        def _(g):
            @pl.when((g % GC == GC - 1) & (g < groups - 1))
            def _():
                receive(par, chunk_of(g // GC + 1))
                if arrive is not None:
                    arrive(chunk_of(g // GC + 1))
            i0 = place(g)
            if dst is not None:
                turn(dst, place((g + NG - 1) % NG), GP)
            base = pl.multiple_of(i0 * PR, S)

            def at(q, r):
                return pl.ds(base + (q * PR + S + r), RB)
            for t in range(W // RB):
                r = t * RB
                um, uc = src[at(0, r), :], src[at(1, r), :]
                for q in range(GP):
                    un = src[at(q + 2, r), :]
                    total = (um + un) + (src[at(q + 1, r - 1), :] + src[at(q + 1, r + 1), :]) + KS[pl.ds(q * W + r, RB), :]
                    visit(i0, at, q, r, uc, total)
                    um, uc = uc, un
            side_sums(par, place((g + 1) % NG))
            if done is not None:
                after_chunk(g, done)
        if dst is not None:
            turn(dst, place(NG - 1), GP)
        if done is not None:
            done(NC - 1)

    def sweep_pass(par, first, last):
        def visit(i0, at, q, r, centre, total):
            fs = F[i0 + q, pl.ds(r, RB), :]
            if first:
                fs = fs * F32(h2)
                F[i0 + q, pl.ds(r, RB), :] = fs
            flats[1 - par][at(q + 1, r), :] = (3.0 * centre + (total + fs)) * ninth

        def done(c):
            k = chunk_of(c)
            first_chunk(1 - par, c)
            send(1 - par, k)
        stencil_pass(par, visit, None if last else 1 - par, None if last else done,
                     (lambda k: load(1, k).wait()) if first else None, NG // 2 if last else NG)

    def start_level0():
        @pl.loop(0, NC)
        def _(c):
            k = chunk_of(c)
            load(0, k).wait()
            load(1, k).start()

            @pl.loop(0, CP // S)
            def _(t):
                turn(0, k * CP + t * S, S)
            first_chunk(0, c)
            send(0, k)

    def residual_pass():
        def visit(i0, at, q, r, centre, total):
            BT[at(q, r), :] = F[i0 + q, pl.ds(r, RB), :] - 6.0 * centre + total
        stencil_pass(0, visit, None, None)
        zero_turned(BT, (-1, W, W + 1))

    def restrict_rows(jc, count):
        def line(plane):
            lo, mid, hi = (BT[pl.ds(plane * PR + S + 2 * jc + d, count, stride=2), :] for d in (-1, 0, 1))
            return (lo + hi) + 2.0 * mid

        def put(i, value):
            X2[pl.ds((i + 64 * cx) * XR + jc, count), :] = value

        def step(t, last):
            for q in range(3):
                i = 1 + t * 3 + q
                odd = line(2 * i + 1)
                put(i, (last + odd) + 2.0 * line(2 * i))
                last = odd
            return last
        odd = line(1)
        put(0, odd + 2.0 * line(0))
        XP[pl.ds(jc, count), :] = lax.fori_loop(0, 21, step, odd)

    JP = (24, 24, 17)

    def to_level1():
        own = pl.ds(64 * cx, 64)
        copies = []
        for m, count in enumerate(JP):
            jc = m * JP[0]
            restrict_rows(jc, count)
            part, rows = X.at[own, pl.ds(jc, JP[0]), :], pl.ds(jc, JP[0])
            pair = [pltpu.make_async_remote_copy(src_ref=src, dst_ref=dst, send_sem=cs.at[2 * m + n], recv_sem=cr.at[2 * m + n],
                                                 device_id=px, device_id_type=MESH)
                    for n, (src, dst) in enumerate(((XP.at[rows, :], RXP.at[rows, :]), (part, part)))]
            for cp in pair:
                cp.start()
            copies.append(pair)
        zero_rows(AT, L1.rows)

        def tile(jc, q):
            TS[q, pl.ds(S, W), :] = jnp.transpose(X2[pl.ds(jc, W, stride=XR), :])
            base = (jc + L1.pj) * L1.nk + L1.kp
            lo, mid, hi = (TS[q, pl.ds(S + d, 64, stride=2), :] for d in (-1, 0, 1))
            G1[pl.ds(pl.multiple_of(base, S), 64), :] = ((lo + hi) + 2.0 * mid) * F32(1 / 16)
            G1[pl.ds(base + 64, 1), :] = TS[q, pl.ds(135, 1), :] * F32(1 / 16)

        for m, pair in enumerate(copies):
            for cp in pair:
                cp.wait()
            jc = m * JP[0]
            rows = pl.ds(jc, JP[0])
            X2[pl.ds(64 * XR + jc, JP[0]), :] += jnp.where(cx == 0, XP[rows, :], RXP[rows, :])

            @pl.loop(0, JP[m] // 4)
            def _(jo):
                for q in range(4):
                    tile(jc + jo * 4 + q, q)
        tile(64, 4)

    def wide_exchange(L, G, SY, RY_, SZ, RZ_, SD, RD, s):
        cnt, wide = L.h, L.n + S
        js, ks = (L.n + 1 - cnt) * (1 - cy) + L.pj, (L.n + 1 - cnt) * (1 - cz) + L.kp
        jd, kd = L.n * (1 - cy) + (1 - cnt) * cy + L.pj, L.n * (1 - cz) + (1 - cnt) * cz + L.kp
        for p in range(cnt):
            SY[pl.ds(p * wide, wide), :] = G[pl.ds(pl.multiple_of((js + p) * L.nk + L.kp, S), wide), :]
            SD[pl.ds(p * S, cnt), :] = G[pl.ds((js + p) * L.nk + ks, cnt), :]
        cps = [pltpu.make_async_remote_copy(src_ref=src, dst_ref=dst, send_sem=cs.at[s + n], recv_sem=cr.at[s + n],
                                            device_id=to, device_id_type=MESH)
               for n, (src, dst, to) in enumerate(((SY, RY_, py), (SD, RD, pyz), (SZ, RZ_, pz)))]
        cps[0].start()
        cps[1].start()

        @pl.loop(0, L.n + 1)
        def _(p):
            SZ[pl.ds(p * cnt, cnt), :] = G[pl.ds((L.pj + p) * L.nk + ks, cnt), :]
        cps[2].start()
        for cp in cps:
            cp.wait()
        for p in range(cnt):
            G[pl.ds(pl.multiple_of((jd + p) * L.nk + L.kp, S), wide), :] += RY_[pl.ds(p * wide, wide), :]
            G[pl.ds((jd + p) * L.nk + kd, cnt), :] += RD[pl.ds(p * S, cnt), :]

        @pl.loop(0, L.n + 1)
        def _(p):
            G[pl.ds((L.pj + p) * L.nk + kd, cnt), :] += RZ_[pl.ds(p * cnt, cnt), :]
        last = L.kp - 1 + (L.n + 1) * cz

        @pl.loop(0, L.region)
        def _(p):
            G[pl.ds((L.pj - (L.region - L.n) * cy + p) * L.nk + last, 1), :] = zero[:1]
        G[pl.ds(pl.multiple_of((L.pj - 1 + (L.n + 1) * cy) * L.nk, S), L.nk), :] = jnp.zeros((L.nk, W), F32)

    def coarse_pass(L, src, visit, own=False):
        j0 = L.pj if own else L.pj - (L.region - L.n) * cy
        k0 = L.kp if own else L.kp - L.hb * cz
        count = L.n if own else L.n + L.hb
        planes = L.n if own else L.region
        size = L.size_own if own else L.unroll
        groups = planes // size
        lanes = lax.broadcasted_iota(jnp.int32, (count, W), 1)

        def place(g):
            return pl.multiple_of((j0 + g * size) * L.nk + k0, S)

        def sides(g):
            out = []
            base = place(g)
            for p in range(size):
                c = src[pl.ds(base + p * L.nk, count), :]
                out.append(jnp.where(lanes == 0, 0.0, pltpu.roll(c, 1, 1)) + jnp.where(
                    lanes == L.ni - 1, 0.0, pltpu.roll(c, LAST, 1)))
            return out

        def keep(sums):
            for p in range(size):
                KS[pl.ds(p * count, count), :] = sums[p]
        keep(sides(0))

        @pl.loop(0, groups)
        def _(g):
            later = sides((g + 1) % groups)
            base = place(g)
            for p in range(size):
                lo, hi, below, above, c = (src[pl.ds(base + (p * L.nk + d), count), :] for d in (-L.nk, L.nk, -1, 1, 0))
                visit(pl.ds(base + p * L.nk, count), c, (lo + hi) + (below + above) + KS[pl.ds(p * count, count), :])
            keep(later)

    def first_two(L, G, V):
        def visit(rows, c, total):
            V[rows, :] = (12.0 * c + total) * F32(1 / 81)
        coarse_pass(L, G, visit)

    def smooth(L, G, V, W_):
        def visit(rows, c, total):
            W_[rows, :] = (3.0 * c + (total + G[rows, :])) * ninth
        coarse_pass(L, V, visit)

    def weights(ni, up, offset=0):
        a = lax.broadcasted_iota(jnp.int32, (W, W), 0)
        b = lax.broadcasted_iota(jnp.int32, (W, W), 1)
        fine, coarse = (b, a - offset) if up else (a, b - offset)
        near = (fine == 2 * coarse + 1) | (fine == 2 * coarse - 1)
        w = jnp.where(fine == 2 * coarse, 1.0, 0.0) + jnp.where(near, 0.5, 0.0)
        return jnp.where((coarse >= 0) & (coarse < ni) & (fine < 2 * ni), w if up else 2.0 * w, 0.0).astype(F32)

    def lane_dot(x, w):
        return jnp.dot(x, w, precision=HI, preferred_element_type=F32)

    def restrict_coarse(L, M, G, V, W_):
        def visit(rows, c, total):
            W_[rows, :] = G[rows, :] - 6.0 * c + total
        coarse_pass(L, V, visit, True)
        for side in (L.pj - 1, L.pj + L.n, L.pj + L.n + 1):
            W_[pl.ds(side * L.nk, L.nk), :] = jnp.zeros((L.nk, W), F32)

        @pl.loop(0, L.n)
        def _(p):
            base = (L.pj + p) * L.nk + L.kp
            W_[eight(pl.multiple_of(base - S, S)), :] = zero
            W_[eight(pl.multiple_of(base + L.n, S)), :] = zero

        @pl.loop(0, M.n + 1)
        def _(p):
            base = (L.pj + 2 * p) * L.nk + L.kp
            rows = M.n + 4
            sums = []
            for dj in (-1, 0, 1):
                lo, mid, hi = (W_[pl.ds(base + dj * L.nk + d, rows, stride=2), :] for d in (-1, 0, 1))
                sums.append((lo + hi) + 2.0 * mid)
            T2[pl.ds(p * (M.n + S), rows), :] = (sums[0] + sums[2]) + 2.0 * sums[1]

    def restrict_lanes(M, Gc):
        hr = M.n + S
        group = 11
        w = weights(M.ni, False)

        @pl.loop(0, (M.n + 1) // group)
        def _(g):
            t0 = pl.multiple_of(g * group * hr, S)
            res = lane_dot(T2[pl.ds(t0, group * hr), :], w) * F32(1 / 16)
            for p in range(group):
                rb = (M.pj + g * group + p) * M.nk + M.kp
                Gc[pl.ds(pl.multiple_of(rb, S), M.n), :] = res[p * hr:p * hr + M.n]
                Gc[pl.ds(rb + M.n, 1), :] = res[p * hr + M.n:p * hr + M.n + 1]

    KR, KA = 48, 32

    def gather_coarsest():
        hr, cells = L3.n + S, L3.n + 1
        parts = [lane_dot(T2[pl.ds(p * S * hr, n * hr), :], weights(L3.ni, False, L3.ni * (2 * cy + p)))
                 for p, n in ((0, S), (1, S), (2, 1))]
        for p in range(S):
            x = parts[0][p * hr:p * hr + cells] + parts[1][p * hr:p * hr + cells]
            x = x + parts[2][:cells] if p == 0 else x
            S3[pl.ds(p * cells, cells), :] = x * F32(1 / 16)
        cps = [pltpu.make_async_remote_copy(src_ref=S3, dst_ref=R3.at[n], send_sem=cs.at[12 + n],
                                            recv_sem=cr.at[12 + n], device_id=to, device_id_type=MESH)
               for n, to in enumerate((py, pz, pyz))]
        for cp in cps:
            cp.start()
        for cp in cps:
            cp.wait()
        low, high = S + L3.n * cz, S + L3.n * (1 - cz)
        for p in range(S):
            rows = pl.ds(p * cells, cells)
            G3[pl.ds(p * KR + low, cells), :] += S3[rows, :] + R3[0, rows, :]
            G3[pl.ds(p * KR + high, cells), :] += R3[1, rows, :] + R3[2, rows, :]
            G3[pl.ds(p * KR + S + KA, 1), :] = zero[:1]

    def coarsest_pass(src, visit):
        lanes = lax.broadcasted_iota(jnp.int32, (KA, W), 1)
        cell = lanes % KA
        at = lambda p: pl.ds(p * KR + S, KA)
        for p in range(S):
            c = src[at(p), :]
            left = jnp.where(cell == 0, 0.0, pltpu.roll(c, 1, 1))
            right = jnp.where(cell == KA - 1, 0.0, pltpu.roll(c, LAST, 1))
            lo = src[at(p - 1), :] if p else jnp.where(lanes < KA, 0.0, pltpu.roll(src[at(S - 1), :], KA, 1))
            hi = src[at(p + 1), :] if p < S - 1 else jnp.where(lanes < W - KA, pltpu.roll(src[at(0), :], W - KA, 1), 0.0)
            total = (lo + hi) + (src[pl.ds(p * KR + S - 1, KA), :] + src[pl.ds(p * KR + S + 1, KA), :]) + (left + right)
            visit(at(p), c, total)

    def solve_coarsest():
        def first(rows, c, total):
            V3[rows, :] = (12.0 * c + total) * F32(1 / 81)
        coarsest_pass(G3, first)

        @pl.loop(0, 7)
        def _(s):
            for V, W_ in ((V3, W3), (W3, V3)):
                def visit(rows, c, total):
                    W_[rows, :] = (3.0 * c + (total + G3[rows, :])) * ninth
                coarsest_pass(V, visit)

    def spread_coarsest():
        def plane(j):
            return pl.ds(pl.multiple_of((L3.pj + j) * L3.nk + L3.kp - S, S), KA)
        E[plane(L3.n), :] = jnp.zeros((KA, W), F32)
        x = jnp.concatenate([V3[pl.ds(pl.multiple_of(p * KR + L3.n * cz, S), KA), :] for p in range(S)], axis=0)
        for q in (0, 1, 2 - 3 * cy):
            y = lane_dot(x, weights(L3.ni, True, L3.ni * (2 * cy + q)))
            for p in range(S):
                E[plane(q * S + p), :] = y[p * KA:p * KA + KA]

    def spread_lanes(M, e):
        w = weights(M.ni, True)
        j0 = M.pj - EXTRA * cy

        @pl.loop(0, (M.n + EXTRA + 1) // M.group)
        def _(g):
            rows = pl.ds(pl.multiple_of((j0 + g * M.group) * M.nk, S), M.group * M.nk)
            E[rows, :] = lane_dot(e[rows, :], w)

    def prolong_coarse(L, M, V):
        j0 = M.pj - EXTRA * cy

        @pl.loop(0, M.n + EXTRA)
        def _(p):
            jc = j0 + p - M.pj
            fb = (L.pj + 2 * jc) * L.nk + L.kp
            eb = (j0 + p) * M.nk + M.kp
            for kc, rows in ((0, M.n), (M.n * (1 - cz) - 4 * cz, 4)):
                a, b = E[pl.ds(eb + kc, rows), :], E[pl.ds(eb + kc + 1, rows), :]
                c, d = E[pl.ds(eb + M.nk + kc, rows), :], E[pl.ds(eb + M.nk + kc + 1, rows), :]
                ab = a + b
                f = fb + 2 * kc
                V[pl.ds(f, rows, stride=2), :] += a
                V[pl.ds(f + 1, rows, stride=2), :] += 0.5 * ab
                V[pl.ds(f + L.nk, rows, stride=2), :] += 0.5 * (a + c)
                V[pl.ds(f + L.nk + 1, rows, stride=2), :] += 0.25 * (ab + (c + d))

    def from_level1():
        @pl.loop(0, 13)
        def _(jo):
          for q in range(5):
            jc = jo * 5 + q
            base = (jc + L1.pj) * L1.nk + L1.kp
            a, b = V1[pl.ds(pl.multiple_of(base, S), 64), :], V1[pl.ds(base + 1, 64), :]
            TS[q, pl.ds(S, 64, stride=2), :] = a
            TS[q, pl.ds(S + 1, 64, stride=2), :] = 0.5 * (a + b)
            X2[pl.ds(jc, W, stride=XR), :] = jnp.transpose(TS[q, pl.ds(S, W), :])

    def prolong_level0():
        zero_turned(AT, (-1, W))

        def done(c):
            first_chunk(1, c)
            send(1, chunk_of(c))

        @pl.loop(0, NG)
        def _(g):
            i0 = place(g)
            turn(1, place((g + NG - 1) % NG), GP)
            for q in range(GP // 2):
                half = W // 2
                xb = (i0 // 2 + q + half * cx) * XR
                a, b = X2[pl.ds(xb, half), :], X2[pl.ds(xb + 1, half), :]
                cc, d = X2[pl.ds(xb + XR, half), :], X2[pl.ds(xb + XR + 1, half), :]
                ab = a + b
                f = (i0 + 2 * q + 1) * PR + S
                for shift, value in ((0, a), (1, 0.5 * ab), (PR, 0.5 * (a + cc)), (PR + 1, 0.25 * (ab + (cc + d)))):
                    rows = pl.ds(f + shift, half, stride=2)
                    B2[rows, :] = A2[rows, :] + value
            after_chunk(g, done)
        turn(1, place(NG - 1), GP)
        done(NC - 1)

    start_level0()
    sweep_pass(0, True, False)
    sweep_pass(1, False, False)
    residual_pass()
    to_level1()
    wide_exchange(L1, G1, SY1, RY1, SZ1, RZ1, SD1, RD1, 6)
    first_two(L1, G1, V1)
    restrict_coarse(L1, L2, G1, V1, W1)
    restrict_lanes(L2, G2)
    wide_exchange(L2, G2, SY2, RY2, SZ2, RZ2, SD2, RD2, 9)
    first_two(L2, G2, V2)
    restrict_coarse(L2, L3, G2, V2, W2)
    gather_coarsest()
    solve_coarsest()
    spread_coarsest()
    prolong_coarse(L2, L3, V2)
    smooth(L2, G2, V2, W2)
    smooth(L2, G2, W2, V2)
    spread_lanes(L2, V2)
    prolong_coarse(L1, L2, V1)
    smooth(L1, G1, V1, W1)
    smooth(L1, G1, W1, V1)
    from_level1()
    prolong_level0()
    sweep_pass(1, False, False)
    sweep_pass(0, False, True)
    for c in range(NC // 2, NC):
        receive(0, chunk_of(c))


def close(B, A, AT, F, out_hbm, O, KS, sems):
    cx = lax.axis_index('sx')

    def chunk_of(c):
        return c * cx + (NC - 1 - c) * (1 - cx)

    def place(g):
        return chunk_of(g // GC) * CP + g % GC * GP

    def rows(i, shift=0, count=W):
        return pl.ds(i * PR + S + shift, count)

    def store(c):
        planes = pl.ds(chunk_of(c) * CP, CP)
        src = B.at[pl.ds(chunk_of(c) * CP + 1, CP), pl.ds(S, W), :] if c < NC // 2 else O.at[pl.ds((c - NC // 2) * CP, CP)]
        return pltpu.make_async_copy(src, out_hbm.at[planes], sems.at[c])
    for c in range(NC // 2):
        store(c).start()
    src = A.reshape(A.shape[0] * PR, W)

    def side_sums(i0):
        for q in range(GP):
            KS[pl.ds(q * W, W), :] = jnp.transpose(AT[rows(i0 + q, -1), :] + AT[rows(i0 + q, 1), :])
    side_sums(place(NG // 2))
    for c in range(NC // 2, NC):
        @pl.loop(c * GC, (c + 1) * GC)
        def _(g):
            i0 = place(g)
            base = pl.multiple_of(i0 * PR, S)

            def at(q, r):
                return pl.ds(base + (q * PR + S + r), RB)
            for t in range(W // RB):
                r = t * RB
                um, uc = src[at(0, r), :], src[at(1, r), :]
                for q in range(GP):
                    un = src[at(q + 2, r), :]
                    total = (um + un) + (src[at(q + 1, r - 1), :] + src[at(q + 1, r + 1), :]) + KS[pl.ds(q * W + r, RB), :]
                    new = (3.0 * uc + (total + F[i0 + q, pl.ds(r, RB), :])) * F32(1 / 9)
                    O[(g - NG // 2) * GP + q, pl.ds(r, RB), :] = new
                    um, uc = uc, un
            side_sums(place((g + 1) % NG))
        store(c).start()
    for c in range(NC):
        store(c).wait()


def solution(mesh):
    spec = P(('dp', 'sx'), 'sy', 'sz')

    def local(f, u):
        size = 2 * f.shape[1]
        h2 = 1.0 / float((size + 1) ** 2)
        vm = lambda *s: pltpu.VMEM(s, F32)
        scratch = [vm(N * PR, W), vm(129, XR, W),
                   vm(XR, W), vm(XR, W), vm(5, 136, W), vm(GP * W, W), vm(2, N, W), vm(2, N, W), vm(2, N, W), vm(2, N, W)]
        scratch += [vm(L1.rows, W)] * 2 + [vm(L2.rows, W)] * 3 + [vm(S * 48, W)] * 3
        for L in (L1, L2):
            z = up8((L.n + 1) * L.h)
            scratch += [vm(L.h * (L.n + S), W)] * 2 + [vm(z, W)] * 2 + [vm(L.h * S, W)] * 2
        scratch += [vm(S * (L3.n + 1), W), vm(3, S * (L3.n + 1), W)]
        dma = pltpu.SemaphoreType.DMA
        scratch += [dma((2, NC)), dma((2,)), dma((2,)), dma((2, NC)), dma((2, NC)), dma((2, NC)), dma((2, NC)),
                    dma((15,)), dma((15,))]
        resident = [vm(130, PR, W), vm(130, PR, W), vm(N * PR, W), vm(N, N, W)]
        used = 4 * sum(math.prod(x.shape) for x in resident)
        kept = pl.pallas_call(
            functools.partial(body, h2),
            out_shape=resident,
            in_specs=[pl.BlockSpec(memory_space=pl.ANY)] * 2,
            out_specs=[pl.BlockSpec(memory_space=pltpu.VMEM)] * len(resident),
            scratch_shapes=scratch,
            compiler_params=pltpu.CompilerParams(collective_id=0, has_side_effects=True, vmem_limit_bytes=67043328 - used),
        )(f, u)
        kept = [pltpu.with_memory_space_constraint(x, pltpu.VMEM) for x in kept]
        return pl.pallas_call(
            close,
            out_shape=jax.ShapeDtypeStruct(f.shape, F32),
            in_specs=[pl.BlockSpec(memory_space=pltpu.VMEM)] * len(kept),
            out_specs=pl.BlockSpec(memory_space=pl.ANY),
            scratch_shapes=[vm(N // 2, N, W), vm(GP * W, W), dma((NC,))],
            compiler_params=pltpu.CompilerParams(vmem_limit_bytes=67043328 - used),
        )(*kept)

    def run(rhs_grid, u_start):
        return jax.shard_map(local, mesh=mesh, in_specs=(spec, spec), out_specs=spec, check_vma=False)(rhs_grid, u_start)
    return run
```
